8 devices in a mesh: dp: 1 (over z), ws: 8 (over y, x, core).
Axes of the slice: x: 2, y: 2, z: 1, core: 2. Of those that a mesh axis runs over, the one named last changes fastest.
Arguments:
- hidden: bfloat16 [128, 768], P(('dp', 'ws'))
- self_k: bfloat16 [128, 12, 512, 64], P(('dp', 'ws'))
- self_v: bfloat16 [128, 12, 512, 64], P(('dp', 'ws'))
- cross_k: bfloat16 [128, 12, 384, 64], P(('dp', 'ws'))
- cross_v: bfloat16 [128, 12, 384, 64], P(('dp', 'ws'))
- positions: int32 [128], P(('dp', 'ws'))
- enc_mask: int32 [128, 384], P(('dp', 'ws'))
- rel_bias: float32 [12, 512], replicated
- expert_idx: int32 [128], P(('dp', 'ws'))
- ln_self: float32 [768], replicated
- ln_cross: float32 [768], replicated
- ln_ffn: float32 [768], replicated
- wq_self: bfloat16 [768, 768], P(None, 'ws')
- wk_self: bfloat16 [768, 768], P(None, 'ws')
- wv_self: bfloat16 [768, 768], P(None, 'ws')
- wo_self: bfloat16 [768, 768], P(None, 'ws')
- wq_cross: bfloat16 [768, 768], P(None, 'ws')
- wo_cross: bfloat16 [768, 768], P(None, 'ws')
- w_router: float32 [768, 8], P(None, 'ws')
- w_in: bfloat16 [8, 768, 3072], P(None, None, 'ws')
- w_out: bfloat16 [8, 3072, 768], P(None, 'ws')
Outputs:
- output 1: bfloat16 [128, 768], P(('dp', 'ws'))
- output 2: bfloat16 [128, 12, 512, 64], P(('dp', 'ws'))
- output 3: bfloat16 [128, 12, 512, 64], P(('dp', 'ws'))
All inputs are finite; a program needn't handle non-finite values.
Results may differ from the reference program's by a relative error of at most 0.0114859.
Values are sent between devices in bfloat16 or wider.
A program may use at most 1 GiB of HBM per device.

```python
import jax
import jax.numpy as jnp
from jax import lax

D_MODEL = 768
NUM_HEADS = 12
HEAD_DIM = 64
D_FF = 3072
EXPERTS = 8
CACHE_LEN = 512
SRC_LEN = 384
GROUP_ROWS = 128

ATTN_WIDTH = NUM_HEADS * HEAD_DIM
CAPACITY = (2 * GROUP_ROWS + EXPERTS - 1) // EXPERTS
EPSILON = 1e-6
NEG_BIG = -1e30


def scaled_normal(key, shape, scale):
    return (jax.random.normal(key, shape, jnp.float32) * scale).astype(jnp.bfloat16)


def setup_inputs(seed: int = 0, part: int = 0) -> dict:
    base_key = jax.random.key(seed)
    shared = jax.random.split(base_key, 13)
    part_keys = jax.random.split(jax.random.fold_in(base_key, part), 12)
    row_ids = jnp.arange(GROUP_ROWS)
    cache_shape = (GROUP_ROWS, NUM_HEADS, CACHE_LEN, HEAD_DIM)
    src_shape = (GROUP_ROWS, NUM_HEADS, SRC_LEN, HEAD_DIM)
    hidden = scaled_normal(part_keys[0], (GROUP_ROWS, D_MODEL), 1.0)
    self_k = scaled_normal(part_keys[1], cache_shape, 1.0)
    self_v = scaled_normal(part_keys[2], cache_shape, 1.0)
    cross_k = scaled_normal(part_keys[3], src_shape, 1.0)
    cross_v = scaled_normal(part_keys[4], src_shape, 1.0)
    positions = jax.random.randint(part_keys[5], (GROUP_ROWS,), 0, CACHE_LEN)
    last_row = jax.random.randint(part_keys[6], (), 0, GROUP_ROWS)
    positions = jnp.where(row_ids == last_row, CACHE_LEN - 1, positions).astype(jnp.int32)
    src_lens = jax.random.randint(part_keys[7], (GROUP_ROWS,), 1, SRC_LEN + 1)
    full_row = jax.random.randint(part_keys[8], (), 0, GROUP_ROWS)
    src_lens = jnp.where(row_ids == full_row, SRC_LEN, src_lens)
    enc_mask = (jnp.arange(SRC_LEN)[None, :] < src_lens[:, None]).astype(jnp.int32)
    hot_expert = jax.random.randint(part_keys[9], (), 0, EXPERTS)
    free_pick = jax.random.randint(part_keys[10], (GROUP_ROWS,), 0, EXPERTS)
    row_order = jax.random.permutation(part_keys[11], GROUP_ROWS)
    hot_rows = jnp.zeros((GROUP_ROWS,), jnp.int32).at[row_order[:CAPACITY + 1]].set(1)
    expert_idx = jnp.where(hot_rows == 1, hot_expert, free_pick).astype(jnp.int32)
    return {
        'hidden': hidden,
        'self_k': self_k,
        'self_v': self_v,
        'cross_k': cross_k,
        'cross_v': cross_v,
        'positions': positions,
        'enc_mask': enc_mask,
        'rel_bias': jax.random.normal(shared[0], (NUM_HEADS, CACHE_LEN), jnp.float32),
        'expert_idx': expert_idx,
        'ln_self': jax.random.uniform(shared[1], (D_MODEL,), jnp.float32, 0.5, 1.5),
        'ln_cross': jax.random.uniform(shared[2], (D_MODEL,), jnp.float32, 0.5, 1.5),
        'ln_ffn': jax.random.uniform(shared[3], (D_MODEL,), jnp.float32, 0.5, 1.5),
        'wq_self': scaled_normal(shared[4], (D_MODEL, ATTN_WIDTH), 1.5 * (D_MODEL * HEAD_DIM) ** -0.5),
        'wk_self': scaled_normal(shared[5], (D_MODEL, ATTN_WIDTH), D_MODEL ** -0.5),
        'wv_self': scaled_normal(shared[6], (D_MODEL, ATTN_WIDTH), D_MODEL ** -0.5),
        'wo_self': scaled_normal(shared[7], (ATTN_WIDTH, D_MODEL), ATTN_WIDTH ** -0.5),
        'wq_cross': scaled_normal(shared[8], (D_MODEL, ATTN_WIDTH), 1.5 * (D_MODEL * HEAD_DIM) ** -0.5),
        'wo_cross': scaled_normal(shared[9], (ATTN_WIDTH, D_MODEL), ATTN_WIDTH ** -0.5),
        'w_router': jax.random.normal(shared[10], (D_MODEL, EXPERTS), jnp.float32) * D_MODEL ** -0.5,
        'w_in': scaled_normal(shared[11], (EXPERTS, D_MODEL, D_FF), D_MODEL ** -0.5),
        'w_out': scaled_normal(shared[12], (EXPERTS, D_FF, D_MODEL), (EXPERTS / D_FF) ** 0.5),
    }


def rms_norm(hidden, scale):
    hid_f32 = hidden.astype(jnp.float32)
    inv_rms = lax.rsqrt(jnp.mean(hid_f32 * hid_f32, axis=-1, keepdims=True) + EPSILON)
    return (hid_f32 * inv_rms * scale).astype(jnp.bfloat16)


def attend_row(row_args):
    queries, cache_keys, cache_vals, score_bias = row_args
    scores = jnp.einsum('hd,hld->hl', queries.astype(jnp.float32), cache_keys.astype(jnp.float32)) + score_bias
    attn_probs = jax.nn.softmax(scores, axis=-1).astype(jnp.bfloat16)
    context = jnp.einsum('hl,hld->hd', attn_probs.astype(jnp.float32), cache_vals.astype(jnp.float32))
    return context.astype(jnp.bfloat16)


def project(x_norm, weight):
    return jnp.dot(x_norm, weight, preferred_element_type=jnp.float32).astype(jnp.bfloat16)


def reference(hidden, self_k, self_v, cross_k, cross_v, positions, enc_mask, rel_bias, expert_idx,
              ln_self, ln_cross, ln_ffn, wq_self, wk_self, wv_self, wo_self, wq_cross, wo_cross,
              w_router, w_in, w_out):
    head_shape = (GROUP_ROWS, NUM_HEADS, HEAD_DIM)
    x_norm = rms_norm(hidden, ln_self)
    queries = project(x_norm, wq_self).reshape(head_shape)
    k_new = project(x_norm, wk_self).reshape(head_shape)
    v_new = project(x_norm, wv_self).reshape(head_shape)
    distance = positions[:, None] - jnp.arange(CACHE_LEN)[None, :]
    write_mask = (distance == 0)[:, None, :, None]
    new_self_k = jnp.where(write_mask, k_new[:, :, None, :], self_k)
    new_self_v = jnp.where(write_mask, v_new[:, :, None, :], self_v)
    pos_bias = jnp.take(rel_bias, jnp.clip(distance, 0, CACHE_LEN - 1), axis=1)
    pos_bias = jnp.where(distance[None] >= 0, pos_bias, NEG_BIG).transpose(1, 0, 2)
    context = lax.map(attend_row, (queries, new_self_k, new_self_v, pos_bias))
    attn_out = jnp.dot(context.reshape(GROUP_ROWS, ATTN_WIDTH), wo_self, preferred_element_type=jnp.float32)
    after_self = (hidden.astype(jnp.float32) + attn_out).astype(jnp.bfloat16)

    x_norm = rms_norm(after_self, ln_cross)
    queries = project(x_norm, wq_cross).reshape(head_shape)
    mask_bias = jnp.where(enc_mask == 1, 0.0, NEG_BIG)[:, None, :]
    context = lax.map(attend_row, (queries, cross_k, cross_v, mask_bias))
    attn_out = jnp.dot(context.reshape(GROUP_ROWS, ATTN_WIDTH), wo_cross, preferred_element_type=jnp.float32)
    after_cross = (after_self.astype(jnp.float32) + attn_out).astype(jnp.bfloat16)

    x_norm = rms_norm(after_cross, ln_ffn)
    logits = jnp.dot(x_norm.astype(jnp.float32), w_router, precision=lax.Precision.HIGHEST,
                     preferred_element_type=jnp.float32)
    router_probs = jax.nn.softmax(logits, axis=-1)
    chosen = jnp.arange(EXPERTS)[None, :] == expert_idx[:, None]
    gate_val = jnp.sum(jnp.where(chosen, router_probs, 0.0), axis=-1)
    row_ids = jnp.arange(GROUP_ROWS)
    earlier = (expert_idx[None, :] == expert_idx[:, None]) & (row_ids[None, :] < row_ids[:, None])
    slot_idx = jnp.sum(earlier.astype(jnp.int32), axis=1)
    keep_gate = jnp.where(slot_idx < CAPACITY, gate_val, 0.0)

    def expert_row(row_args):
        x_row, expert = row_args
        ffn_hidden = jnp.dot(x_row[None, :], w_in[expert], preferred_element_type=jnp.float32)
        ffn_hidden = jax.nn.relu(ffn_hidden).astype(jnp.bfloat16)
        ffn_out = jnp.dot(ffn_hidden, w_out[expert], preferred_element_type=jnp.float32)
        return ffn_out.astype(jnp.bfloat16)[0]

    expert_out = lax.map(expert_row, (x_norm, expert_idx))
    hidden_out = (after_cross.astype(jnp.float32) + expert_out.astype(jnp.float32) * keep_gate[:, None]).astype(jnp.bfloat16)
    return (hidden_out, new_self_k, new_self_v)
```

```python
import functools
import jax
import jax.numpy as jnp
from jax import lax
from jax.sharding import PartitionSpec as P
from jax.experimental import pallas as pl
from jax.experimental.pallas import tpu as pltpu

EPSILON = 1e-6
NEG_BIG = -1e30
LANES = 128
GROUP = 2
PIECES = 2
NT = (((1,), (1,)), ((), ()))
MESH = pl.DeviceIdType.MESH
VMEM = pl.BlockSpec(memory_space=pltpu.VMEM)
HBM = pl.BlockSpec(memory_space=pltpu.HBM)
SMEM = pl.BlockSpec(memory_space=pltpu.SMEM)


def hbm(x):
    return pltpu.with_memory_space_constraint(x, pltpu.HBM)


def rms_norm(hidden, scale):
    hid_f32 = hidden.astype(jnp.float32)
    inv_rms = lax.rsqrt(jnp.mean(hid_f32 * hid_f32, axis=-1, keepdims=True) + EPSILON)
    return (hid_f32 * inv_rms * scale).astype(jnp.bfloat16)


def entry_barrier(me, n):
    barrier = pltpu.get_barrier_semaphore()
    for k in range(1, n):
        pl.semaphore_signal(barrier, inc=1, device_id={'ws': lax.rem(me + k, n)}, device_id_type=MESH)
    pl.semaphore_wait(barrier, n - 1)


def remote(src, dst, send_sem, recv_sem, peer):
    return pltpu.make_async_remote_copy(src_ref=src, dst_ref=dst, send_sem=send_sem, recv_sem=recv_sem,
                                        device_id={'ws': peer}, device_id_type=MESH)


def reverse_lanes(x):
    size = x.shape[-1]
    lane = lax.broadcasted_iota(jnp.int32, x.shape, 1)
    step = 1
    while step < size:
        x = jnp.where((lane & step) != 0, pltpu.roll(x, step, 1), pltpu.roll(x, size - step, 1))
        step *= 2
    return x


def gather_kernel(n, hid, eid, ln, bias, wr, wq, wk, wv, wo, wqc, woc, sk, sv, ck, cv,
                  qkv, eid_all, wr_all, bias_rev, wo_all, wqc_all, woc_all, *rest):
    caches, (hall, wqkv, snd, loc_sem, s1, r1, s2, r2, sw, rw) = rest[:4 * PIECES], rest[4 * PIECES:]
    me = lax.axis_index('ws')
    rows, width = hid.shape
    cols = wq.shape[0]
    core, xpos, ypos = lax.rem(me, 2), lax.rem(me // 2, 2), me // 4
    pair = me + 1 - 2 * core
    xnb = me + 2 - 4 * xpos
    ynb = me + 4 - 8 * ypos
    diag = me + 2 - 4 * xpos + 4 - 8 * ypos

    locals_ = []

    def local(src, dst):
        copy = pltpu.make_async_copy(src, dst, loc_sem.at[len(locals_)])
        copy.start()
        locals_.append(copy)
        return copy

    def load_cache(i, src):
        size = src.shape[0] // PIECES
        for t in range(PIECES):
            local(src.at[pl.ds(t * size, size)], caches[i * PIECES + t])

    proj = [local(w, wqkv.at[i]) for i, w in enumerate((wq, wk, wv))]
    for r in range(rows):
        eid_all[me, r:r + 1, :] = jnp.full((1, LANES), eid[r], jnp.int32)
    wr_all[me] = wr[...]
    hall[me] = hid[...]
    entry_barrier(me, n)

    first = []
    for k in range(1, n):
        peer = lax.rem(me + k, n)
        first.append(remote(hid, hall.at[me], s1.at[k - 1, 0], r1.at[k - 1, 0], peer))
        first[-1].start()
    for k in range(1, n):
        peer = lax.rem(me + k, n)
        first.append(remote(eid_all.at[me], eid_all.at[me], s1.at[k - 1, 1], r1.at[k - 1, 1], peer))
        first[-1].start()
        first.append(remote(wr, wr_all.at[me], s1.at[k - 1, 2], r1.at[k - 1, 2], peer))
        first[-1].start()

    fulls = ((wo, wo_all), (wqc, wqc_all), (woc, woc_all))
    half = cols // 2
    to_x, to_y, to_p = [], [], []
    sent = []

    def own_share(i):
        src, dst = fulls[i]
        at = dst.at[pl.ds(pl.multiple_of(me * cols, cols), cols)]
        to_x.append(remote(src, at, sw.at[0, i], rw.at[0, i], xnb))
        to_y.append(remote(src, at, sw.at[1, i], rw.at[1, i], ynb))
        to_p.append(remote(src, at, sw.at[2, i], rw.at[2, i], pair))
        for c in (to_x[-1], to_y[-1], to_p[-1]):
            c.start()
            sent.append(c)
        local(src, at)

    own_share(0)
    load_cache(0, sk)
    load_cache(1, sv)
    bias_rev[...] = reverse_lanes(jnp.concatenate(
        [bias[...], jnp.zeros((bias_rev.shape[0] - bias.shape[0], bias.shape[1]), jnp.float32)], axis=0))

    for c in first[:n - 1]:
        c.wait_recv()
    for c in proj:
        c.wait()
    x_norm = rms_norm(hall[...].reshape(n * rows, width), ln[...])
    for i in range(3):
        y = lax.dot_general(x_norm, wqkv[i], NT, preferred_element_type=jnp.float32)
        snd[:, i] = y.astype(jnp.bfloat16).reshape(n, rows, cols)
    second = []
    for k in range(1, n):
        peer = lax.rem(me + k, n)
        second.append(remote(snd.at[peer], qkv.at[me], s2.at[k - 1], r2.at[k - 1], peer))
        second[-1].start()
    qkv[me] = snd[me]
    own_share(1)
    own_share(2)
    load_cache(2, ck)
    load_cache(3, cv)

    def block(ref, dev, lo, size):
        return ref.at[pl.ds(pl.multiple_of(dev * cols + lo, half), size)]

    def forward(src_dev, lo, size, i, slot, peer):
        dst = fulls[i][1]
        c = remote(block(dst, src_dev, lo, size), block(dst, src_dev, lo, size), sw.at[slot, i], rw.at[slot, i], peer)
        c.start()
        sent.append(c)
        return c

    relay_y, relay_x, pairs = [], [], []
    for i in range(3):
        to_x[i].wait_recv()
        relay_y.append(forward(xnb, 0, half, i, 3, ynb))
        pairs.append(forward(xnb, 0, cols, i, 4, pair))
        to_y[i].wait_recv()
        relay_x.append(forward(ynb, half, half, i, 5, xnb))
        pairs.append(forward(ynb, 0, cols, i, 6, pair))
        if i:
            relay_y[i - 1].wait_recv()
            pairs.append(forward(diag, 0, half, i - 1, 7, pair))
            relay_x[i - 1].wait_recv()
            pairs.append(forward(diag, half, half, i - 1, 8, pair))
    relay_y[2].wait_recv()
    pairs.append(forward(diag, 0, half, 2, 7, pair))
    relay_x[2].wait_recv()
    pairs.append(forward(diag, half, half, 2, 8, pair))

    for c in first[n - 1:]:
        c.wait_recv()
    for c in second:
        c.wait_recv()
    for c in to_p + pairs:
        c.wait_recv()
    for c in first + second + sent:
        c.wait_send()
    for c in locals_[3:]:
        c.wait()


def attn_kernel(pos, hid, qkv, bias_rev, mask, ln_c, ln_f, wo, wqc, woc, *rest):
    cross, (h2_out, x_out, nk, nv), self_kv, (q_sc, ctx_sc, kt_sc, vt_sc, out_sem) = (
        rest[2 * PIECES:4 * PIECES], rest[4 * PIECES:4 * PIECES + 4], rest[4 * PIECES + 4:-5], rest[-5:])
    n, _, rows, cols = qkv.shape
    width = hid.shape[1]
    heads = bias_rev.shape[0]
    head_dim = 64
    self_len = nk.shape[2]
    piece = rows // PIECES
    f32 = jnp.float32
    head_of = lax.broadcasted_iota(jnp.int32, (heads, width), 1) // head_dim
    head_mask = head_of == lax.broadcasted_iota(jnp.int32, (heads, width), 0)
    lane = lax.broadcasted_iota(jnp.int32, (1, LANES), 1)
    key_pos = lax.broadcasted_iota(jnp.int32, (1, self_len), 1)

    def assemble(i):
        return jnp.concatenate([qkv[p, i].astype(f32) for p in range(n)], axis=1)

    q_sc[...] = assemble(0)
    for i, ref in ((1, kt_sc), (2, vt_sc)):
        padded = jnp.concatenate([assemble(i), jnp.zeros((LANES - rows, width), f32)], axis=0)
        cols_t = padded.T
        for g in range(rows // GROUP):
            shifted = cols_t if g == 0 else pltpu.roll(cols_t, LANES - g * GROUP, 1)
            ref[g] = shifted.astype(jnp.bfloat16)

    def softmax(s):
        e = jnp.exp(s - jnp.max(s, axis=-1, keepdims=True))
        return (e / jnp.sum(e, axis=-1, keepdims=True)).astype(jnp.bfloat16)

    def heads_q(b):
        return jnp.where(head_mask, q_sc[pl.ds(b, 1), :], 0.0).astype(jnp.bfloat16)

    def context(b, probs, vals):
        o = lax.dot_general(probs, vals, NT, preferred_element_type=f32)
        ctx_sc[pl.ds(b, 1), :] = jnp.sum(jnp.where(head_mask, o, 0.0), axis=0, keepdims=True)

    for t in range(PIECES):
        keys, vals = self_kv[t], self_kv[PIECES + t]

        @pl.loop(0, piece // GROUP)
        def _(i):
            g = t * (piece // GROUP) + i
            for j in range(GROUP):
                r = i * GROUP + j
                p = pos[g * GROUP + j]
                win = pl.ds(pl.multiple_of((p // LANES) * LANES, LANES), LANES)
                hit = lane == p % LANES
                for cache, new in ((keys, kt_sc), (vals, vt_sc)):
                    cache[r, :, win] = jnp.where(hit, new[g, :, j:j + 1], cache[r, :, win])
            for j in range(GROUP):
                b, r = g * GROUP + j, i * GROUP + j
                p = pos[b]
                s = jnp.dot(heads_q(b), keys[r], preferred_element_type=f32)
                s = s + jnp.where(key_pos <= p, pltpu.roll(bias_rev[...], lax.rem(p + 1, self_len), 1), NEG_BIG)
                context(b, softmax(s), vals[r])
            for j in range(GROUP):
                b, r = g * GROUP + j, i * GROUP + j
                pltpu.make_async_copy(keys.at[r], nk.at[b], out_sem.at[0, b]).start()
                pltpu.make_async_copy(vals.at[r], nv.at[b], out_sem.at[1, b]).start()

    def project(x, w):
        return lax.dot_general(x, w[...], NT, preferred_element_type=f32)

    h1 = (hid[...].astype(f32) + project(ctx_sc[...].astype(jnp.bfloat16), wo)).astype(jnp.bfloat16)
    q_sc[...] = project(rms_norm(h1, ln_c[...]), wqc).astype(jnp.bfloat16).astype(f32)

    for t in range(PIECES):
        keys, vals = cross[t], cross[PIECES + t]

        @pl.loop(0, piece // GROUP)
        def _(i):
            for j in range(GROUP):
                r = i * GROUP + j
                b = t * piece + r
                s = jnp.dot(heads_q(b), keys[r], preferred_element_type=f32)
                s = s + jnp.where(mask[pl.ds(b, 1), :] == 1, 0.0, NEG_BIG)
                context(b, softmax(s), vals[r])

    h2 = (h1.astype(f32) + project(ctx_sc[...].astype(jnp.bfloat16), woc)).astype(jnp.bfloat16)
    h2_out[...] = h2
    x_out[...] = rms_norm(h2, ln_f[...])

    for b in range(rows):
        t, r = b // piece, b % piece
        pltpu.make_async_copy(self_kv[t].at[r], nk.at[b], out_sem.at[0, b]).wait()
        pltpu.make_async_copy(self_kv[PIECES + t].at[r], nv.at[b], out_sem.at[1, b]).wait()


def ffn_kernel(n, capacity, x, h2, eid_all, wr_all, win, wout, out,
               xall, win_v, wout_v, part, acc, loc_sem, s1, r1, s2, r2):
    me = lax.axis_index('ws')
    rows, width = x.shape
    experts, _, hidden_units = win.shape
    group_rows = n * rows
    f32 = jnp.float32
    loads = [pltpu.make_async_copy(win, win_v, loc_sem.at[0]), pltpu.make_async_copy(wout, wout_v, loc_sem.at[1])]
    for c in loads:
        c.start()
    xall[me] = x[...]
    entry_barrier(me, n)
    first = []
    for k in range(1, n):
        peer = lax.rem(me + k, n)
        first.append(remote(x, xall.at[me], s1.at[k - 1], r1.at[k - 1], peer))
        first[-1].start()

    logits = [jnp.sum(x[...].astype(f32) * wr_all[e], axis=-1, keepdims=True) for e in range(experts)]
    top = functools.reduce(jnp.maximum, logits)
    exps = [jnp.exp(l - top) for l in logits]
    total = functools.reduce(jnp.add, exps)
    eid = eid_all[...].reshape(group_rows, LANES)
    own = eid_all[me]
    own_col = own[:, 0:1]
    chosen = functools.reduce(jnp.add, [jnp.where(own_col == e, exps[e], 0.0) for e in range(experts)])
    across = eid.astype(f32).T[0:1, :].astype(jnp.int32)
    row_ids = me * rows + lax.broadcasted_iota(jnp.int32, (rows, group_rows), 0)
    earlier = (across == own_col) & (lax.broadcasted_iota(jnp.int32, (rows, group_rows), 1) < row_ids)
    slot = jnp.sum(jnp.where(earlier, 1.0, 0.0), axis=1, keepdims=True)
    keep_gate = jnp.where(slot < capacity, chosen / total, 0.0)

    for c in first:
        c.wait_recv()
    for c in loads:
        c.wait()
    xs = xall[...].reshape(group_rows, width)
    eid_col = eid[:, 0:1]
    y = jnp.zeros((group_rows, width), f32)
    for e in range(experts):
        u = jnp.dot(xs, win_v[e], preferred_element_type=f32)
        u = jnp.where(eid_col == e, jnp.maximum(u, 0.0), 0.0).astype(jnp.bfloat16)
        y += jnp.dot(u, wout_v[e], preferred_element_type=f32)
    part[...] = y.reshape(n, rows, width)
    second = []
    for k in range(1, n):
        peer = lax.rem(me + k, n)
        second.append(remote(part.at[peer], acc.at[me], s2.at[k - 1], r2.at[k - 1], peer))
        second[-1].start()
    acc[me] = part[me]
    for c in second:
        c.wait_recv()
    y_own = functools.reduce(jnp.add, [acc[p] for p in range(n)]).astype(jnp.bfloat16)
    out[...] = (h2[...].astype(f32) + y_own.astype(f32) * keep_gate).astype(jnp.bfloat16)
    for c in first + second:
        c.wait_send()


def solution(mesh):
    n = mesh.shape['ws']
    row_axes = ('dp', 'ws')
    row_vec = P(row_axes)
    row_mat = P(row_axes, None)
    cache_spec = P(row_axes, None, None, None)
    col_split = P(None, 'ws')
    in_specs = (row_mat, cache_spec, cache_spec, cache_spec, cache_spec, row_vec, row_mat, P(None, None), row_vec,
                P(None), P(None), P(None), col_split, col_split, col_split, col_split, col_split, col_split,
                col_split, P(None, None, 'ws'), P(None, 'ws', None))
    out_specs = (row_mat, cache_spec, cache_spec)

    def decoder_block(hidden, self_k, self_v, cross_k, cross_v, positions, enc_mask, rel_bias, expert_idx,
                      ln_self, ln_cross, ln_ffn, wq_self, wk_self, wv_self, wo_self, wq_cross, wo_cross,
                      w_router, w_in, w_out):
        rows, width = hidden.shape
        heads, head_dim = self_k.shape[1], self_k.shape[3]
        cols = wq_self.shape[1]
        experts, _, units = w_in.shape
        group_rows = rows * n
        capacity = (2 * group_rows + experts - 1) // experts
        bf16, f32, i32 = jnp.bfloat16, jnp.float32, jnp.int32
        pad_heads = 16
        dma = pltpu.SemaphoreType.DMA

        def flat(cache):
            return cache.transpose(0, 1, 3, 2).reshape(rows, heads * head_dim, cache.shape[2])

        sk, sv, ck, cv = (flat(c) for c in (self_k, self_v, cross_k, cross_v))
        pieces = [pltpu.VMEM((rows // PIECES,) + c.shape[1:], bf16) for c in (sk, sv, ck, cv) for _ in range(PIECES)]
        gathered = pl.pallas_call(
            functools.partial(gather_kernel, n),
            out_shape=(
                pltpu.VMEM((n, 3, rows, cols), bf16), pltpu.VMEM((n, rows, LANES), i32), pltpu.VMEM((n, 1, width), f32),
                pltpu.VMEM((pad_heads, rel_bias.shape[1]), f32),
                pltpu.VMEM((n * cols, width), bf16), pltpu.VMEM((n * cols, width), bf16), pltpu.VMEM((n * cols, width), bf16),
                *pieces),
            in_specs=[VMEM, SMEM, VMEM, VMEM, VMEM] + [HBM] * 10,
            out_specs=(VMEM,) * (7 + len(pieces)),
            scratch_shapes=[pltpu.VMEM((n, rows, width), bf16), pltpu.VMEM((3, cols, width), bf16),
                            pltpu.VMEM((n, 3, rows, cols), bf16), dma((6 + 4 * PIECES,)),
                            dma((n - 1, 3)), dma((n - 1, 3)), dma((n - 1,)), dma((n - 1,)), dma((9, 3)), dma((9, 3))],
            compiler_params=pltpu.CompilerParams(collective_id=0, has_side_effects=True, vmem_limit_bytes=7 << 20),
            name='gather')(hidden, expert_idx, ln_self.reshape(1, width), rel_bias, w_router.T,
                           wq_self.T, wk_self.T, wv_self.T, wo_self.T, wq_cross.T, wo_cross.T, hbm(sk), hbm(sv), hbm(ck), hbm(cv))
        qkv, eid_all, wr_all, bias_rev, wo_all, wqc_all, woc_all, *caches = gathered

        h2, x, new_k, new_v, *_ = pl.pallas_call(
            attn_kernel,
            out_shape=(pltpu.VMEM((rows, width), bf16), pltpu.VMEM((rows, width), bf16),
                       pltpu.HBM(sk.shape, bf16), pltpu.HBM(sv.shape, bf16),
                       *pieces[:2 * PIECES]),
            in_specs=[SMEM] + [VMEM] * (9 + len(pieces)),
            out_specs=(VMEM, VMEM, HBM, HBM) + (VMEM,) * (2 * PIECES),
            input_output_aliases={10 + t: 4 + t for t in range(2 * PIECES)},
            scratch_shapes=[pltpu.VMEM((rows, width), f32), pltpu.VMEM((rows, width), f32),
                            pltpu.VMEM((rows // GROUP, width, LANES), bf16), pltpu.VMEM((rows // GROUP, width, LANES), bf16),
                            dma((2, rows))],
            compiler_params=pltpu.CompilerParams(vmem_limit_bytes=7 << 20),
            name='attend')(positions, hidden, qkv, bias_rev, enc_mask, ln_cross.reshape(1, width), ln_ffn.reshape(1, width),
                           wo_all, wqc_all, woc_all, *caches)

        hidden_out = pl.pallas_call(
            functools.partial(ffn_kernel, n, capacity),
            out_shape=jax.ShapeDtypeStruct((rows, width), bf16),
            in_specs=[VMEM] * 4 + [HBM] * 2,
            out_specs=VMEM,
            scratch_shapes=[pltpu.VMEM((n, rows, width), bf16), pltpu.VMEM(w_in.shape, bf16), pltpu.VMEM(w_out.shape, bf16),
                            pltpu.VMEM((n, rows, width), f32), pltpu.VMEM((n, rows, width), f32), dma((2,)),
                            dma((n - 1,)), dma((n - 1,)), dma((n - 1,)), dma((n - 1,))],
            compiler_params=pltpu.CompilerParams(collective_id=1, has_side_effects=True, vmem_limit_bytes=20 << 20),
            name='experts')(x, h2, eid_all, wr_all, hbm(w_in), hbm(w_out))

        def unflat(cache):
            return cache.reshape(rows, heads, head_dim, cache.shape[2]).transpose(0, 1, 3, 2)

        return hidden_out, unflat(new_k), unflat(new_v)

    return jax.shard_map(decoder_block, mesh=mesh, in_specs=in_specs, out_specs=out_specs, check_vma=False)
```

```python
import functools
import jax
import jax.numpy as jnp
from jax import lax
from jax.sharding import PartitionSpec as P
from jax.experimental import pallas as pl
from jax.experimental.pallas import tpu as pltpu

EPSILON = 1e-6
NEG_BIG = -1e30
LANES = 128
GROUP = 4
PIECES = 2
NT = (((1,), (1,)), ((), ()))
MESH = pl.DeviceIdType.MESH
VMEM = pl.BlockSpec(memory_space=pltpu.VMEM)
HBM = pl.BlockSpec(memory_space=pltpu.HBM)
SMEM = pl.BlockSpec(memory_space=pltpu.SMEM)


def hbm(x):
    return pltpu.with_memory_space_constraint(x, pltpu.HBM)


def rms_norm(hidden, scale):
    hid_f32 = hidden.astype(jnp.float32)
    inv_rms = lax.rsqrt(jnp.mean(hid_f32 * hid_f32, axis=-1, keepdims=True) + EPSILON)
    return (hid_f32 * inv_rms * scale).astype(jnp.bfloat16)


def entry_barrier(me, n):
    barrier = pltpu.get_barrier_semaphore()
    for k in range(1, n):
        pl.semaphore_signal(barrier, inc=1, device_id={'ws': lax.rem(me + k, n)}, device_id_type=MESH)
    pl.semaphore_wait(barrier, n - 1)


def remote(src, dst, send_sem, recv_sem, peer):
    return pltpu.make_async_remote_copy(src_ref=src, dst_ref=dst, send_sem=send_sem, recv_sem=recv_sem,
                                        device_id={'ws': peer}, device_id_type=MESH)


def reverse_lanes(x):
    size = x.shape[-1]
    lane = lax.broadcasted_iota(jnp.int32, x.shape, 1)
    step = 1
    while step < size:
        x = jnp.where((lane & step) != 0, pltpu.roll(x, step, 1), pltpu.roll(x, size - step, 1))
        step *= 2
    return x


def load_row(src, dst, sem):
    return pltpu.make_async_copy(src, dst.at[0], sem)


def head_mask_of(heads, width, head_dim):
    lane = lax.broadcasted_iota(jnp.int32, (heads, width), 1)
    return lane // head_dim == lax.broadcasted_iota(jnp.int32, (heads, width), 0)


def project(x, w):
    return lax.dot_general(x, w, NT, preferred_element_type=jnp.float32)


def gather_kernel(n, head_dim, hid, pos, eid, ln_s, ln_c, bias, wr, wq, wk, wv, wo, wqc, woc, sk, sv, ck, cv,
                  h1_out, qc_out, kv_out, eid_all, wr_all, wo_all, wqc_all, woc_all, *rest):
    caches = rest[:4 * PIECES]
    (hid_v, pos_s, eid_s, ln_sv, ln_cv, bias_v, hall, wqkv, snd, qkv, q_sc, s_sc, p_sc, b_sc, pn_sc, ctx_sc,
     loc_sem, s1, r1, s2, r2, sw, rw) = rest[4 * PIECES:]
    me = lax.axis_index('ws')
    rows, width = hid.shape
    cols = wq.shape[0]
    heads, length = b_sc.shape[1:]
    f32 = jnp.float32
    core, xpos, ypos = lax.rem(me, 2), lax.rem(me // 2, 2), me // 4
    pair = me + 1 - 2 * core
    xnb = me + 2 - 4 * xpos
    ynb = me + 4 - 8 * ypos
    diag = me + 2 - 4 * xpos + 4 - 8 * ypos

    locals_ = []

    def local(src, dst):
        copy = pltpu.make_async_copy(src, dst, loc_sem.at[len(locals_)])
        copy.start()
        locals_.append(copy)
        return copy

    def load_cache(i, src):
        size = src.shape[0] // PIECES
        for t in range(PIECES):
            local(src.at[pl.ds(t * size, size)], caches[i * PIECES + t])

    small = [local(hid, hid_v), local(wr, wr_all.at[me]), local(eid, eid_s), local(pos, pos_s),
             local(bias, bias_v), local(ln_s, ln_sv.at[0]), local(ln_c, ln_cv.at[0])]
    proj = [local(w, wqkv.at[i]) for i, w in enumerate((wq, wk, wv))]
    entry_barrier(me, n)
    for c in small:
        c.wait()
    first = []
    for k in range(1, n):
        peer = lax.rem(me + k, n)
        first.append(remote(hid_v, hall.at[me], s1.at[k - 1, 0], r1.at[k - 1, 0], peer))
        first[-1].start()

    fulls = ((wo, wo_all), (wqc, wqc_all), (woc, woc_all))
    half = cols // 2
    to_x, to_y, to_p = [], [], []
    sent = []
    for i in range(3):
        src, dst = fulls[i]
        at = dst.at[pl.ds(pl.multiple_of(me * cols, cols), cols)]
        to_x.append(remote(src, at, sw.at[0, i], rw.at[0, i], xnb))
        to_y.append(remote(src, at, sw.at[1, i], rw.at[1, i], ynb))
        to_p.append(remote(src, at, sw.at[2, i], rw.at[2, i], pair))
        for c in (to_x[-1], to_y[-1], to_p[-1]):
            c.start()
            sent.append(c)
        local(src, at)
    load_cache(0, sk)
    load_cache(1, sv)
    load_cache(2, ck)
    load_cache(3, cv)
    hall[me] = hid_v[...]
    for r in range(rows):
        eid_all[me, r:r + 1, :] = jnp.full((1, LANES), eid_s[r], jnp.int32)
    extra = []
    for k in range(1, n):
        peer = lax.rem(me + k, n)
        extra.append(remote(eid_all.at[me], eid_all.at[me], s1.at[k - 1, 1], r1.at[k - 1, 1], peer))
        extra[-1].start()
        extra.append(remote(wr_all.at[me], wr_all.at[me], s1.at[k - 1, 2], r1.at[k - 1, 2], peer))
        extra[-1].start()

    key_pos = lax.broadcasted_iota(jnp.int32, (1, length), 1)
    table = reverse_lanes(jnp.concatenate(
        [bias_v[...], jnp.zeros((heads - bias_v.shape[0], length), f32)], axis=0))

    @pl.loop(0, rows)
    def _(b):
        p = jnp.full((1, length), pos_s[b], jnp.int32)
        turned, step = table, 1
        while step < length:
            turned = jnp.where(((p + 1) & step) != 0, pltpu.roll(turned, step, 1), turned)
            step *= 2
        b_sc[b] = jnp.where(key_pos <= p, turned, NEG_BIG)

    for c in first:
        c.wait_recv()
    for c in proj:
        c.wait()
    x_norm = rms_norm(hall[...].reshape(n * rows, width), ln_sv[...])
    for i in range(3):
        snd[:, i] = project(x_norm, wqkv[i]).astype(jnp.bfloat16).reshape(n, rows, cols)
    second = []
    for k in range(1, n):
        peer = lax.rem(me + k, n)
        second.append(remote(snd.at[peer], qkv.at[me], s2.at[k - 1], r2.at[k - 1], peer))
        second[-1].start()
    qkv[me] = snd[me]

    def block(ref, dev, lo, size):
        return ref.at[pl.ds(pl.multiple_of(dev * cols + lo, half), size)]

    def forward(src_dev, lo, size, i, slot, peer):
        dst = fulls[i][1]
        c = remote(block(dst, src_dev, lo, size), block(dst, src_dev, lo, size), sw.at[slot, i], rw.at[slot, i], peer)
        c.start()
        sent.append(c)
        return c

    relay_y, relay_x, pairs = [], [], []

    def relay(i):
        to_x[i].wait_recv()
        relay_y.append(forward(xnb, 0, half, i, 3, ynb))
        pairs.append(forward(xnb, 0, cols, i, 4, pair))
        to_y[i].wait_recv()
        relay_x.append(forward(ynb, half, half, i, 5, xnb))
        pairs.append(forward(ynb, 0, cols, i, 6, pair))

    def relay_diag(i):
        relay_y[i].wait_recv()
        pairs.append(forward(diag, 0, half, i, 7, pair))
        relay_x[i].wait_recv()
        pairs.append(forward(diag, half, half, i, 8, pair))

    relay(0)
    for c in second:
        c.wait_recv()
    own_kv = locals_[len(small) + 3 + 3:]
    for c in own_kv[:2 * PIECES]:
        c.wait()

    def assemble(i):
        return jnp.concatenate([qkv[p, i].astype(f32) for p in range(n)], axis=1)

    q_sc[...] = assemble(0)
    kv_out[0] = assemble(1)
    kv_out[1] = assemble(2)
    head_mask = head_mask_of(heads, width, head_dim)
    piece = rows // PIECES

    def scores(t):
        @pl.loop(0, piece // GROUP)
        def _(i):
            for j in range(GROUP):
                r = i * GROUP + j
                b = t * piece + r
                q = jnp.where(head_mask, q_sc[pl.ds(b, 1), :], 0.0)
                s_new = jnp.sum(q * kv_out[0, pl.ds(b, 1), :], axis=1, keepdims=True)
                s = jnp.dot(q.astype(jnp.bfloat16), caches[t][r], preferred_element_type=f32)
                s_sc[b] = jnp.where(key_pos == pos_s[b], s_new, s) + b_sc[b]

    def softmax():
        @pl.loop(0, rows // GROUP)
        def _(i):
            for j in range(GROUP):
                b = i * GROUP + j
                s = s_sc[b]
                e = jnp.exp(s - jnp.max(s, axis=-1, keepdims=True))
                probs = (e / jnp.sum(e, axis=-1, keepdims=True)).astype(jnp.bfloat16).astype(f32)
                hit = key_pos == pos_s[b]
                p_new = jnp.sum(jnp.where(hit, probs, 0.0), axis=1, keepdims=True)
                pn_sc[b] = jnp.broadcast_to(p_new, (heads, LANES))
                p_sc[b] = jnp.where(hit, 0.0, probs).astype(jnp.bfloat16)

    def contexts(t):
        @pl.loop(0, piece // GROUP)
        def _(i):
            for j in range(GROUP):
                r = i * GROUP + j
                b = t * piece + r
                o = project(p_sc[b], caches[PIECES + t][r])
                o = o + pn_sc[b, :, 0:1] * kv_out[1, pl.ds(b, 1), :]
                ctx_sc[pl.ds(b, 1), :] = jnp.sum(jnp.where(head_mask, o, 0.0), axis=0, keepdims=True)

    scores(0)
    relay(1)
    scores(1)
    softmax()
    relay_diag(0)
    contexts(0)
    relay(2)
    relay_diag(1)
    contexts(1)
    relay_diag(2)

    def wait_weight(i):
        to_p[i].wait_recv()
        for c in pairs_of(i):
            c.wait_recv()
        locals_[len(small) + 3 + i].wait()

    def pairs_of(i):
        return [pairs[k] for k in order[i]]

    order = ([0, 1, 4, 5], [2, 3, 8, 9], [6, 7, 10, 11])
    wait_weight(0)
    h1 = (hid_v[...].astype(f32) + project(ctx_sc[...].astype(jnp.bfloat16), wo_all[...])).astype(jnp.bfloat16)
    h1_out[...] = h1
    wait_weight(1)
    qc_out[...] = project(rms_norm(h1, ln_cv[...]), wqc_all[...]).astype(jnp.bfloat16).astype(f32)
    wait_weight(2)
    for c in extra:
        c.wait_recv()
    for c in first + extra + second + sent:
        c.wait_send()
    for c in own_kv[2 * PIECES:]:
        c.wait()


def attn_kernel(head_dim, pos, h1, qc, kv, mask, ln_f, woc, *rest):
    cross, (h2_out, x_out, nk, nv), self_kv, (ln_v, s_sc, p_sc, ctx_sc, kt_sc, vt_sc, ln_sem, out_sem) = (
        rest[2 * PIECES:4 * PIECES], rest[4 * PIECES:4 * PIECES + 4], rest[4 * PIECES + 4:-8], rest[-8:])
    rows, width = h1.shape
    heads = s_sc.shape[1]
    piece = rows // PIECES
    f32 = jnp.float32
    load_ln = pltpu.make_async_copy(ln_f, ln_v.at[0], ln_sem)
    load_ln.start()
    head_mask = head_mask_of(heads, width, head_dim)
    lane = lax.broadcasted_iota(jnp.int32, (1, LANES), 1)

    for i, ref in ((0, kt_sc), (1, vt_sc)):
        cols_t = jnp.concatenate([kv[i], jnp.zeros((LANES - rows, width), f32)], axis=0).T
        for g in range(rows // GROUP):
            shifted = cols_t if g == 0 else pltpu.roll(cols_t, LANES - g * GROUP, 1)
            ref[g] = shifted.astype(jnp.bfloat16)

    for t in range(PIECES):
        keys, vals = self_kv[t], self_kv[PIECES + t]

        @pl.loop(0, piece // GROUP)
        def _(i):
            g = t * (piece // GROUP) + i
            for j in range(GROUP):
                r = i * GROUP + j
                b = t * piece + r
                q = jnp.where(head_mask, qc[pl.ds(b, 1), :], 0.0).astype(jnp.bfloat16)
                s = jnp.dot(q, cross[t][r], preferred_element_type=f32)
                s_sc[b] = s + jnp.where(mask[pl.ds(b, 1), :] == 1, 0.0, NEG_BIG)
                p = pos[b]
                win = pl.ds(pl.multiple_of((p // LANES) * LANES, LANES), LANES)
                hit = lane == p % LANES
                for cache, new in ((keys, kt_sc), (vals, vt_sc)):
                    cache[r, :, win] = jnp.where(hit, new[g, :, j:j + 1], cache[r, :, win])
            for j in range(GROUP):
                r = i * GROUP + j
                b = t * piece + r
                pltpu.make_async_copy(keys.at[r], nk.at[b], out_sem.at[0, b]).start()
                pltpu.make_async_copy(vals.at[r], nv.at[b], out_sem.at[1, b]).start()

    @pl.loop(0, rows // GROUP)
    def _(i):
        for j in range(GROUP):
            b = i * GROUP + j
            s = s_sc[b]
            e = jnp.exp(s - jnp.max(s, axis=-1, keepdims=True))
            p_sc[b] = (e / jnp.sum(e, axis=-1, keepdims=True)).astype(jnp.bfloat16)

    for t in range(PIECES):
        @pl.loop(0, piece // GROUP)
        def _(i):
            for j in range(GROUP):
                r = i * GROUP + j
                b = t * piece + r
                o = project(p_sc[b], cross[PIECES + t][r])
                ctx_sc[pl.ds(b, 1), :] = jnp.sum(jnp.where(head_mask, o, 0.0), axis=0, keepdims=True)

    h2 = (h1[...].astype(f32) + project(ctx_sc[...].astype(jnp.bfloat16), woc[...])).astype(jnp.bfloat16)
    h2_out[...] = h2
    load_ln.wait()
    x_out[...] = rms_norm(h2, ln_v[...])
    for b in range(rows):
        t, r = b // piece, b % piece
        pltpu.make_async_copy(self_kv[t].at[r], nk.at[b], out_sem.at[0, b]).wait()
        pltpu.make_async_copy(self_kv[PIECES + t].at[r], nv.at[b], out_sem.at[1, b]).wait()


def ffn_kernel(n, capacity, x, h2, eid_all, wr_all, win, wout, out,
               xall, win_v, wout_v, part, acc, loc_sem, s1, r1, s2, r2):
    me = lax.axis_index('ws')
    rows, width = x.shape
    experts, _, hidden_units = win.shape
    group_rows = n * rows
    f32 = jnp.float32
    loads = [pltpu.make_async_copy(win, win_v, loc_sem.at[0]), pltpu.make_async_copy(wout, wout_v, loc_sem.at[1])]
    for c in loads:
        c.start()
    xall[me] = x[...]
    entry_barrier(me, n)
    first = []
    for k in range(1, n):
        peer = lax.rem(me + k, n)
        first.append(remote(x, xall.at[me], s1.at[k - 1], r1.at[k - 1], peer))
        first[-1].start()

    logits = [jnp.sum(x[...].astype(f32) * wr_all[e], axis=-1, keepdims=True) for e in range(experts)]
    top = functools.reduce(jnp.maximum, logits)
    exps = [jnp.exp(l - top) for l in logits]
    total = functools.reduce(jnp.add, exps)
    eid = eid_all[...].reshape(group_rows, LANES)
    own = eid_all[me]
    own_col = own[:, 0:1]
    chosen = functools.reduce(jnp.add, [jnp.where(own_col == e, exps[e], 0.0) for e in range(experts)])
    across = eid.astype(f32).T[0:1, :].astype(jnp.int32)
    row_ids = me * rows + lax.broadcasted_iota(jnp.int32, (rows, group_rows), 0)
    earlier = (across == own_col) & (lax.broadcasted_iota(jnp.int32, (rows, group_rows), 1) < row_ids)
    slot = jnp.sum(jnp.where(earlier, 1.0, 0.0), axis=1, keepdims=True)
    keep_gate = jnp.where(slot < capacity, chosen / total, 0.0)

    for c in first:
        c.wait_recv()
    for c in loads:
        c.wait()
    xs = xall[...].reshape(group_rows, width)
    eid_col = eid[:, 0:1]
    y = jnp.zeros((group_rows, width), f32)
    for e in range(experts):
        u = jnp.dot(xs, win_v[e], preferred_element_type=f32)
        u = jnp.where(eid_col == e, jnp.maximum(u, 0.0), 0.0).astype(jnp.bfloat16)
        y += jnp.dot(u, wout_v[e], preferred_element_type=f32)
    part[...] = y.reshape(n, rows, width)
    second = []
    for k in range(1, n):
        peer = lax.rem(me + k, n)
        second.append(remote(part.at[peer], acc.at[me], s2.at[k - 1], r2.at[k - 1], peer))
        second[-1].start()
    acc[me] = part[me]
    for c in second:
        c.wait_recv()
    y_own = functools.reduce(jnp.add, [acc[p] for p in range(n)]).astype(jnp.bfloat16)
    out[...] = (h2[...].astype(f32) + y_own.astype(f32) * keep_gate).astype(jnp.bfloat16)
    for c in first + second:
        c.wait_send()


def solution(mesh):
    n = mesh.shape['ws']
    row_axes = ('dp', 'ws')
    row_vec = P(row_axes)
    row_mat = P(row_axes, None)
    cache_spec = P(row_axes, None, None, None)
    col_split = P(None, 'ws')
    in_specs = (row_mat, cache_spec, cache_spec, cache_spec, cache_spec, row_vec, row_mat, P(None, None), row_vec,
                P(None), P(None), P(None), col_split, col_split, col_split, col_split, col_split, col_split,
                col_split, P(None, None, 'ws'), P(None, 'ws', None))
    out_specs = (row_mat, cache_spec, cache_spec)

    def decoder_block(hidden, self_k, self_v, cross_k, cross_v, positions, enc_mask, rel_bias, expert_idx,
                      ln_self, ln_cross, ln_ffn, wq_self, wk_self, wv_self, wo_self, wq_cross, wo_cross,
                      w_router, w_in, w_out):
        rows, width = hidden.shape
        heads, head_dim = self_k.shape[1], self_k.shape[3]
        cols = wq_self.shape[1]
        experts, _, units = w_in.shape
        group_rows = rows * n
        capacity = (2 * group_rows + experts - 1) // experts
        bf16, f32, i32 = jnp.bfloat16, jnp.float32, jnp.int32
        pad_heads = 16
        dma = pltpu.SemaphoreType.DMA

        def flat(cache):
            return cache.transpose(0, 1, 3, 2).reshape(rows, heads * head_dim, cache.shape[2])

        sk, sv, ck, cv = (flat(c) for c in (self_k, self_v, cross_k, cross_v))
        pieces = [pltpu.VMEM((rows // PIECES,) + c.shape[1:], bf16) for c in (sk, sv, ck, cv) for _ in range(PIECES)]
        length, src_len = sk.shape[2], ck.shape[2]
        row_bf16, row_f32 = pltpu.VMEM((rows, width), bf16), pltpu.VMEM((rows, width), f32)
        full = pltpu.VMEM((n * cols, width), bf16)
        ln_row = pltpu.VMEM((1, width), f32)
        operands = (hidden, positions, expert_idx, ln_self, ln_cross, rel_bias, w_router.T,
                    wq_self.T, wk_self.T, wv_self.T, wo_self.T, wq_cross.T, wo_cross.T, sk, sv, ck, cv)
        gathered = pl.pallas_call(
            functools.partial(gather_kernel, n, head_dim),
            out_shape=(row_bf16, row_f32, pltpu.VMEM((2, rows, width), f32),
                       pltpu.VMEM((n, rows, LANES), i32), pltpu.VMEM((n, 1, width), f32), full, full, full, *pieces),
            in_specs=[HBM] * len(operands),
            out_specs=(VMEM,) * (8 + len(pieces)),
            scratch_shapes=[row_bf16, pltpu.SMEM((rows,), i32), pltpu.SMEM((rows,), i32), ln_row, ln_row,
                            pltpu.VMEM(rel_bias.shape, f32),
                            pltpu.VMEM((n, rows, width), bf16), pltpu.VMEM((3, cols, width), bf16),
                            pltpu.VMEM((n, 3, rows, cols), bf16), pltpu.VMEM((n, 3, rows, cols), bf16), row_f32,
                            pltpu.VMEM((rows, pad_heads, length), f32), pltpu.VMEM((rows, pad_heads, length), bf16),
                            pltpu.VMEM((rows, pad_heads, length), f32), pltpu.VMEM((rows, pad_heads, LANES), f32), row_f32,
                            dma((13 + 4 * PIECES,)),
                            dma((n - 1, 3)), dma((n - 1, 3)), dma((n - 1,)), dma((n - 1,)), dma((9, 3)), dma((9, 3))],
            compiler_params=pltpu.CompilerParams(collective_id=0, has_side_effects=True, vmem_limit_bytes=7 << 20),
            name='gather')(*(hbm(x) for x in operands))
        h1, qc, kv, eid_all, wr_all, _, _, woc_all, *caches = gathered

        h2, x, new_k, new_v, *_ = pl.pallas_call(
            functools.partial(attn_kernel, head_dim),
            out_shape=(row_bf16, row_bf16, pltpu.HBM(sk.shape, bf16), pltpu.HBM(sv.shape, bf16), *pieces[:2 * PIECES]),
            in_specs=[SMEM] + [VMEM] * 4 + [HBM] + [VMEM] * (1 + len(pieces)),
            out_specs=(VMEM, VMEM, HBM, HBM) + (VMEM,) * (2 * PIECES),
            input_output_aliases={7 + t: 4 + t for t in range(2 * PIECES)},
            scratch_shapes=[ln_row, pltpu.VMEM((rows, pad_heads, src_len), f32), pltpu.VMEM((rows, pad_heads, src_len), bf16),
                            row_f32, pltpu.VMEM((rows // GROUP, width, LANES), bf16),
                            pltpu.VMEM((rows // GROUP, width, LANES), bf16), dma, dma((2, rows))],
            compiler_params=pltpu.CompilerParams(vmem_limit_bytes=7 << 20),
            name='attend')(positions, h1, qc, kv, enc_mask, hbm(ln_ffn), woc_all, *caches)

        hidden_out = pl.pallas_call(
            functools.partial(ffn_kernel, n, capacity),
            out_shape=jax.ShapeDtypeStruct((rows, width), bf16),
            in_specs=[VMEM] * 4 + [HBM] * 2,
            out_specs=VMEM,
            scratch_shapes=[pltpu.VMEM((n, rows, width), bf16), pltpu.VMEM(w_in.shape, bf16), pltpu.VMEM(w_out.shape, bf16),
                            pltpu.VMEM((n, rows, width), f32), pltpu.VMEM((n, rows, width), f32), dma((2,)),
                            dma((n - 1,)), dma((n - 1,)), dma((n - 1,)), dma((n - 1,))],
            compiler_params=pltpu.CompilerParams(collective_id=1, has_side_effects=True, vmem_limit_bytes=20 << 20),
            name='experts')(x, h2, eid_all, wr_all, hbm(w_in), hbm(w_out))

        def unflat(cache):
            return cache.reshape(rows, heads, head_dim, cache.shape[2]).transpose(0, 1, 3, 2)

        return hidden_out, unflat(new_k), unflat(new_v)

    return jax.shard_map(decoder_block, mesh=mesh, in_specs=in_specs, out_specs=out_specs, check_vma=False)
```

```python
import functools
import jax
import jax.numpy as jnp
from jax import lax
from jax.sharding import PartitionSpec as P
from jax.experimental import pallas as pl
from jax.experimental.pallas import tpu as pltpu

EPSILON = 1e-6
NEG_BIG = -1e30
LANES = 128
GROUP = 4
UPDATE = 4
PIECES = 2
NT = (((1,), (1,)), ((), ()))
MESH = pl.DeviceIdType.MESH
VMEM = pl.BlockSpec(memory_space=pltpu.VMEM)
HBM = pl.BlockSpec(memory_space=pltpu.HBM)
SMEM = pl.BlockSpec(memory_space=pltpu.SMEM)


def hbm(x):
    return pltpu.with_memory_space_constraint(x, pltpu.HBM)


def rms_norm(hidden, scale):
    hid_f32 = hidden.astype(jnp.float32)
    inv_rms = lax.rsqrt(jnp.mean(hid_f32 * hid_f32, axis=-1, keepdims=True) + EPSILON)
    return (hid_f32 * inv_rms * scale).astype(jnp.bfloat16)


def entry_barrier(me, n):
    barrier = pltpu.get_barrier_semaphore()
    for k in range(1, n):
        pl.semaphore_signal(barrier, inc=1, device_id={'ws': lax.rem(me + k, n)}, device_id_type=MESH)
    pl.semaphore_wait(barrier, n - 1)


def remote(src, dst, send_sem, recv_sem, peer):
    return pltpu.make_async_remote_copy(src_ref=src, dst_ref=dst, send_sem=send_sem, recv_sem=recv_sem,
                                        device_id={'ws': peer}, device_id_type=MESH)


def reverse_lanes(x):
    size = x.shape[-1]
    lane = lax.broadcasted_iota(jnp.int32, x.shape, 1)
    step = 1
    while step < size:
        x = jnp.where((lane & step) != 0, pltpu.roll(x, step, 1), pltpu.roll(x, size - step, 1))
        step *= 2
    return x


def head_mask_of(heads, width, head_dim):
    lane = lax.broadcasted_iota(jnp.int32, (heads, width), 1)
    return lane // head_dim == lax.broadcasted_iota(jnp.int32, (heads, width), 0)


def project(x, w):
    return lax.dot_general(x, w, NT, preferred_element_type=jnp.float32)


def gather_kernel(n, head_dim, hid, pos, eid, mask, ln_s, ln_c, ln_f, bias, wr, wq, wk, wv, wo, wqc, woc,
                  sk, sv, ck, cv,
                  h2_out, xall, eid_all, wr_all, *rest):
    (kt_out, vt_out), self_kv = rest[:2], rest[2:2 * PIECES + 2]
    (ck_v, cv_v, wo_all, wqc_all, woc_all, hid_v, pos_s, eid_s, mask_v, ln_sv, ln_cv, ln_fv, bias_v, hall, wqkv, snd, qkv,
     q_sc, kv_out, s_sc, p_sc, pn_sc, ctx_sc, loc_sem, send, recv, sw, rw, rp) = rest[2 * PIECES + 2:]
    me = lax.axis_index('ws')
    rows, width = hid.shape
    cols = wq.shape[0]
    heads, length = s_sc.shape[1:]
    src_len = ck.shape[2]
    piece = rows // PIECES
    f32, bf16 = jnp.float32, jnp.bfloat16
    core, xpos, ypos = lax.rem(me, 2), lax.rem(me // 2, 2), me // 4
    pair = me + 1 - 2 * core
    xnb = me + 2 - 4 * xpos
    ynb = me + 4 - 8 * ypos
    diag = me + 2 - 4 * xpos + 4 - 8 * ypos
    peers = [lax.rem(me + k, n) for k in range(1, n)]

    count = []

    def local(src, dst):
        copy = pltpu.make_async_copy(src, dst, loc_sem.at[len(count)])
        copy.start()
        count.append(copy)
        return copy

    small = [local(hid, hid_v), local(wr, wr_all.at[me]), local(eid, eid_s), local(pos, pos_s), local(bias, bias_v),
             local(ln_s, ln_sv.at[0]), local(ln_c, ln_cv.at[0]), local(ln_f, ln_fv.at[0]), local(mask, mask_v)]
    proj = [local(w, wqkv.at[i]) for i, w in enumerate((wq, wk, wv))]
    entry_barrier(me, n)
    for c in small:
        c.wait()
    first = [remote(hid_v, hall.at[me], send.at[0], recv.at[0], p) for p in peers]
    others = pl.ds(0, n - 1)

    def all_of(ref, i):
        return remote(ref.at[others], ref.at[others], send.at[i], recv.at[i], peers[0])

    for c in first:
        c.start()

    fulls = ((wo, wo_all), (wqc, wqc_all), (woc, woc_all))
    half = cols // 2
    to_x, to_y, own_copies = [], [], []

    def own_share(i):
        src, dst = fulls[i]
        at = dst.at[pl.ds(pl.multiple_of(me * cols, cols), cols)]
        to_x.append(remote(src, at, sw.at[i], rw.at[0, i], xnb))
        to_y.append(remote(src, at, sw.at[i], rw.at[1, i], ynb))
        for c in (to_x[-1], to_y[-1], remote(src, at, sw.at[i], rp.at[i], pair)):
            c.start()
        own_copies.append(local(src, at))

    own_share(0)
    load_self = [local(src.at[pl.ds(t * piece, piece)], self_kv[i * PIECES + t])
                 for i, src in enumerate((sk, sv)) for t in range(PIECES)]
    load_cross = [local(ck, ck_v), local(cv.at[pl.ds(0, piece)], cv_v)]
    hall[me] = hid_v[...]
    for r in range(rows):
        eid_all[me, r:r + 1, :] = jnp.full((1, LANES), eid_s[r], jnp.int32)
    for p in peers:
        remote(eid_all.at[me], eid_all.at[me], send.at[1], recv.at[1], p).start()
        remote(wr_all.at[me], wr_all.at[me], send.at[2], recv.at[2], p).start()

    key_pos = lax.broadcasted_iota(jnp.int32, (1, length), 1)
    table = reverse_lanes(jnp.concatenate(
        [bias_v[...], jnp.zeros((heads - bias_v.shape[0], length), f32)], axis=0))

    @pl.loop(0, rows // GROUP)
    def _(i):
        marks = [jnp.full((1, length), pos_s[i * GROUP + j], jnp.int32) for j in range(GROUP)]
        turned, step = [table] * GROUP, 1
        while step < length:
            turned = [jnp.where(((p + 1) & step) != 0, pltpu.roll(t, step, 1), t) for p, t in zip(marks, turned)]
            step *= 2
        for j in range(GROUP):
            s_sc[i * GROUP + j] = jnp.where(key_pos <= marks[j], turned[j], NEG_BIG)

    all_of(hall, 0).wait_recv()
    for c in proj:
        c.wait()
    x_norm = rms_norm(hall[...].reshape(n * rows, width), ln_sv[...])
    for i in range(3):
        snd[:, i] = project(x_norm, wqkv[i]).astype(bf16).reshape(n, rows, cols)
    second = [remote(snd.at[p], qkv.at[me], send.at[3], recv.at[3], p) for p in peers]
    for c in second:
        c.start()
    qkv[me] = snd[me]
    own_share(1)

    def forward(src_dev, lo, size, i, sem, peer):
        dst = fulls[i][1].at[pl.ds(pl.multiple_of(src_dev * cols + lo, half), size)]
        c = remote(dst, dst, sw.at[i], sem, peer)
        c.start()
        return c

    relay_y, relay_x = {}, {}

    def relay(i):
        to_x[i].wait_recv()
        relay_y[i] = forward(xnb, 0, half, i, rw.at[2, i], ynb)
        forward(xnb, 0, cols, i, rp.at[i], pair)
        to_y[i].wait_recv()
        relay_x[i] = forward(ynb, half, half, i, rw.at[3, i], xnb)
        forward(ynb, 0, cols, i, rp.at[i], pair)

    def relay_diag(i):
        relay_y[i].wait_recv()
        forward(diag, 0, half, i, rp.at[i], pair)
        relay_x[i].wait_recv()
        forward(diag, half, half, i, rp.at[i], pair)

    def wait_weight(i):
        theirs = fulls[i][1].at[pl.ds(0, 4 * cols)]
        remote(theirs, theirs, sw.at[i], rp.at[i], pair).wait_recv()
        own_copies[i].wait()

    all_of(qkv, 3).wait_recv()
    for c in load_self:
        c.wait()

    def assemble(i):
        return jnp.concatenate([qkv[p, i].astype(f32) for p in range(n)], axis=1)

    q_sc[...] = assemble(0)
    kv_out[0] = assemble(1)
    kv_out[1] = assemble(2)
    head_mask = head_mask_of(heads, width, head_dim)

    def over_rows(lo, hi, body):
        @pl.loop(0, (hi - lo) // GROUP)
        def _(i):
            for j in range(GROUP):
                body(lo + i * GROUP + j, i * GROUP + j)

    def softmax(s):
        e = jnp.exp(s - jnp.max(s, axis=-1, keepdims=True))
        return (e / jnp.sum(e, axis=-1, keepdims=True)).astype(bf16)

    def store_context(b, o):
        ctx_sc[pl.ds(b, 1), :] = jnp.sum(jnp.where(head_mask, o, 0.0), axis=0, keepdims=True)

    def self_scores(t):
        def body(b, r):
            q = jnp.where(head_mask, q_sc[pl.ds(b, 1), :], 0.0)
            s_new = jnp.sum(q * kv_out[0, pl.ds(b, 1), :], axis=1, keepdims=True)
            s = jnp.dot(q.astype(bf16), self_kv[t][r], preferred_element_type=f32)
            s_sc[b] = jnp.where(key_pos == pos_s[b], s_new, s) + s_sc[b]
        over_rows(t * piece, (t + 1) * piece, body)

    def self_softmax():
        def body(b, r):
            probs = softmax(s_sc[b]).astype(f32)
            hit = key_pos == pos_s[b]
            p_new = jnp.sum(jnp.where(hit, probs, 0.0), axis=1, keepdims=True)
            pn_sc[b] = jnp.broadcast_to(p_new, (heads, LANES))
            p_sc[b] = jnp.where(hit, 0.0, probs).astype(bf16)
        over_rows(0, rows, body)

    def self_context(t):
        def body(b, r):
            o = project(p_sc[b], self_kv[PIECES + t][r])
            store_context(b, o + pn_sc[b, :, 0:1] * kv_out[1, pl.ds(b, 1), :])
        over_rows(t * piece, (t + 1) * piece, body)

    relay(0)
    own_share(2)
    self_scores(0)
    self_scores(1)
    relay(1)
    self_softmax()
    relay_diag(0)
    self_context(0)
    self_context(1)
    relay_diag(1)
    relay(2)

    wait_weight(0)
    h1 = (hid_v[...].astype(f32) + project(ctx_sc[...].astype(bf16), wo_all[...])).astype(bf16)
    wait_weight(1)
    q_sc[...] = project(rms_norm(h1, ln_cv[...]), wqc_all[...]).astype(bf16).astype(f32)
    for c in load_cross:
        c.wait()

    def cross_scores(b, r):
        q = jnp.where(head_mask, q_sc[pl.ds(b, 1), :], 0.0).astype(bf16)
        s_sc[b, :, 0:src_len] = (jnp.dot(q, ck_v[b], preferred_element_type=f32)
                                 + jnp.where(mask_v[pl.ds(b, 1), :] == 1, 0.0, NEG_BIG))

    def cross_softmax(b, r):
        p_sc[b, :, 0:src_len] = softmax(s_sc[b, :, 0:src_len])

    def cross_context(b, r):
        store_context(b, project(p_sc[b, :, 0:src_len], cv_v[b]))

    def cross_context_late(b, r):
        store_context(b, project(p_sc[b, :, 0:src_len], ck_v[r]))

    over_rows(0, piece, cross_scores)
    relay_diag(2)
    load_late = local(cv.at[pl.ds(piece, piece)], ck_v.at[pl.ds(0, piece)])
    over_rows(piece, rows, cross_scores)
    over_rows(0, rows, cross_softmax)
    over_rows(0, piece, cross_context)
    load_late.wait()
    over_rows(piece, rows, cross_context_late)
    wait_weight(2)
    h2 = (h1.astype(f32) + project(ctx_sc[...].astype(bf16), woc_all[...])).astype(bf16)
    xall[me] = rms_norm(h2, ln_fv[...])
    h2_out[...] = h2
    third = [remote(xall.at[me], xall.at[me], send.at[4], recv.at[4], p) for p in peers]
    for c in third:
        c.start()
    for i, ref in enumerate((kt_out, vt_out)):
        cols_t = jnp.concatenate([kv_out[i], jnp.zeros((LANES - rows, width), f32)], axis=0).T
        for g in range(rows // UPDATE):
            shifted = cols_t if g == 0 else pltpu.roll(cols_t, LANES - g * UPDATE, 1)
            ref[g] = shifted.astype(bf16)
    for i, ref in ((1, eid_all), (2, wr_all), (4, xall)):
        all_of(ref, i).wait_recv()
    for i, ref in enumerate((hall, eid_all, wr_all, snd, xall)):
        all_of(ref, i).wait_send()
    for i in range(3):
        moved = fulls[i][1].at[pl.ds(0, 7 * cols)]
        remote(moved, moved, sw.at[i], rp.at[i], pair).wait_send()


def update_kernel(n, capacity, pos, kt, vt, xall, eid_all, wr_all, win, wout, *rest):
    (part, gate, nk, nv), self_kv, (hidden_sc, out_sem) = (
        rest[2 * PIECES:2 * PIECES + 4], rest[2 * PIECES + 4:-2], rest[-2:])
    me = lax.axis_index('ws')
    _, rows, width = xall.shape
    experts, _, units = win.shape
    group_rows = n * rows
    piece = rows // PIECES
    f32 = jnp.float32
    lane = lax.broadcasted_iota(jnp.int32, (1, LANES), 1)

    for t in range(PIECES):
        keys, vals = self_kv[t], self_kv[PIECES + t]

        @pl.loop(0, piece // UPDATE)
        def _(i):
            g = t * (piece // UPDATE) + i
            for j in range(UPDATE):
                r = i * UPDATE + j
                b = t * piece + r
                p = pos[b]
                win_at = pl.ds(pl.multiple_of((p // LANES) * LANES, LANES), LANES)
                hit = lane == p % LANES
                for cache, new in ((keys, kt), (vals, vt)):
                    cache[r, :, win_at] = jnp.where(hit, new[g, :, j:j + 1], cache[r, :, win_at])
            for j in range(UPDATE):
                r = i * UPDATE + j
                b = t * piece + r
                pltpu.make_async_copy(keys.at[r], nk.at[b], out_sem.at[0]).start()
                pltpu.make_async_copy(vals.at[r], nv.at[b], out_sem.at[1]).start()

    eid = eid_all[...].reshape(group_rows, LANES)
    eid_col = eid[:, 0:1]
    xs = xall[...].reshape(group_rows, width)
    for e in range(experts):
        u = jnp.dot(xs, win[e], preferred_element_type=f32)
        hidden_sc[:, e * units:(e + 1) * units] = jnp.where(eid_col == e, jnp.maximum(u, 0.0), 0.0).astype(jnp.bfloat16)
    y = jnp.dot(hidden_sc[...], wout[...].reshape(experts * units, width), preferred_element_type=f32)
    part[...] = y.reshape(n, rows, width)

    x_own = xall[me].astype(f32)
    logits = [jnp.sum(x_own * wr_all[e], axis=-1, keepdims=True) for e in range(experts)]
    top = functools.reduce(jnp.maximum, logits)
    exps = [jnp.exp(l - top) for l in logits]
    total = functools.reduce(jnp.add, exps)
    own_col = eid_all[me][:, 0:1]
    chosen = functools.reduce(jnp.add, [jnp.where(own_col == e, exps[e], 0.0) for e in range(experts)])
    across = eid.astype(f32).T[0:1, :].astype(jnp.int32)
    row_ids = me * rows + lax.broadcasted_iota(jnp.int32, (rows, group_rows), 0)
    earlier = (across == own_col) & (lax.broadcasted_iota(jnp.int32, (rows, group_rows), 1) < row_ids)
    slot = jnp.sum(jnp.where(earlier, 1.0, 0.0), axis=1, keepdims=True)
    gate[...] = jnp.broadcast_to(jnp.where(slot < capacity, chosen / total, 0.0), gate.shape)

    for i, ref in enumerate((nk, nv)):
        pltpu.make_async_copy(ref, ref, out_sem.at[i]).wait()


def reduce_kernel(n, part, gate, h2, out, acc, send, recv):
    me = lax.axis_index('ws')
    f32 = jnp.float32
    entry_barrier(me, n)
    for k in range(1, n):
        peer = lax.rem(me + k, n)
        remote(part.at[peer], acc.at[me], send, recv, peer).start()
    acc[me] = part[me]
    others = pl.ds(0, n - 1)
    copies = remote(part.at[others], acc.at[others], send, recv, lax.rem(me + 1, n))
    copies.wait_recv()
    y_own = functools.reduce(jnp.add, [acc[p] for p in range(n)]).astype(jnp.bfloat16)
    out[...] = (h2[...].astype(f32) + y_own.astype(f32) * gate[:, 0:1]).astype(jnp.bfloat16)
    copies.wait_send()


def solution(mesh):
    n = mesh.shape['ws']
    row_axes = ('dp', 'ws')
    row_vec = P(row_axes)
    row_mat = P(row_axes, None)
    cache_spec = P(row_axes, None, None, None)
    col_split = P(None, 'ws')
    in_specs = (row_mat, cache_spec, cache_spec, cache_spec, cache_spec, row_vec, row_mat, P(None, None), row_vec,
                P(None), P(None), P(None), col_split, col_split, col_split, col_split, col_split, col_split,
                col_split, P(None, None, 'ws'), P(None, 'ws', None))
    out_specs = (row_mat, cache_spec, cache_spec)

    def decoder_block(hidden, self_k, self_v, cross_k, cross_v, positions, enc_mask, rel_bias, expert_idx,
                      ln_self, ln_cross, ln_ffn, wq_self, wk_self, wv_self, wo_self, wq_cross, wo_cross,
                      w_router, w_in, w_out):
        rows, width = hidden.shape
        heads, head_dim = self_k.shape[1], self_k.shape[3]
        cols = wq_self.shape[1]
        experts, _, units = w_in.shape
        group_rows = rows * n
        capacity = (2 * group_rows + experts - 1) // experts
        bf16, f32, i32 = jnp.bfloat16, jnp.float32, jnp.int32
        pad_heads = 16
        dma = pltpu.SemaphoreType.DMA

        def flat(cache):
            return cache.transpose(0, 1, 3, 2).reshape(rows, heads * head_dim, cache.shape[2])

        sk, sv, ck, cv = (flat(c) for c in (self_k, self_v, cross_k, cross_v))
        pieces = [pltpu.VMEM((rows // PIECES,) + c.shape[1:], bf16) for c in (sk, sv) for _ in range(PIECES)]
        length, src_len = sk.shape[2], ck.shape[2]
        row_bf16, row_f32 = pltpu.VMEM((rows, width), bf16), pltpu.VMEM((rows, width), f32)
        full = pltpu.VMEM((n * cols, width), bf16)
        columns = pltpu.VMEM((rows // UPDATE, width, LANES), bf16)
        ln_row = pltpu.VMEM((1, width), f32)
        index = pltpu.SMEM((rows,), i32)
        exchange = pltpu.VMEM((n, 3, rows, cols), bf16)
        operands = (hidden, positions, expert_idx, enc_mask, ln_self, ln_cross, ln_ffn, rel_bias, w_router.T,
                    wq_self.T, wk_self.T, wv_self.T, wo_self.T, wq_cross.T, wo_cross.T, sk, sv, ck, cv)
        gathered = pl.pallas_call(
            functools.partial(gather_kernel, n, head_dim),
            out_shape=(row_bf16, pltpu.VMEM((n, rows, width), bf16),
                       pltpu.VMEM((n, rows, LANES), i32), pltpu.VMEM((n, 1, width), f32),
                       columns, columns, *pieces),
            in_specs=[HBM] * len(operands),
            out_specs=(VMEM,) * (6 + len(pieces)),
            scratch_shapes=[pltpu.VMEM(ck.shape, bf16), pltpu.VMEM((rows // PIECES,) + cv.shape[1:], bf16), full, full, full,
                            row_bf16, index, index, pltpu.VMEM(enc_mask.shape, i32), ln_row, ln_row, ln_row,
                            pltpu.VMEM(rel_bias.shape, f32), pltpu.VMEM((n, rows, width), bf16),
                            pltpu.VMEM((3, cols, width), bf16), exchange, exchange, row_f32, pltpu.VMEM((2, rows, width), f32),
                            pltpu.VMEM((rows, pad_heads, length), f32), pltpu.VMEM((rows, pad_heads, length), bf16),
                            pltpu.VMEM((rows, pad_heads, LANES), f32), row_f32,
                            dma((20 + 2 * PIECES,)), dma((5,)), dma((5,)), dma((3,)), dma((4, 3)), dma((3,))],
            compiler_params=pltpu.CompilerParams(collective_id=0, has_side_effects=True, vmem_limit_bytes=40 << 19),
            name='gather')(*(hbm(x) for x in operands))
        h2, xall, eid_all, wr_all, kt, vt, *caches = gathered

        part, gate, new_k, new_v, *_ = pl.pallas_call(
            functools.partial(update_kernel, n, capacity),
            out_shape=(pltpu.VMEM((n, rows, width), f32), pltpu.VMEM((rows, LANES), f32),
                       pltpu.HBM(sk.shape, bf16), pltpu.HBM(sv.shape, bf16), *pieces),
            in_specs=[SMEM] + [VMEM] * (7 + len(pieces)),
            out_specs=(VMEM, VMEM, HBM, HBM) + (VMEM,) * len(pieces),
            input_output_aliases={8 + t: 4 + t for t in range(len(pieces))},
            scratch_shapes=[pltpu.VMEM((group_rows, experts * units), bf16), dma((2,))],
            compiler_params=pltpu.CompilerParams(vmem_limit_bytes=10 << 19),
            name='attend')(positions, kt, vt, xall, eid_all, wr_all, w_in, w_out, *caches)

        hidden_out = pl.pallas_call(
            functools.partial(reduce_kernel, n),
            out_shape=jax.ShapeDtypeStruct((rows, width), bf16),
            in_specs=[VMEM] * 3,
            out_specs=VMEM,
            scratch_shapes=[pltpu.VMEM((n, rows, width), f32), dma, dma],
            compiler_params=pltpu.CompilerParams(collective_id=1, has_side_effects=True, vmem_limit_bytes=4 << 20),
            name='experts')(part, gate, h2)

        def unflat(cache):
            return cache.reshape(rows, heads, head_dim, cache.shape[2]).transpose(0, 1, 3, 2)

        return hidden_out, unflat(new_k), unflat(new_v)

    return jax.shard_map(decoder_block, mesh=mesh, in_specs=in_specs, out_specs=out_specs, check_vma=False)
```

```python
import functools
import jax
import jax.numpy as jnp
from jax import lax
from jax.sharding import PartitionSpec as P
from jax.experimental import pallas as pl
from jax.experimental.pallas import tpu as pltpu

EPSILON = 1e-6
NEG_BIG = -1e30
LANES = 128
GROUP = 4
UPDATE = 4
PIECES = 2
NT = (((1,), (1,)), ((), ()))
MESH = pl.DeviceIdType.MESH
VMEM = pl.BlockSpec(memory_space=pltpu.VMEM)
HBM = pl.BlockSpec(memory_space=pltpu.HBM)
SMEM = pl.BlockSpec(memory_space=pltpu.SMEM)


def hbm(x):
    return pltpu.with_memory_space_constraint(x, pltpu.HBM)


def rms_norm(hidden, scale):
    hid_f32 = hidden.astype(jnp.float32)
    inv_rms = lax.rsqrt(jnp.mean(hid_f32 * hid_f32, axis=-1, keepdims=True) + EPSILON)
    return (hid_f32 * inv_rms * scale).astype(jnp.bfloat16)


def entry_barrier(me, n):
    barrier = pltpu.get_barrier_semaphore()
    for k in range(1, n):
        pl.semaphore_signal(barrier, inc=1, device_id={'ws': lax.rem(me + k, n)}, device_id_type=MESH)
    pl.semaphore_wait(barrier, n - 1)


def neighbours(me):
    core, xpos, ypos = lax.rem(me, 2), lax.rem(me // 2, 2), me // 4
    other, across_x, across_y = 1 - 2 * core, 2 - 4 * xpos, 4 - 8 * ypos
    xnb, ynb, diag = me + across_x, me + across_y, me + across_x + across_y
    far_first = [diag, diag + other, xnb, ynb, xnb + other, ynb + other, me + other]
    return me + other, xnb, ynb, diag, far_first


def remote(src, dst, send_sem, recv_sem, peer):
    return pltpu.make_async_remote_copy(src_ref=src, dst_ref=dst, send_sem=send_sem, recv_sem=recv_sem,
                                        device_id={'ws': peer}, device_id_type=MESH)


def reverse_lanes(x):
    size = x.shape[-1]
    lane = lax.broadcasted_iota(jnp.int32, x.shape, 1)
    step = 1
    while step < size:
        x = jnp.where((lane & step) != 0, pltpu.roll(x, step, 1), pltpu.roll(x, size - step, 1))
        step *= 2
    return x


def head_mask_of(heads, width, head_dim):
    lane = lax.broadcasted_iota(jnp.int32, (heads, width), 1)
    return lane // head_dim == lax.broadcasted_iota(jnp.int32, (heads, width), 0)


def project(x, w):
    return lax.dot_general(x, w, NT, preferred_element_type=jnp.float32)


def gather_kernel(n, head_dim, hid, pos, eid, mask, ln_s, ln_c, ln_f, bias, wr, wq, wk, wv, wo, wqc, woc,
                  sk, sv, ck, cv,
                  h2_out, xall, eid_all, wr_all, *rest):
    (kt_out, vt_out), self_kv = rest[:2], rest[2:2 * PIECES + 2]
    (ck_v, cv_v, wo_all, wqc_all, woc_all, hid_v, pos_s, eid_s, mask_v, ln_sv, ln_cv, ln_fv, bias_v, hall, wqkv, snd, qkv,
     q_sc, kv_out, s_sc, p_sc, pn_sc, ctx_sc, loc_sem, send, recv, sw, rw, rp) = rest[2 * PIECES + 2:]
    me = lax.axis_index('ws')
    rows, width = hid.shape
    cols = wq.shape[0]
    heads, length = s_sc.shape[1:]
    src_len = ck.shape[2]
    piece = rows // PIECES
    f32, bf16 = jnp.float32, jnp.bfloat16
    pair, xnb, ynb, diag, peers = neighbours(me)

    count = []

    def local(src, dst):
        copy = pltpu.make_async_copy(src, dst, loc_sem.at[len(count)])
        copy.start()
        count.append(copy)
        return copy

    small = [local(hid, hid_v), local(wr, wr_all.at[me]), local(eid, eid_s), local(pos, pos_s), local(bias, bias_v),
             local(ln_s, ln_sv.at[0]), local(ln_c, ln_cv.at[0]), local(ln_f, ln_fv.at[0]), local(mask, mask_v)]
    proj = [local(w, wqkv.at[i]) for i, w in enumerate((wq, wk, wv))]
    entry_barrier(me, n)
    for c in small:
        c.wait()
    first = [remote(hid_v, hall.at[me], send.at[0], recv.at[0], p) for p in peers]
    others = pl.ds(0, n - 1)

    def all_of(ref, i):
        return remote(ref.at[others], ref.at[others], send.at[i], recv.at[i], peers[0])

    for c in first:
        c.start()

    fulls = ((wo, wo_all), (wqc, wqc_all), (woc, woc_all))
    half = cols // 2
    to_x, to_y, own_copies = [], [], []

    def own_share(i):
        src, dst = fulls[i]
        at = dst.at[pl.ds(pl.multiple_of(me * cols, cols), cols)]
        to_x.append(remote(src, at, sw.at[i], rw.at[0, i], xnb))
        to_y.append(remote(src, at, sw.at[i], rw.at[1, i], ynb))
        for c in (to_x[-1], to_y[-1], remote(src, at, sw.at[i], rp.at[i], pair)):
            c.start()
        own_copies.append(local(src, at))

    load_self = [local(src.at[pl.ds(t * piece, piece)], self_kv[i * PIECES + t])
                 for i, src in enumerate((sk, sv)) for t in range(PIECES)]
    load_cross = [local(ck, ck_v), local(cv.at[pl.ds(0, piece)], cv_v)]
    hall[me] = hid_v[...]
    for r in range(rows):
        eid_all[me, r:r + 1, :] = jnp.full((1, LANES), eid_s[r], jnp.int32)

    own_share(0)
    key_pos = lax.broadcasted_iota(jnp.int32, (1, length), 1)
    table = reverse_lanes(jnp.concatenate(
        [bias_v[...], jnp.zeros((heads - bias_v.shape[0], length), f32)], axis=0))

    @pl.loop(0, rows // GROUP)
    def _(i):
        marks = [jnp.full((1, length), pos_s[i * GROUP + j], jnp.int32) for j in range(GROUP)]
        turned, step = [table] * GROUP, 1
        while step < length:
            turned = [jnp.where(((p + 1) & step) != 0, pltpu.roll(t, step, 1), t) for p, t in zip(marks, turned)]
            step *= 2
        for j in range(GROUP):
            s_sc[i * GROUP + j] = jnp.where(key_pos <= marks[j], turned[j], NEG_BIG)

    all_of(hall, 0).wait_recv()
    for c in proj:
        c.wait()
    x_norm = rms_norm(hall[...].reshape(n * rows, width), ln_sv[...])
    for i in range(3):
        snd[:, i] = project(x_norm, wqkv[i]).astype(bf16).reshape(n, rows, cols)
    second = [remote(snd.at[p], qkv.at[me], send.at[3], recv.at[3], p) for p in peers]
    for c in second:
        c.start()
    qkv[me] = snd[me]
    own_share(1)

    def forward(src_dev, lo, size, i, sem, peer):
        dst = fulls[i][1].at[pl.ds(pl.multiple_of(src_dev * cols + lo, half), size)]
        c = remote(dst, dst, sw.at[i], sem, peer)
        c.start()
        return c

    relay_y, relay_x = {}, {}

    def relay(i):
        to_x[i].wait_recv()
        relay_y[i] = forward(xnb, 0, half, i, rw.at[2, i], ynb)
        forward(xnb, 0, cols, i, rp.at[i], pair)
        to_y[i].wait_recv()
        relay_x[i] = forward(ynb, half, half, i, rw.at[3, i], xnb)
        forward(ynb, 0, cols, i, rp.at[i], pair)

    def relay_diag(i):
        relay_y[i].wait_recv()
        forward(diag, 0, half, i, rp.at[i], pair)
        relay_x[i].wait_recv()
        forward(diag, half, half, i, rp.at[i], pair)

    def wait_weight(i):
        theirs = fulls[i][1].at[pl.ds(0, 4 * cols)]
        remote(theirs, theirs, sw.at[i], rp.at[i], pair).wait_recv()
        own_copies[i].wait()

    all_of(qkv, 3).wait_recv()
    for c in load_self[:PIECES]:
        c.wait()

    def assemble(i):
        return jnp.concatenate([qkv[p, i].astype(f32) for p in range(n)], axis=1)

    q_sc[...] = assemble(0)
    kv_out[0] = assemble(1)
    kv_out[1] = assemble(2)
    head_mask = head_mask_of(heads, width, head_dim)

    def over_rows(lo, hi, body):
        @pl.loop(0, (hi - lo) // GROUP)
        def _(i):
            for j in range(GROUP):
                body(lo + i * GROUP + j, i * GROUP + j)

    def softmax(s):
        e = jnp.exp(s - jnp.max(s, axis=-1, keepdims=True))
        return (e / jnp.sum(e, axis=-1, keepdims=True)).astype(bf16)

    def store_context(b, o):
        ctx_sc[pl.ds(b, 1), :] = jnp.sum(jnp.where(head_mask, o, 0.0), axis=0, keepdims=True)

    def self_scores(t):
        def body(b, r):
            q = jnp.where(head_mask, q_sc[pl.ds(b, 1), :], 0.0)
            s_new = jnp.sum(q * kv_out[0, pl.ds(b, 1), :], axis=1, keepdims=True)
            s = jnp.dot(q.astype(bf16), self_kv[t][r], preferred_element_type=f32)
            s_sc[b] = jnp.where(key_pos == pos_s[b], s_new, s) + s_sc[b]
        over_rows(t * piece, (t + 1) * piece, body)

    def self_softmax():
        def body(b, r):
            probs = softmax(s_sc[b]).astype(f32)
            hit = key_pos == pos_s[b]
            p_new = jnp.sum(jnp.where(hit, probs, 0.0), axis=1, keepdims=True)
            pn_sc[b] = jnp.broadcast_to(p_new, (heads, LANES))
            p_sc[b] = jnp.where(hit, 0.0, probs).astype(bf16)
        over_rows(0, rows, body)

    def self_context(t):
        def body(b, r):
            o = project(p_sc[b], self_kv[PIECES + t][r])
            store_context(b, o + pn_sc[b, :, 0:1] * kv_out[1, pl.ds(b, 1), :])
        over_rows(t * piece, (t + 1) * piece, body)

    relay(0)
    own_share(2)
    self_scores(0)
    self_scores(1)
    relay(1)
    self_softmax()
    relay_diag(0)
    for c in load_self[PIECES:]:
        c.wait()
    self_context(0)
    self_context(1)
    relay_diag(1)
    relay(2)
    for p in peers:
        remote(eid_all.at[me], eid_all.at[me], send.at[1], recv.at[1], p).start()
        remote(wr_all.at[me], wr_all.at[me], send.at[2], recv.at[2], p).start()

    wait_weight(0)
    h1 = (hid_v[...].astype(f32) + project(ctx_sc[...].astype(bf16), wo_all[...])).astype(bf16)
    wait_weight(1)
    q_sc[...] = project(rms_norm(h1, ln_cv[...]), wqc_all[...]).astype(bf16).astype(f32)
    for c in load_cross:
        c.wait()

    def cross_scores(b, r):
        q = jnp.where(head_mask, q_sc[pl.ds(b, 1), :], 0.0).astype(bf16)
        s_sc[b, :, 0:src_len] = (jnp.dot(q, ck_v[b], preferred_element_type=f32)
                                 + jnp.where(mask_v[pl.ds(b, 1), :] == 1, 0.0, NEG_BIG))

    def cross_softmax(b, r):
        p_sc[b, :, 0:src_len] = softmax(s_sc[b, :, 0:src_len])

    def cross_context(b, r):
        store_context(b, project(p_sc[b, :, 0:src_len], cv_v[b]))

    def cross_context_late(b, r):
        store_context(b, project(p_sc[b, :, 0:src_len], ck_v[r]))

    over_rows(0, piece, cross_scores)
    load_late = local(cv.at[pl.ds(piece, piece)], ck_v.at[pl.ds(0, piece)])
    over_rows(piece, rows, cross_scores)
    over_rows(0, rows, cross_softmax)
    relay_diag(2)
    over_rows(0, piece, cross_context)
    load_late.wait()
    over_rows(piece, rows, cross_context_late)
    wait_weight(2)
    h2 = (h1.astype(f32) + project(ctx_sc[...].astype(bf16), woc_all[...])).astype(bf16)
    xall[me] = rms_norm(h2, ln_fv[...])
    h2_out[...] = h2
    third = [remote(xall.at[me], xall.at[me], send.at[4], recv.at[4], p) for p in peers]
    for c in third:
        c.start()
    for i, ref in enumerate((kt_out, vt_out)):
        cols_t = jnp.concatenate([kv_out[i], jnp.zeros((LANES - rows, width), f32)], axis=0).T
        for g in range(rows // UPDATE):
            shifted = cols_t if g == 0 else pltpu.roll(cols_t, LANES - g * UPDATE, 1)
            ref[g] = shifted.astype(bf16)
    for i, ref in ((1, eid_all), (2, wr_all), (4, xall)):
        all_of(ref, i).wait_recv()
    for i, ref in enumerate((hall, eid_all, wr_all, snd, xall)):
        all_of(ref, i).wait_send()
    for i in range(3):
        moved = fulls[i][1].at[pl.ds(0, 7 * cols)]
        remote(moved, moved, sw.at[i], rp.at[i], pair).wait_send()


def update_kernel(n, capacity, pos, kt, vt, xall, eid_all, wr_all, win, wout, *rest):
    (part, gate, nk, nv), self_kv, (hidden_sc, out_sem) = (
        rest[2 * PIECES:2 * PIECES + 4], rest[2 * PIECES + 4:-2], rest[-2:])
    me = lax.axis_index('ws')
    _, rows, width = xall.shape
    experts, _, units = win.shape
    group_rows = n * rows
    piece = rows // PIECES
    f32 = jnp.float32
    lane = lax.broadcasted_iota(jnp.int32, (1, LANES), 1)

    for t in range(PIECES):
        keys, vals = self_kv[t], self_kv[PIECES + t]

        @pl.loop(0, piece // UPDATE)
        def _(i):
            g = t * (piece // UPDATE) + i
            def write(j):
                r = i * UPDATE + j
                b = t * piece + r
                pltpu.make_async_copy(keys.at[r], nk.at[b], out_sem.at[0]).start()
                pltpu.make_async_copy(vals.at[r], nv.at[b], out_sem.at[1]).start()

            for j in range(UPDATE):
                r = i * UPDATE + j
                b = t * piece + r
                p = pos[b]
                win_at = pl.ds(pl.multiple_of((p // LANES) * LANES, LANES), LANES)
                hit = lane == p % LANES
                for cache, new in ((keys, kt), (vals, vt)):
                    cache[r, :, win_at] = jnp.where(hit, new[g, :, j:j + 1], cache[r, :, win_at])
                if j:
                    write(j - 1)
            write(UPDATE - 1)

    eid = eid_all[...].reshape(group_rows, LANES)
    eid_col = eid[:, 0:1]
    xs = xall[...].reshape(group_rows, width)
    for e in range(experts):
        u = jnp.dot(xs, win[e], preferred_element_type=f32)
        hidden_sc[:, e * units:(e + 1) * units] = jnp.where(eid_col == e, jnp.maximum(u, 0.0), 0.0).astype(jnp.bfloat16)
    y = jnp.dot(hidden_sc[...], wout[...].reshape(experts * units, width), preferred_element_type=f32)
    part[...] = y.reshape(n, rows, width)

    x_own = xall[me].astype(f32)
    logits = [jnp.sum(x_own * wr_all[e], axis=-1, keepdims=True) for e in range(experts)]
    top = functools.reduce(jnp.maximum, logits)
    exps = [jnp.exp(l - top) for l in logits]
    total = functools.reduce(jnp.add, exps)
    own_col = eid_all[me][:, 0:1]
    chosen = functools.reduce(jnp.add, [jnp.where(own_col == e, exps[e], 0.0) for e in range(experts)])
    across = eid.astype(f32).T[0:1, :].astype(jnp.int32)
    row_ids = me * rows + lax.broadcasted_iota(jnp.int32, (rows, group_rows), 0)
    earlier = (across == own_col) & (lax.broadcasted_iota(jnp.int32, (rows, group_rows), 1) < row_ids)
    slot = jnp.sum(jnp.where(earlier, 1.0, 0.0), axis=1, keepdims=True)
    gate[...] = jnp.broadcast_to(jnp.where(slot < capacity, chosen / total, 0.0), gate.shape)

    for i, ref in enumerate((nk, nv)):
        pltpu.make_async_copy(ref, ref, out_sem.at[i]).wait()


def reduce_kernel(n, part, gate, h2, out, acc, send, recv):
    me = lax.axis_index('ws')
    f32 = jnp.float32
    entry_barrier(me, n)
    for peer in neighbours(me)[-1]:
        remote(part.at[peer], acc.at[me], send, recv, peer).start()
    acc[me] = part[me]
    others = pl.ds(0, n - 1)
    copies = remote(part.at[others], acc.at[others], send, recv, lax.rem(me + 1, n))
    copies.wait_recv()
    y_own = functools.reduce(jnp.add, [acc[p] for p in range(n)]).astype(jnp.bfloat16)
    out[...] = (h2[...].astype(f32) + y_own.astype(f32) * gate[:, 0:1]).astype(jnp.bfloat16)
    copies.wait_send()


def solution(mesh):
    n = mesh.shape['ws']
    row_axes = ('dp', 'ws')
    row_vec = P(row_axes)
    row_mat = P(row_axes, None)
    cache_spec = P(row_axes, None, None, None)
    col_split = P(None, 'ws')
    in_specs = (row_mat, cache_spec, cache_spec, cache_spec, cache_spec, row_vec, row_mat, P(None, None), row_vec,
                P(None), P(None), P(None), col_split, col_split, col_split, col_split, col_split, col_split,
                col_split, P(None, None, 'ws'), P(None, 'ws', None))
    out_specs = (row_mat, cache_spec, cache_spec)

    def decoder_block(hidden, self_k, self_v, cross_k, cross_v, positions, enc_mask, rel_bias, expert_idx,
                      ln_self, ln_cross, ln_ffn, wq_self, wk_self, wv_self, wo_self, wq_cross, wo_cross,
                      w_router, w_in, w_out):
        rows, width = hidden.shape
        heads, head_dim = self_k.shape[1], self_k.shape[3]
        cols = wq_self.shape[1]
        experts, _, units = w_in.shape
        group_rows = rows * n
        capacity = (2 * group_rows + experts - 1) // experts
        bf16, f32, i32 = jnp.bfloat16, jnp.float32, jnp.int32
        pad_heads = 16
        dma = pltpu.SemaphoreType.DMA

        def flat(cache):
            return cache.transpose(0, 1, 3, 2).reshape(rows, heads * head_dim, cache.shape[2])

        sk, sv, ck, cv = (flat(c) for c in (self_k, self_v, cross_k, cross_v))
        pieces = [pltpu.VMEM((rows // PIECES,) + c.shape[1:], bf16) for c in (sk, sv) for _ in range(PIECES)]
        length, src_len = sk.shape[2], ck.shape[2]
        row_bf16, row_f32 = pltpu.VMEM((rows, width), bf16), pltpu.VMEM((rows, width), f32)
        full = pltpu.VMEM((n * cols, width), bf16)
        columns = pltpu.VMEM((rows // UPDATE, width, LANES), bf16)
        ln_row = pltpu.VMEM((1, width), f32)
        index = pltpu.SMEM((rows,), i32)
        exchange = pltpu.VMEM((n, 3, rows, cols), bf16)
        operands = (hidden, positions, expert_idx, enc_mask, ln_self, ln_cross, ln_ffn, rel_bias, w_router.T,
                    wq_self.T, wk_self.T, wv_self.T, wo_self.T, wq_cross.T, wo_cross.T, sk, sv, ck, cv)
        gathered = pl.pallas_call(
            functools.partial(gather_kernel, n, head_dim),
            out_shape=(row_bf16, pltpu.VMEM((n, rows, width), bf16),
                       pltpu.VMEM((n, rows, LANES), i32), pltpu.VMEM((n, 1, width), f32),
                       columns, columns, *pieces),
            in_specs=[HBM] * len(operands),
            out_specs=(VMEM,) * (6 + len(pieces)),
            scratch_shapes=[pltpu.VMEM(ck.shape, bf16), pltpu.VMEM((rows // PIECES,) + cv.shape[1:], bf16), full, full, full,
                            row_bf16, index, index, pltpu.VMEM(enc_mask.shape, i32), ln_row, ln_row, ln_row,
                            pltpu.VMEM(rel_bias.shape, f32), pltpu.VMEM((n, rows, width), bf16),
                            pltpu.VMEM((3, cols, width), bf16), exchange, exchange, row_f32, pltpu.VMEM((2, rows, width), f32),
                            pltpu.VMEM((rows, pad_heads, length), f32), pltpu.VMEM((rows, pad_heads, length), bf16),
                            pltpu.VMEM((rows, pad_heads, LANES), f32), row_f32,
                            dma((20 + 2 * PIECES,)), dma((5,)), dma((5,)), dma((3,)), dma((4, 3)), dma((3,))],
            compiler_params=pltpu.CompilerParams(collective_id=0, has_side_effects=True, vmem_limit_bytes=40 << 19),
            name='gather')(*(hbm(x) for x in operands))
        h2, xall, eid_all, wr_all, kt, vt, *caches = gathered

        part, gate, new_k, new_v, *_ = pl.pallas_call(
            functools.partial(update_kernel, n, capacity),
            out_shape=(pltpu.VMEM((n, rows, width), f32), pltpu.VMEM((rows, LANES), f32),
                       pltpu.HBM(sk.shape, bf16), pltpu.HBM(sv.shape, bf16), *pieces),
            in_specs=[SMEM] + [VMEM] * (7 + len(pieces)),
            out_specs=(VMEM, VMEM, HBM, HBM) + (VMEM,) * len(pieces),
            input_output_aliases={8 + t: 4 + t for t in range(len(pieces))},
            scratch_shapes=[pltpu.VMEM((group_rows, experts * units), bf16), dma((2,))],
            compiler_params=pltpu.CompilerParams(vmem_limit_bytes=10 << 19),
            name='attend')(positions, kt, vt, xall, eid_all, wr_all, w_in, w_out, *caches)

        hidden_out = pl.pallas_call(
            functools.partial(reduce_kernel, n),
            out_shape=jax.ShapeDtypeStruct((rows, width), bf16),
            in_specs=[VMEM] * 3,
            out_specs=VMEM,
            scratch_shapes=[pltpu.VMEM((n, rows, width), f32), dma, dma],
            compiler_params=pltpu.CompilerParams(collective_id=1, has_side_effects=True, vmem_limit_bytes=4 << 20),
            name='experts')(part, gate, h2)

        def unflat(cache):
            return cache.reshape(rows, heads, head_dim, cache.shape[2]).transpose(0, 1, 3, 2)

        return hidden_out, unflat(new_k), unflat(new_v)

    return jax.shard_map(decoder_block, mesh=mesh, in_specs=in_specs, out_specs=out_specs, check_vma=False)
```

```python
import functools
import jax
import jax.numpy as jnp
from jax import lax
from jax.sharding import PartitionSpec as P
from jax.experimental import pallas as pl
from jax.experimental.pallas import tpu as pltpu

EPSILON = 1e-6
NEG_BIG = -1e30
LANES = 128
GROUP = 4
SOFTMAX_GROUP = 8
BIAS_GROUP = 4
MXU_HEADS = 6
UPDATE = 4
READY = 4
PIECES = 2
NT = (((1,), (1,)), ((), ()))
MESH = pl.DeviceIdType.MESH
VMEM = pl.BlockSpec(memory_space=pltpu.VMEM)
HBM = pl.BlockSpec(memory_space=pltpu.HBM)
SMEM = pl.BlockSpec(memory_space=pltpu.SMEM)


def hbm(x):
    return pltpu.with_memory_space_constraint(x, pltpu.HBM)


def rms_norm(hidden, scale):
    hid_f32 = hidden.astype(jnp.float32)
    inv_rms = lax.rsqrt(jnp.mean(hid_f32 * hid_f32, axis=-1, keepdims=True) + EPSILON)
    return (hid_f32 * inv_rms * scale).astype(jnp.bfloat16)


def entry_barrier(me, n):
    barrier = pltpu.get_barrier_semaphore()
    for k in range(1, n):
        pl.semaphore_signal(barrier, inc=1, device_id={'ws': lax.rem(me + k, n)}, device_id_type=MESH)
    pl.semaphore_wait(barrier, n - 1)


def neighbours(me):
    core, xpos, ypos = lax.rem(me, 2), lax.rem(me // 2, 2), me // 4
    other, across_x, across_y = 1 - 2 * core, 2 - 4 * xpos, 4 - 8 * ypos
    xnb, ynb, diag = me + across_x, me + across_y, me + across_x + across_y
    far_first = [diag, diag + other, xnb, ynb, xnb + other, ynb + other, me + other]
    return me + other, xnb, ynb, diag, far_first


def remote(src, dst, send_sem, recv_sem, peer):
    return pltpu.make_async_remote_copy(src_ref=src, dst_ref=dst, send_sem=send_sem, recv_sem=recv_sem,
                                        device_id={'ws': peer}, device_id_type=MESH)


def reverse_lanes(x):
    size = x.shape[-1]
    lane = lax.broadcasted_iota(jnp.int32, x.shape, 1)
    step = 1
    while step < size:
        x = jnp.where((lane & step) != 0, pltpu.roll(x, step, 1), pltpu.roll(x, size - step, 1))
        step *= 2
    return x


def head_mask_of(heads, width, head_dim):
    lane = lax.broadcasted_iota(jnp.int32, (heads, width), 1)
    return lane // head_dim == lax.broadcasted_iota(jnp.int32, (heads, width), 0)


def project(x, w):
    return lax.dot_general(x, w, NT, preferred_element_type=jnp.float32)


def gather_kernel(n, head_dim, hid, pos, eid, mask, ln_s, ln_c, ln_f, bias, wr, wq, wk, wv, wo, wqc, woc,
                  sk, sv, ck, cv,
                  h2_out, xall, eid_all, wr_all, *rest):
    (kt_out, vt_out), self_kv = rest[:2], rest[2:2 * PIECES + 2]
    (ck_v, cv_v, wo_all, wqc_all, woc_all, hid_v, pos_s, eid_s, mask_v, ln_sv, ln_cv, ln_fv, bias_v, hall, wqkv, snd, qkv,
     q_sc, kv_out, s_sc, p_sc, pn_sc, ctx_sc, col_sc, loc_sem, send, recv, sw, rw, rp) = rest[2 * PIECES + 2:]
    me = lax.axis_index('ws')
    rows, width = hid.shape
    cols = wq.shape[0]
    heads, length = s_sc.shape[1:]
    src_len = ck.shape[2]
    piece = rows // PIECES
    f32, bf16 = jnp.float32, jnp.bfloat16
    pair, xnb, ynb, diag, peers = neighbours(me)

    count = []

    def local(src, dst):
        copy = pltpu.make_async_copy(src, dst, loc_sem.at[len(count)])
        copy.start()
        count.append(copy)
        return copy

    small = [local(hid, hid_v), local(wr, wr_all.at[me]), local(eid, eid_s), local(pos, pos_s), local(bias, bias_v),
             local(ln_s, ln_sv.at[0]), local(ln_c, ln_cv.at[0]), local(ln_f, ln_fv.at[0]), local(mask, mask_v)]
    proj = [local(w, wqkv.at[i]) for i, w in enumerate((wq, wk, wv))]
    entry_barrier(me, n)
    for c in small:
        c.wait()
    first = [remote(hid_v, hall.at[me], send.at[0], recv.at[0], p) for p in peers]
    others = pl.ds(0, n - 1)

    def all_of(ref, i):
        return remote(ref.at[others], ref.at[others], send.at[i], recv.at[i], peers[0])

    for c in first:
        c.start()

    fulls = ((wo, wo_all), (wqc, wqc_all), (woc, woc_all))
    half = cols // 2
    own_copies = []
    moves = {}

    def move(name, i, src_dev, lo, size, sem, peer, src=None):
        dst = fulls[i][1].at[pl.ds(pl.multiple_of(src_dev * cols + lo, half), size)]
        moves[name, i] = remote(dst if src is None else src, dst, sw.at[i], sem, peer)
        moves[name, i].start()

    def own_share(i):
        src, dst = fulls[i]
        upper, lower = src.at[pl.ds(0, half)], src.at[pl.ds(half, half)]
        move('x0', i, me, 0, half, rw.at[0, i], xnb, upper)
        move('y1', i, me, half, half, rw.at[1, i], ynb, lower)
        move('x1', i, me, half, half, rw.at[2, i], xnb, lower)
        move('y0', i, me, 0, half, rw.at[3, i], ynb, upper)
        move('pair', i, me, 0, cols, rp.at[i], pair, src)
        own_copies.append(local(src, dst.at[pl.ds(pl.multiple_of(me * cols, cols), cols)]))

    load_self = [local(src.at[pl.ds(t * piece, piece)], self_kv[i * PIECES + t])
                 for i, src in enumerate((sk, sv)) for t in range(PIECES)]
    load_cross = [local(ck, ck_v), local(cv.at[pl.ds(0, piece)], cv_v)]
    hall[me] = hid_v[...]
    col_sc[...] = jnp.zeros_like(col_sc)
    for r in range(rows):
        eid_all[me, r:r + 1, :] = jnp.full((1, LANES), eid_s[r], jnp.int32)

    own_share(0)
    key_pos = lax.broadcasted_iota(jnp.int32, (1, length), 1)
    table = reverse_lanes(jnp.concatenate(
        [bias_v[...], jnp.zeros((heads - bias_v.shape[0], length), f32)], axis=0))

    @pl.loop(0, rows // BIAS_GROUP)
    def _(i):
        marks = [jnp.full((1, length), pos_s[i * BIAS_GROUP + j], jnp.int32) for j in range(BIAS_GROUP)]
        turned, step = [table] * BIAS_GROUP, 1
        while step < length:
            turned = [jnp.where(((p + 1) & step) != 0, pltpu.roll(t, step, 1), t) for p, t in zip(marks, turned)]
            step *= 2
        for j in range(BIAS_GROUP):
            s_sc[i * BIAS_GROUP + j] = jnp.where(key_pos <= marks[j], turned[j], NEG_BIG)

    all_of(hall, 0).wait_recv()
    for c in proj:
        c.wait()
    x_norm = rms_norm(hall[...].reshape(n * rows, width), ln_sv[...])
    for i in range(3):
        snd[:, i] = project(x_norm, wqkv[i]).astype(bf16).reshape(n, rows, cols)
    second = [remote(snd.at[p], qkv.at[me], send.at[3], recv.at[3], p) for p in peers]
    for c in second:
        c.start()
    qkv[me] = snd[me]
    own_share(1)

    def relay(i):
        moves['x0', i].wait_recv()
        move('ry', i, xnb, 0, half, rw.at[4, i], ynb)
        moves['y1', i].wait_recv()
        move('rx', i, ynb, half, half, rw.at[5, i], xnb)
        move('p0', i, xnb, 0, half, rp.at[i], pair)
        move('p1', i, ynb, half, half, rp.at[i], pair)

    def relay_rest(i):
        moves['x1', i].wait_recv()
        move('p2', i, xnb, half, half, rp.at[i], pair)
        moves['y0', i].wait_recv()
        move('p3', i, ynb, 0, half, rp.at[i], pair)

    def relay_diag(i):
        moves['ry', i].wait_recv()
        move('p4', i, diag, 0, half, rp.at[i], pair)
        moves['rx', i].wait_recv()
        move('p5', i, diag, half, half, rp.at[i], pair)

    def wait_weight(i):
        theirs = fulls[i][1].at[pl.ds(0, 4 * cols)]
        remote(theirs, theirs, sw.at[i], rp.at[i], pair).wait_recv()
        own_copies[i].wait()

    all_of(qkv, 3).wait_recv()
    for c in load_self[:PIECES]:
        c.wait()

    def assemble(i):
        return jnp.concatenate([qkv[p, i].astype(f32) for p in range(n)], axis=1)

    q_sc[...] = assemble(0)
    kv_out[0] = assemble(1)
    kv_out[1] = assemble(2)
    head_mask = head_mask_of(heads, width, head_dim)

    def over_rows(lo, hi, body, group=GROUP):
        @pl.loop(0, (hi - lo) // group)
        def _(i):
            for j in range(group):
                body(lo + i * group + j, i * group + j)

    def softmax(s):
        e = jnp.exp(s - jnp.max(s, axis=-1, keepdims=True))
        return (e / jnp.sum(e, axis=-1, keepdims=True)).astype(bf16)

    split = MXU_HEADS * head_dim
    lane = lax.broadcasted_iota(jnp.int32, (1, LANES), 1)

    def store_context(b, probs, vals, r, new=0.0):
        size = probs.shape[1]
        o = jnp.concatenate([project(probs, vals[r, 0:split]), jnp.zeros((heads, width - split), f32)], axis=1) + new
        ctx_sc[pl.ds(b, 1), :] = jnp.sum(jnp.where(head_mask, o, 0.0), axis=0, keepdims=True)
        weights = probs.astype(f32)
        for lo in range(split, width, head_dim):
            h = lo // head_dim
            terms = vals[r, lo:lo + head_dim].astype(f32) * weights[h:h + 1]
            folded = functools.reduce(jnp.add, [terms[:, c:c + LANES] for c in range(0, size, LANES)])
            column = jnp.sum(folded, axis=1, keepdims=True)
            at = slice(lo - split, lo - split + head_dim)
            col_sc[at] = jnp.where(lane == b, column, col_sc[at])

    def contexts():
        late = col_sc[...].T[0:rows]
        return (ctx_sc[...] + jnp.concatenate([jnp.zeros((rows, split), f32), late], axis=1)).astype(bf16)

    def self_scores(t):
        def body(b, r):
            q = jnp.where(head_mask, q_sc[pl.ds(b, 1), :], 0.0)
            s_new = jnp.sum(q * kv_out[0, pl.ds(b, 1), :], axis=1, keepdims=True)
            s = jnp.dot(q.astype(bf16), self_kv[t][r], preferred_element_type=f32)
            s_sc[b] = jnp.where(key_pos == pos_s[b], s_new, s) + s_sc[b]
        over_rows(t * piece, (t + 1) * piece, body)

    def self_softmax():
        def body(b, r):
            probs = softmax(s_sc[b]).astype(f32)
            hit = key_pos == pos_s[b]
            p_new = jnp.sum(jnp.where(hit, probs, 0.0), axis=1, keepdims=True)
            pn_sc[b] = jnp.broadcast_to(p_new, (heads, LANES))
            p_sc[b] = jnp.where(hit, 0.0, probs).astype(bf16)
        over_rows(0, rows, body, SOFTMAX_GROUP)

    def self_context(t):
        def body(b, r):
            store_context(b, p_sc[b], self_kv[PIECES + t], r, pn_sc[b, :, 0:1] * kv_out[1, pl.ds(b, 1), :])
        over_rows(t * piece, (t + 1) * piece, body)

    relay(0)
    self_scores(0)
    relay(1)
    own_share(2)
    self_scores(1)
    relay_rest(0)
    self_softmax()
    for c in load_self[PIECES:]:
        c.wait()
    self_context(0)
    relay_diag(0)
    relay_rest(1)
    self_context(1)
    relay_diag(1)
    wait_weight(0)
    h1 = (hid_v[...].astype(f32) + project(contexts(), wo_all[...])).astype(bf16)
    relay(2)
    for p in peers:
        remote(eid_all.at[me], eid_all.at[me], send.at[1], recv.at[1], p).start()
        remote(wr_all.at[me], wr_all.at[me], send.at[2], recv.at[2], p).start()

    wait_weight(1)
    q_sc[...] = project(rms_norm(h1, ln_cv[...]), wqc_all[...]).astype(bf16).astype(f32)
    for c in load_cross:
        c.wait()

    def cross_scores(b, r):
        q = jnp.where(head_mask, q_sc[pl.ds(b, 1), :], 0.0).astype(bf16)
        s_sc[b, :, 0:src_len] = (jnp.dot(q, ck_v[b], preferred_element_type=f32)
                                 + jnp.where(mask_v[pl.ds(b, 1), :] == 1, 0.0, NEG_BIG))

    def cross_softmax(b, r):
        p_sc[b, :, 0:src_len] = softmax(s_sc[b, :, 0:src_len])

    def cross_context(b, r):
        store_context(b, p_sc[b, :, 0:src_len], cv_v, b)

    def cross_context_late(b, r):
        store_context(b, p_sc[b, :, 0:src_len], ck_v, r)

    over_rows(0, piece, cross_scores)
    load_late = local(cv.at[pl.ds(piece, piece)], ck_v.at[pl.ds(0, piece)])
    over_rows(piece, rows, cross_scores)
    relay_rest(2)
    over_rows(0, rows, cross_softmax, SOFTMAX_GROUP)
    relay_diag(2)
    over_rows(0, piece, cross_context)
    load_late.wait()
    over_rows(piece, rows, cross_context_late)
    wait_weight(2)
    h2 = (h1.astype(f32) + project(contexts(), woc_all[...])).astype(bf16)
    xall[me] = rms_norm(h2, ln_fv[...])
    h2_out[...] = h2
    third = [remote(xall.at[me], xall.at[me], send.at[4], recv.at[4], p) for p in peers]
    for c in third:
        c.start()
    for i, ref in enumerate((kt_out, vt_out)):
        cols_t = jnp.concatenate([kv_out[i], jnp.zeros((LANES - rows, width), f32)], axis=0).T
        for g in range(rows // UPDATE):
            shifted = cols_t if g == 0 else pltpu.roll(cols_t, LANES - g * UPDATE, 1)
            ref[g] = shifted.astype(bf16)
    for j in range(READY):
        hit = key_pos == pos_s[j]
        for i, ref in enumerate((kt_out, vt_out)):
            cache = self_kv[i * PIECES]
            cache[j] = jnp.where(hit, ref[0, :, j:j + 1], cache[j])
    for i, ref in ((1, eid_all), (2, wr_all), (4, xall)):
        all_of(ref, i).wait_recv()
    for i, ref in enumerate((hall, eid_all, wr_all, snd, xall)):
        all_of(ref, i).wait_send()
    for i in range(3):
        moved = fulls[i][1].at[pl.ds(0, 7 * cols)]
        remote(moved, moved, sw.at[i], rp.at[i], pair).wait_send()


def update_kernel(n, capacity, pos, kt, vt, xall, eid_all, wr_all, win, wout, *rest):
    (part, gate, nk, nv), self_kv, (hidden_sc, out_sem) = (
        rest[2 * PIECES:2 * PIECES + 4], rest[2 * PIECES + 4:-2], rest[-2:])
    me = lax.axis_index('ws')
    _, rows, width = xall.shape
    experts, _, units = win.shape
    group_rows = n * rows
    piece = rows // PIECES
    f32 = jnp.float32
    lane = lax.broadcasted_iota(jnp.int32, (1, LANES), 1)

    for b in range(READY):
        pltpu.make_async_copy(self_kv[0].at[b], nk.at[b], out_sem.at[0]).start()
        pltpu.make_async_copy(self_kv[PIECES].at[b], nv.at[b], out_sem.at[1]).start()

    for t in range(PIECES):
        keys, vals = self_kv[t], self_kv[PIECES + t]

        @pl.loop(READY // UPDATE if t == 0 else 0, piece // UPDATE)
        def _(i):
            g = t * (piece // UPDATE) + i
            def write(j):
                r = i * UPDATE + j
                b = t * piece + r
                pltpu.make_async_copy(keys.at[r], nk.at[b], out_sem.at[0]).start()
                pltpu.make_async_copy(vals.at[r], nv.at[b], out_sem.at[1]).start()

            for j in range(UPDATE):
                r = i * UPDATE + j
                b = t * piece + r
                p = pos[b]
                win_at = pl.ds(pl.multiple_of((p // LANES) * LANES, LANES), LANES)
                hit = lane == p % LANES
                for cache, new in ((keys, kt), (vals, vt)):
                    cache[r, :, win_at] = jnp.where(hit, new[g, :, j:j + 1], cache[r, :, win_at])
                if j:
                    write(j - 1)
            write(UPDATE - 1)

    eid = eid_all[...].reshape(group_rows, LANES)
    eid_col = eid[:, 0:1]
    xs = xall[...].reshape(group_rows, width)
    for e in range(experts):
        u = jnp.dot(xs, win[e], preferred_element_type=f32)
        hidden_sc[:, e * units:(e + 1) * units] = jnp.where(eid_col == e, jnp.maximum(u, 0.0), 0.0).astype(jnp.bfloat16)
    y = jnp.dot(hidden_sc[...], wout[...].reshape(experts * units, width), preferred_element_type=f32)
    part[...] = y.reshape(n, rows, width)

    x_own = xall[me].astype(f32)
    logits = [jnp.sum(x_own * wr_all[e], axis=-1, keepdims=True) for e in range(experts)]
    top = functools.reduce(jnp.maximum, logits)
    exps = [jnp.exp(l - top) for l in logits]
    total = functools.reduce(jnp.add, exps)
    own_col = eid_all[me][:, 0:1]
    chosen = functools.reduce(jnp.add, [jnp.where(own_col == e, exps[e], 0.0) for e in range(experts)])
    across = eid.astype(f32).T[0:1, :].astype(jnp.int32)
    row_ids = me * rows + lax.broadcasted_iota(jnp.int32, (rows, group_rows), 0)
    earlier = (across == own_col) & (lax.broadcasted_iota(jnp.int32, (rows, group_rows), 1) < row_ids)
    slot = jnp.sum(jnp.where(earlier, 1.0, 0.0), axis=1, keepdims=True)
    gate[...] = jnp.broadcast_to(jnp.where(slot < capacity, chosen / total, 0.0), gate.shape)

    for i, ref in enumerate((nk, nv)):
        pltpu.make_async_copy(ref, ref, out_sem.at[i]).wait()


def reduce_kernel(n, part, gate, h2, out, acc, send, recv):
    me = lax.axis_index('ws')
    f32 = jnp.float32
    entry_barrier(me, n)
    for peer in neighbours(me)[-1]:
        remote(part.at[peer], acc.at[me], send, recv, peer).start()
    acc[me] = part[me]
    others = pl.ds(0, n - 1)
    copies = remote(part.at[others], acc.at[others], send, recv, lax.rem(me + 1, n))
    copies.wait_recv()
    y_own = functools.reduce(jnp.add, [acc[p] for p in range(n)]).astype(jnp.bfloat16)
    out[...] = (h2[...].astype(f32) + y_own.astype(f32) * gate[:, 0:1]).astype(jnp.bfloat16)
    copies.wait_send()


def solution(mesh):
    n = mesh.shape['ws']
    row_axes = ('dp', 'ws')
    row_vec = P(row_axes)
    row_mat = P(row_axes, None)
    cache_spec = P(row_axes, None, None, None)
    col_split = P(None, 'ws')
    in_specs = (row_mat, cache_spec, cache_spec, cache_spec, cache_spec, row_vec, row_mat, P(None, None), row_vec,
                P(None), P(None), P(None), col_split, col_split, col_split, col_split, col_split, col_split,
                col_split, P(None, None, 'ws'), P(None, 'ws', None))
    out_specs = (row_mat, cache_spec, cache_spec)

    def decoder_block(hidden, self_k, self_v, cross_k, cross_v, positions, enc_mask, rel_bias, expert_idx,
                      ln_self, ln_cross, ln_ffn, wq_self, wk_self, wv_self, wo_self, wq_cross, wo_cross,
                      w_router, w_in, w_out):
        rows, width = hidden.shape
        heads, head_dim = self_k.shape[1], self_k.shape[3]
        cols = wq_self.shape[1]
        experts, _, units = w_in.shape
        group_rows = rows * n
        capacity = (2 * group_rows + experts - 1) // experts
        bf16, f32, i32 = jnp.bfloat16, jnp.float32, jnp.int32
        pad_heads = 16
        dma = pltpu.SemaphoreType.DMA

        def flat(cache):
            return cache.transpose(0, 1, 3, 2).reshape(rows, heads * head_dim, cache.shape[2])

        sk, sv, ck, cv = (flat(c) for c in (self_k, self_v, cross_k, cross_v))
        pieces = [pltpu.VMEM((rows // PIECES,) + c.shape[1:], bf16) for c in (sk, sv) for _ in range(PIECES)]
        length, src_len = sk.shape[2], ck.shape[2]
        row_bf16, row_f32 = pltpu.VMEM((rows, width), bf16), pltpu.VMEM((rows, width), f32)
        full = pltpu.VMEM((n * cols, width), bf16)
        columns = pltpu.VMEM((rows // UPDATE, width, LANES), bf16)
        ln_row = pltpu.VMEM((1, width), f32)
        index = pltpu.SMEM((rows,), i32)
        exchange = pltpu.VMEM((n, 3, rows, cols), bf16)
        operands = (hidden, positions, expert_idx, enc_mask, ln_self, ln_cross, ln_ffn, rel_bias, w_router.T,
                    wq_self.T, wk_self.T, wv_self.T, wo_self.T, wq_cross.T, wo_cross.T, sk, sv, ck, cv)
        gathered = pl.pallas_call(
            functools.partial(gather_kernel, n, head_dim),
            out_shape=(row_bf16, pltpu.VMEM((n, rows, width), bf16),
                       pltpu.VMEM((n, rows, LANES), i32), pltpu.VMEM((n, 1, width), f32),
                       columns, columns, *pieces),
            in_specs=[HBM] * len(operands),
            out_specs=(VMEM,) * (6 + len(pieces)),
            scratch_shapes=[pltpu.VMEM(ck.shape, bf16), pltpu.VMEM((rows // PIECES,) + cv.shape[1:], bf16), full, full, full,
                            row_bf16, index, index, pltpu.VMEM(enc_mask.shape, i32), ln_row, ln_row, ln_row,
                            pltpu.VMEM(rel_bias.shape, f32), pltpu.VMEM((n, rows, width), bf16),
                            pltpu.VMEM((3, cols, width), bf16), exchange, exchange, row_f32, pltpu.VMEM((2, rows, width), f32),
                            pltpu.VMEM((rows, pad_heads, length), f32), pltpu.VMEM((rows, pad_heads, length), bf16),
                            pltpu.VMEM((rows, pad_heads, LANES), f32), row_f32,
                            pltpu.VMEM((width - MXU_HEADS * head_dim, LANES), f32),
                            dma((20 + 2 * PIECES,)), dma((5,)), dma((5,)), dma((3,)), dma((6, 3)), dma((3,))],
            compiler_params=pltpu.CompilerParams(collective_id=0, has_side_effects=True, vmem_limit_bytes=40 << 19),
            name='gather')(*(hbm(x) for x in operands))
        h2, xall, eid_all, wr_all, kt, vt, *caches = gathered

        part, gate, new_k, new_v, *_ = pl.pallas_call(
            functools.partial(update_kernel, n, capacity),
            out_shape=(pltpu.VMEM((n, rows, width), f32), pltpu.VMEM((rows, LANES), f32),
                       pltpu.HBM(sk.shape, bf16), pltpu.HBM(sv.shape, bf16), *pieces),
            in_specs=[SMEM] + [VMEM] * (7 + len(pieces)),
            out_specs=(VMEM, VMEM, HBM, HBM) + (VMEM,) * len(pieces),
            input_output_aliases={8 + t: 4 + t for t in range(len(pieces))},
            scratch_shapes=[pltpu.VMEM((group_rows, experts * units), bf16), dma((2,))],
            compiler_params=pltpu.CompilerParams(vmem_limit_bytes=10 << 19),
            name='attend')(positions, kt, vt, xall, eid_all, wr_all, w_in, w_out, *caches)

        hidden_out = pl.pallas_call(
            functools.partial(reduce_kernel, n),
            out_shape=jax.ShapeDtypeStruct((rows, width), bf16),
            in_specs=[VMEM] * 3,
            out_specs=VMEM,
            scratch_shapes=[pltpu.VMEM((n, rows, width), f32), dma, dma],
            compiler_params=pltpu.CompilerParams(collective_id=1, has_side_effects=True, vmem_limit_bytes=4 << 20),
            name='experts')(part, gate, h2)

        def unflat(cache):
            return cache.reshape(rows, heads, head_dim, cache.shape[2]).transpose(0, 1, 3, 2)

        return hidden_out, unflat(new_k), unflat(new_v)

    return jax.shard_map(decoder_block, mesh=mesh, in_specs=in_specs, out_specs=out_specs, check_vma=False)
```

```python
import functools
import jax
import jax.numpy as jnp
from jax import lax
from jax.sharding import PartitionSpec as P
from jax.experimental import pallas as pl
from jax.experimental.pallas import tpu as pltpu

EPSILON = 1e-6
NEG_BIG = -1e30
LANES = 128
GROUP = 4
SOFTMAX_GROUP = 8
BIAS_GROUP = 4
MXU_HEADS = 6
UPDATE = 4
READY = 4
PIECES = 2
NT = (((1,), (1,)), ((), ()))
MESH = pl.DeviceIdType.MESH
VMEM = pl.BlockSpec(memory_space=pltpu.VMEM)
HBM = pl.BlockSpec(memory_space=pltpu.HBM)
SMEM = pl.BlockSpec(memory_space=pltpu.SMEM)


def hbm(x):
    return pltpu.with_memory_space_constraint(x, pltpu.HBM)


def rms_norm(hidden, scale):
    hid_f32 = hidden.astype(jnp.float32)
    inv_rms = lax.rsqrt(jnp.mean(hid_f32 * hid_f32, axis=-1, keepdims=True) + EPSILON)
    return (hid_f32 * inv_rms * scale).astype(jnp.bfloat16)


def entry_barrier(me, n):
    barrier = pltpu.get_barrier_semaphore()
    for k in range(1, n):
        pl.semaphore_signal(barrier, inc=1, device_id={'ws': lax.rem(me + k, n)}, device_id_type=MESH)
    pl.semaphore_wait(barrier, n - 1)


def neighbours(me):
    core, xpos, ypos = lax.rem(me, 2), lax.rem(me // 2, 2), me // 4
    other, across_x, across_y = 1 - 2 * core, 2 - 4 * xpos, 4 - 8 * ypos
    xnb, ynb, diag = me + across_x, me + across_y, me + across_x + across_y
    far_first = [diag, diag + other, xnb, ynb, xnb + other, ynb + other, me + other]
    return me + other, xnb, ynb, diag, far_first


def remote(src, dst, send_sem, recv_sem, peer):
    return pltpu.make_async_remote_copy(src_ref=src, dst_ref=dst, send_sem=send_sem, recv_sem=recv_sem,
                                        device_id={'ws': peer}, device_id_type=MESH)


def reverse_lanes(x):
    size = x.shape[-1]
    lane = lax.broadcasted_iota(jnp.int32, x.shape, 1)
    step = 1
    while step < size:
        x = jnp.where((lane & step) != 0, pltpu.roll(x, step, 1), pltpu.roll(x, size - step, 1))
        step *= 2
    return x


def head_mask_of(heads, width, head_dim):
    lane = lax.broadcasted_iota(jnp.int32, (heads, width), 1)
    return lane // head_dim == lax.broadcasted_iota(jnp.int32, (heads, width), 0)


def project(x, w):
    return lax.dot_general(x, w, NT, preferred_element_type=jnp.float32)


def gather_kernel(n, head_dim, hid, pos, eid, mask, ln_s, ln_c, ln_f, bias, wr, wq, wk, wv, wo, wqc, woc,
                  sk, sv, ck, cv,
                  h2_out, xall, eid_all, wr_all, *rest):
    (kt_out, vt_out), self_kv = rest[:2], rest[2:2 * PIECES + 2]
    (ck_v, cv_v, wo_all, wqc_all, woc_all, hid_v, pos_s, eid_s, mask_v, ln_sv, ln_cv, ln_fv, bias_v, hall, wqkv, snd, qkv,
     q_sc, kv_out, s_sc, p_sc, pn_sc, ctx_sc, col_sc, loc_sem, send, recv, sw, rw, rp) = rest[2 * PIECES + 2:]
    me = lax.axis_index('ws')
    rows, width = hid.shape
    cols = wq.shape[0]
    heads, length = s_sc.shape[1:]
    src_len = ck.shape[2]
    piece = rows // PIECES
    f32, bf16 = jnp.float32, jnp.bfloat16
    pair, xnb, ynb, diag, peers = neighbours(me)

    count = []

    def local(src, dst):
        copy = pltpu.make_async_copy(src, dst, loc_sem.at[len(count)])
        copy.start()
        count.append(copy)
        return copy

    small = [local(hid, hid_v), local(wr, wr_all.at[me]), local(eid, eid_s), local(pos, pos_s), local(bias, bias_v),
             local(ln_s, ln_sv.at[0]), local(ln_c, ln_cv.at[0]), local(ln_f, ln_fv.at[0]), local(mask, mask_v)]
    proj = [local(w, wqkv.at[i]) for i, w in enumerate((wq, wk, wv))]
    entry_barrier(me, n)
    for c in small:
        c.wait()
    first = [remote(hid_v, hall.at[me], send.at[0], recv.at[0], p) for p in peers]
    others = pl.ds(0, n - 1)

    def all_of(ref, i):
        return remote(ref.at[others], ref.at[others], send.at[i], recv.at[i], peers[0])

    for c in first:
        c.start()

    fulls = ((wo, wo_all), (wqc, wqc_all), (woc, woc_all))
    half = cols // 2
    own_copies = []
    moves = {}

    def move(name, i, src_dev, lo, size, sem, peer, src=None):
        dst = fulls[i][1].at[pl.ds(pl.multiple_of(src_dev * cols + lo, half), size)]
        moves[name, i] = remote(dst if src is None else src, dst, sw.at[i], sem, peer)
        moves[name, i].start()

    def own_share(i):
        src, dst = fulls[i]
        upper, lower = src.at[pl.ds(0, half)], src.at[pl.ds(half, half)]
        move('x0', i, me, 0, half, rw.at[0, i], xnb, upper)
        move('y1', i, me, half, half, rw.at[1, i], ynb, lower)
        move('x1', i, me, half, half, rw.at[2, i], xnb, lower)
        move('y0', i, me, 0, half, rw.at[3, i], ynb, upper)
        move('pair', i, me, 0, cols, rp.at[i], pair, src)
        own_copies.append(local(src, dst.at[pl.ds(pl.multiple_of(me * cols, cols), cols)]))

    load_self = [local(src.at[pl.ds(t * piece, piece)], self_kv[i * PIECES + t])
                 for i, src in enumerate((sk, sv)) for t in range(PIECES)]
    load_cross = [local(ck, ck_v), local(cv.at[pl.ds(0, piece)], cv_v)]
    hall[me] = hid_v[...]
    col_sc[...] = jnp.zeros_like(col_sc)
    for r in range(rows):
        eid_all[me, r:r + 1, :] = jnp.full((1, LANES), eid_s[r], jnp.int32)

    own_share(0)
    key_pos = lax.broadcasted_iota(jnp.int32, (1, length), 1)
    table = reverse_lanes(jnp.concatenate(
        [bias_v[...], jnp.zeros((heads - bias_v.shape[0], length), f32)], axis=0))

    @pl.loop(0, rows // BIAS_GROUP)
    def _(i):
        marks = [jnp.full((1, length), pos_s[i * BIAS_GROUP + j], jnp.int32) for j in range(BIAS_GROUP)]
        turned, step = [table] * BIAS_GROUP, 1
        while step < length:
            turned = [jnp.where(((p + 1) & step) != 0, pltpu.roll(t, step, 1), t) for p, t in zip(marks, turned)]
            step *= 2
        for j in range(BIAS_GROUP):
            s_sc[i * BIAS_GROUP + j] = jnp.where(key_pos <= marks[j], turned[j], NEG_BIG)

    all_of(hall, 0).wait_recv()
    for c in proj:
        c.wait()
    x_norm = rms_norm(hall[...].reshape(n * rows, width), ln_sv[...])
    for i in range(3):
        snd[:, i] = project(x_norm, wqkv[i]).astype(bf16).reshape(n, rows, cols)
    second = [remote(snd.at[p], qkv.at[me], send.at[3], recv.at[3], p) for p in peers]
    for c in second:
        c.start()
    qkv[me] = snd[me]
    own_share(1)

    def relay(i):
        moves['x0', i].wait_recv()
        move('ry', i, xnb, 0, half, rw.at[4, i], ynb)
        moves['y1', i].wait_recv()
        move('rx', i, ynb, half, half, rw.at[5, i], xnb)
        move('p0', i, xnb, 0, half, rp.at[i], pair)
        move('p1', i, ynb, half, half, rp.at[i], pair)

    def relay_rest(i):
        moves['x1', i].wait_recv()
        move('p2', i, xnb, half, half, rp.at[i], pair)
        moves['y0', i].wait_recv()
        move('p3', i, ynb, 0, half, rp.at[i], pair)

    def relay_diag(i):
        moves['ry', i].wait_recv()
        move('p4', i, diag, 0, half, rp.at[i], pair)
        moves['rx', i].wait_recv()
        move('p5', i, diag, half, half, rp.at[i], pair)

    def wait_weight(i):
        theirs = fulls[i][1].at[pl.ds(0, 4 * cols)]
        remote(theirs, theirs, sw.at[i], rp.at[i], pair).wait_recv()
        own_copies[i].wait()

    all_of(qkv, 3).wait_recv()
    for c in load_self[:PIECES]:
        c.wait()

    def assemble(i):
        return jnp.concatenate([qkv[p, i].astype(f32) for p in range(n)], axis=1)

    q_sc[...] = assemble(0)
    kv_out[0] = assemble(1)
    kv_out[1] = assemble(2)
    head_mask = head_mask_of(heads, width, head_dim)

    def over_rows(lo, hi, body, group=GROUP):
        @pl.loop(0, (hi - lo) // group)
        def _(i):
            for j in range(group):
                body(lo + i * group + j, i * group + j)

    def softmax(s):
        e = jnp.exp(s - jnp.max(s, axis=-1, keepdims=True))
        return (e / jnp.sum(e, axis=-1, keepdims=True)).astype(bf16)

    split = MXU_HEADS * head_dim
    lane = lax.broadcasted_iota(jnp.int32, (1, LANES), 1)

    def store_context(b, probs, vals, r, new=0.0):
        size = probs.shape[1]
        o = jnp.concatenate([project(probs, vals[r, 0:split]), jnp.zeros((heads, width - split), f32)], axis=1) + new
        ctx_sc[pl.ds(b, 1), :] = jnp.sum(jnp.where(head_mask, o, 0.0), axis=0, keepdims=True)
        weights = probs.astype(f32)
        for lo in range(split, width, head_dim):
            h = lo // head_dim
            terms = vals[r, lo:lo + head_dim].astype(f32) * weights[h:h + 1]
            folded = functools.reduce(jnp.add, [terms[:, c:c + LANES] for c in range(0, size, LANES)])
            column = jnp.sum(folded, axis=1, keepdims=True)
            at = slice(lo - split, lo - split + head_dim)
            col_sc[at] = jnp.where(lane == b, column, col_sc[at])

    def contexts():
        late = col_sc[...].T[0:rows]
        return (ctx_sc[...] + jnp.concatenate([jnp.zeros((rows, split), f32), late], axis=1)).astype(bf16)

    def self_scores(t):
        def body(b, r):
            q = jnp.where(head_mask, q_sc[pl.ds(b, 1), :], 0.0)
            s_new = jnp.sum(q * kv_out[0, pl.ds(b, 1), :], axis=1, keepdims=True)
            s = jnp.dot(q.astype(bf16), self_kv[t][r], preferred_element_type=f32)
            s_sc[b] = jnp.where(key_pos == pos_s[b], s_new, s) + s_sc[b]
        over_rows(t * piece, (t + 1) * piece, body)

    def self_softmax():
        def body(b, r):
            probs = softmax(s_sc[b]).astype(f32)
            hit = key_pos == pos_s[b]
            p_new = jnp.sum(jnp.where(hit, probs, 0.0), axis=1, keepdims=True)
            pn_sc[b] = jnp.broadcast_to(p_new, (heads, LANES))
            p_sc[b] = jnp.where(hit, 0.0, probs).astype(bf16)
        over_rows(0, rows, body, SOFTMAX_GROUP)

    def self_context(t):
        def body(b, r):
            store_context(b, p_sc[b], self_kv[PIECES + t], r, pn_sc[b, :, 0:1] * kv_out[1, pl.ds(b, 1), :])
        over_rows(t * piece, (t + 1) * piece, body)

    relay(0)
    self_scores(0)
    relay(1)
    own_share(2)
    self_scores(1)
    relay_rest(0)
    self_softmax()
    for c in load_self[PIECES:]:
        c.wait()
    self_context(0)
    relay_diag(0)
    relay_rest(1)
    self_context(1)
    relay_diag(1)
    wait_weight(0)
    h1 = (hid_v[...].astype(f32) + project(contexts(), wo_all[...])).astype(bf16)
    relay(2)
    for p in peers:
        remote(eid_all.at[me], eid_all.at[me], send.at[1], recv.at[1], p).start()
        remote(wr_all.at[me], wr_all.at[me], send.at[2], recv.at[2], p).start()

    wait_weight(1)
    q_sc[...] = project(rms_norm(h1, ln_cv[...]), wqc_all[...]).astype(bf16).astype(f32)
    for c in load_cross:
        c.wait()

    def cross_scores(b, r):
        q = jnp.where(head_mask, q_sc[pl.ds(b, 1), :], 0.0).astype(bf16)
        s_sc[b, :, 0:src_len] = (jnp.dot(q, ck_v[b], preferred_element_type=f32)
                                 + jnp.where(mask_v[pl.ds(b, 1), :] == 1, 0.0, NEG_BIG))

    def cross_softmax(b, r):
        p_sc[b, :, 0:src_len] = softmax(s_sc[b, :, 0:src_len])

    def cross_context(b, r):
        store_context(b, p_sc[b, :, 0:src_len], cv_v, b)

    def cross_context_late(b, r):
        store_context(b, p_sc[b, :, 0:src_len], ck_v, r)

    over_rows(0, piece, cross_scores)
    load_late = local(cv.at[pl.ds(piece, piece)], ck_v.at[pl.ds(0, piece)])
    over_rows(piece, rows, cross_scores)
    relay_rest(2)
    over_rows(0, rows, cross_softmax, SOFTMAX_GROUP)
    relay_diag(2)
    over_rows(0, piece, cross_context)
    load_late.wait()
    over_rows(piece, rows, cross_context_late)
    wait_weight(2)
    h2 = (h1.astype(f32) + project(contexts(), woc_all[...])).astype(bf16)
    xall[me] = rms_norm(h2, ln_fv[...])
    h2_out[...] = h2
    third = [remote(xall.at[me], xall.at[me], send.at[4], recv.at[4], p) for p in peers]
    for c in third:
        c.start()
    for i, ref in enumerate((kt_out, vt_out)):
        cols_t = jnp.concatenate([kv_out[i], jnp.zeros((LANES - rows, width), f32)], axis=0).T
        for g in range(rows // UPDATE):
            shifted = cols_t if g == 0 else pltpu.roll(cols_t, LANES - g * UPDATE, 1)
            ref[g] = shifted.astype(bf16)
    for j in range(READY):
        hit = key_pos == pos_s[j]
        for i, ref in enumerate((kt_out, vt_out)):
            cache = self_kv[i * PIECES]
            cache[j] = jnp.where(hit, ref[0, :, j:j + 1], cache[j])
    for i, ref in ((1, eid_all), (2, wr_all), (4, xall)):
        all_of(ref, i).wait_recv()
    for i, ref in enumerate((hall, eid_all, wr_all, snd, xall)):
        all_of(ref, i).wait_send()
    for i in range(3):
        moved = fulls[i][1].at[pl.ds(0, 7 * cols)]
        remote(moved, moved, sw.at[i], rp.at[i], pair).wait_send()


def update_kernel(n, capacity, pos, kt, vt, xall, eid_all, wr_all, win, wout, *rest):
    (part, gate, nk, nv), self_kv, (hidden_sc, out_sem) = (
        rest[2 * PIECES:2 * PIECES + 4], rest[2 * PIECES + 4:-2], rest[-2:])
    me = lax.axis_index('ws')
    _, rows, width = xall.shape
    experts, _, units = win.shape
    group_rows = n * rows
    piece = rows // PIECES
    f32 = jnp.float32
    lane = lax.broadcasted_iota(jnp.int32, (1, LANES), 1)

    for b in range(READY):
        pltpu.make_async_copy(self_kv[0].at[b], nk.at[b], out_sem.at[0]).start()
        pltpu.make_async_copy(self_kv[PIECES].at[b], nv.at[b], out_sem.at[1]).start()

    for t in range(PIECES):
        keys, vals = self_kv[t], self_kv[PIECES + t]

        @pl.loop(READY // UPDATE if t == 0 else 0, piece // UPDATE)
        def _(i):
            g = t * (piece // UPDATE) + i
            def write(j):
                r = i * UPDATE + j
                b = t * piece + r
                pltpu.make_async_copy(keys.at[r], nk.at[b], out_sem.at[0]).start()
                pltpu.make_async_copy(vals.at[r], nv.at[b], out_sem.at[1]).start()

            for j in range(UPDATE):
                r = i * UPDATE + j
                b = t * piece + r
                p = pos[b]
                win_at = pl.ds(pl.multiple_of((p // LANES) * LANES, LANES), LANES)
                hit = lane == p % LANES
                for cache, new in ((keys, kt), (vals, vt)):
                    cache[r, :, win_at] = jnp.where(hit, new[g, :, j:j + 1], cache[r, :, win_at])
                if j:
                    write(j - 1)
            write(UPDATE - 1)

    eid = eid_all[...].reshape(group_rows, LANES)
    eid_col = eid[:, 0:1]
    xs = xall[...].reshape(group_rows, width)
    for e in range(experts):
        u = jnp.dot(xs, win[e], preferred_element_type=f32)
        hidden_sc[:, e * units:(e + 1) * units] = jnp.where(eid_col == e, jnp.maximum(u, 0.0), 0.0).astype(jnp.bfloat16)
    y = jnp.dot(hidden_sc[...], wout[...].reshape(experts * units, width), preferred_element_type=f32)
    part[...] = y.reshape(n, rows, width)

    x_own = xall[me].astype(f32)
    logits = [jnp.sum(x_own * wr_all[e], axis=-1, keepdims=True) for e in range(experts)]
    top = functools.reduce(jnp.maximum, logits)
    exps = [jnp.exp(l - top) for l in logits]
    total = functools.reduce(jnp.add, exps)
    own_col = eid_all[me][:, 0:1]
    chosen = functools.reduce(jnp.add, [jnp.where(own_col == e, exps[e], 0.0) for e in range(experts)])
    across = eid.astype(f32).T[0:1, :].astype(jnp.int32)
    row_ids = me * rows + lax.broadcasted_iota(jnp.int32, (rows, group_rows), 0)
    earlier = (across == own_col) & (lax.broadcasted_iota(jnp.int32, (rows, group_rows), 1) < row_ids)
    slot = jnp.sum(jnp.where(earlier, 1.0, 0.0), axis=1, keepdims=True)
    gate[...] = jnp.broadcast_to(jnp.where(slot < capacity, chosen / total, 0.0), gate.shape)

    for i, ref in enumerate((nk, nv)):
        pltpu.make_async_copy(ref, ref, out_sem.at[i]).wait()


def reduce_kernel(n, part, gate, h2, out, near, mixed, far, s1, r1, s2, r2):
    me = lax.axis_index('ws')
    f32 = jnp.float32
    entry_barrier(me, n)
    _, _, _, _, (diag, diag_o, x_same, y_same, x_o, y_o, pair) = neighbours(me)
    to_pair = [remote(part.at[d], near.at[t], s1.at[t], r1.at[t], pair) for t, d in enumerate((diag, x_same, y_same, pair))]
    for c in to_pair:
        c.start()
    to_far = []
    for t, d in enumerate((diag_o, x_o, y_o)):
        to_pair[t].wait_recv()
        mixed[t] = part[d] + near[t]
        to_far.append(remote(mixed.at[t], far.at[t], s2.at[t], r2.at[t], d))
        to_far[-1].start()
    to_pair[3].wait_recv()
    y_own = part[me] + near[3]
    for t, c in enumerate(to_far):
        c.wait_recv()
        y_own = y_own + far[t]
    out[...] = (h2[...].astype(f32) + y_own.astype(jnp.bfloat16).astype(f32) * gate[:, 0:1]).astype(jnp.bfloat16)
    for c in to_pair + to_far:
        c.wait_send()


def solution(mesh):
    n = mesh.shape['ws']
    row_axes = ('dp', 'ws')
    row_vec = P(row_axes)
    row_mat = P(row_axes, None)
    cache_spec = P(row_axes, None, None, None)
    col_split = P(None, 'ws')
    in_specs = (row_mat, cache_spec, cache_spec, cache_spec, cache_spec, row_vec, row_mat, P(None, None), row_vec,
                P(None), P(None), P(None), col_split, col_split, col_split, col_split, col_split, col_split,
                col_split, P(None, None, 'ws'), P(None, 'ws', None))
    out_specs = (row_mat, cache_spec, cache_spec)

    def decoder_block(hidden, self_k, self_v, cross_k, cross_v, positions, enc_mask, rel_bias, expert_idx,
                      ln_self, ln_cross, ln_ffn, wq_self, wk_self, wv_self, wo_self, wq_cross, wo_cross,
                      w_router, w_in, w_out):
        rows, width = hidden.shape
        heads, head_dim = self_k.shape[1], self_k.shape[3]
        cols = wq_self.shape[1]
        experts, _, units = w_in.shape
        group_rows = rows * n
        capacity = (2 * group_rows + experts - 1) // experts
        bf16, f32, i32 = jnp.bfloat16, jnp.float32, jnp.int32
        pad_heads = 16
        dma = pltpu.SemaphoreType.DMA

        def flat(cache):
            return cache.transpose(0, 1, 3, 2).reshape(rows, heads * head_dim, cache.shape[2])

        sk, sv, ck, cv = (flat(c) for c in (self_k, self_v, cross_k, cross_v))
        pieces = [pltpu.VMEM((rows // PIECES,) + c.shape[1:], bf16) for c in (sk, sv) for _ in range(PIECES)]
        length, src_len = sk.shape[2], ck.shape[2]
        row_bf16, row_f32 = pltpu.VMEM((rows, width), bf16), pltpu.VMEM((rows, width), f32)
        full = pltpu.VMEM((n * cols, width), bf16)
        columns = pltpu.VMEM((rows // UPDATE, width, LANES), bf16)
        ln_row = pltpu.VMEM((1, width), f32)
        index = pltpu.SMEM((rows,), i32)
        exchange = pltpu.VMEM((n, 3, rows, cols), bf16)
        operands = (hidden, positions, expert_idx, enc_mask, ln_self, ln_cross, ln_ffn, rel_bias, w_router.T,
                    wq_self.T, wk_self.T, wv_self.T, wo_self.T, wq_cross.T, wo_cross.T, sk, sv, ck, cv)
        gathered = pl.pallas_call(
            functools.partial(gather_kernel, n, head_dim),
            out_shape=(row_bf16, pltpu.VMEM((n, rows, width), bf16),
                       pltpu.VMEM((n, rows, LANES), i32), pltpu.VMEM((n, 1, width), f32),
                       columns, columns, *pieces),
            in_specs=[HBM] * len(operands),
            out_specs=(VMEM,) * (6 + len(pieces)),
            scratch_shapes=[pltpu.VMEM(ck.shape, bf16), pltpu.VMEM((rows // PIECES,) + cv.shape[1:], bf16), full, full, full,
                            row_bf16, index, index, pltpu.VMEM(enc_mask.shape, i32), ln_row, ln_row, ln_row,
                            pltpu.VMEM(rel_bias.shape, f32), pltpu.VMEM((n, rows, width), bf16),
                            pltpu.VMEM((3, cols, width), bf16), exchange, exchange, row_f32, pltpu.VMEM((2, rows, width), f32),
                            pltpu.VMEM((rows, pad_heads, length), f32), pltpu.VMEM((rows, pad_heads, length), bf16),
                            pltpu.VMEM((rows, pad_heads, LANES), f32), row_f32,
                            pltpu.VMEM((width - MXU_HEADS * head_dim, LANES), f32),
                            dma((20 + 2 * PIECES,)), dma((5,)), dma((5,)), dma((3,)), dma((6, 3)), dma((3,))],
            compiler_params=pltpu.CompilerParams(collective_id=0, has_side_effects=True, vmem_limit_bytes=40 << 19),
            name='gather')(*(hbm(x) for x in operands))
        h2, xall, eid_all, wr_all, kt, vt, *caches = gathered

        part, gate, new_k, new_v, *_ = pl.pallas_call(
            functools.partial(update_kernel, n, capacity),
            out_shape=(pltpu.VMEM((n, rows, width), f32), pltpu.VMEM((rows, LANES), f32),
                       pltpu.HBM(sk.shape, bf16), pltpu.HBM(sv.shape, bf16), *pieces),
            in_specs=[SMEM] + [VMEM] * (7 + len(pieces)),
            out_specs=(VMEM, VMEM, HBM, HBM) + (VMEM,) * len(pieces),
            input_output_aliases={8 + t: 4 + t for t in range(len(pieces))},
            scratch_shapes=[pltpu.VMEM((group_rows, experts * units), bf16), dma((2,))],
            compiler_params=pltpu.CompilerParams(vmem_limit_bytes=10 << 19),
            name='attend')(positions, kt, vt, xall, eid_all, wr_all, w_in, w_out, *caches)

        hidden_out = pl.pallas_call(
            functools.partial(reduce_kernel, n),
            out_shape=jax.ShapeDtypeStruct((rows, width), bf16),
            in_specs=[VMEM] * 3,
            out_specs=VMEM,
            scratch_shapes=[pltpu.VMEM((4, rows, width), f32), pltpu.VMEM((3, rows, width), f32),
                            pltpu.VMEM((3, rows, width), f32), dma((4,)), dma((4,)), dma((3,)), dma((3,))],
            compiler_params=pltpu.CompilerParams(collective_id=1, has_side_effects=True, vmem_limit_bytes=4 << 20),
            name='experts')(part, gate, h2)

        def unflat(cache):
            return cache.reshape(rows, heads, head_dim, cache.shape[2]).transpose(0, 1, 3, 2)

        return hidden_out, unflat(new_k), unflat(new_v)

    return jax.shard_map(decoder_block, mesh=mesh, in_specs=in_specs, out_specs=out_specs, check_vma=False)
```

```python
import functools
import jax
import jax.numpy as jnp
from jax import lax
from jax.sharding import PartitionSpec as P
from jax.experimental import pallas as pl
from jax.experimental.pallas import tpu as pltpu

EPSILON = 1e-6
NEG_BIG = -1e30
LANES = 128
GROUP = 4
SOFTMAX_GROUP = 8
BIAS_GROUP = 4
MXU_HEADS = 6
UPDATE = 4
READY = 4
PIECES = 2
NT = (((1,), (1,)), ((), ()))
MESH = pl.DeviceIdType.MESH
VMEM = pl.BlockSpec(memory_space=pltpu.VMEM)
HBM = pl.BlockSpec(memory_space=pltpu.HBM)
SMEM = pl.BlockSpec(memory_space=pltpu.SMEM)


def hbm(x):
    return pltpu.with_memory_space_constraint(x, pltpu.HBM)


def rms_norm(hidden, scale):
    hid_f32 = hidden.astype(jnp.float32)
    inv_rms = lax.rsqrt(jnp.mean(hid_f32 * hid_f32, axis=-1, keepdims=True) + EPSILON)
    return (hid_f32 * inv_rms * scale).astype(jnp.bfloat16)


def entry_barrier(me, n):
    barrier = pltpu.get_barrier_semaphore()
    for k in range(1, n):
        pl.semaphore_signal(barrier, inc=1, device_id={'ws': lax.rem(me + k, n)}, device_id_type=MESH)
    pl.semaphore_wait(barrier, n - 1)


def neighbours(me):
    core, xpos, ypos = lax.rem(me, 2), lax.rem(me // 2, 2), me // 4
    other, across_x, across_y = 1 - 2 * core, 2 - 4 * xpos, 4 - 8 * ypos
    xnb, ynb, diag = me + across_x, me + across_y, me + across_x + across_y
    far_first = [diag, diag + other, xnb, ynb, xnb + other, ynb + other, me + other]
    return me + other, xnb, ynb, diag, far_first


def remote(src, dst, send_sem, recv_sem, peer):
    return pltpu.make_async_remote_copy(src_ref=src, dst_ref=dst, send_sem=send_sem, recv_sem=recv_sem,
                                        device_id={'ws': peer}, device_id_type=MESH)


def reverse_lanes(x):
    size = x.shape[-1]
    lane = lax.broadcasted_iota(jnp.int32, x.shape, 1)
    step = 1
    while step < size:
        x = jnp.where((lane & step) != 0, pltpu.roll(x, step, 1), pltpu.roll(x, size - step, 1))
        step *= 2
    return x


def head_mask_of(heads, width, head_dim):
    lane = lax.broadcasted_iota(jnp.int32, (heads, width), 1)
    return lane // head_dim == lax.broadcasted_iota(jnp.int32, (heads, width), 0)


def project(x, w):
    return lax.dot_general(x, w, NT, preferred_element_type=jnp.float32)


def gather_kernel(n, head_dim, hid, pos, eid, mask, ln_s, ln_c, ln_f, bias, wr, wq, wk, wv, wo, wqc, woc,
                  sk, sv, ck, cv,
                  h2_out, xall, eid_all, wr_all, *rest):
    (kt_out, vt_out), self_kv = rest[:2], rest[2:2 * PIECES + 2]
    (ck_v, cv_v, wo_all, wqc_all, woc_all, hid_v, pos_s, eid_s, mask_v, ln_sv, ln_cv, ln_fv, bias_v, hall, wqkv, snd, qkv,
     q_sc, kv_out, s_sc, p_sc, pn_sc, ctx_sc, col_sc, loc_sem, send, recv, sw, rw, rp) = rest[2 * PIECES + 2:]
    me = lax.axis_index('ws')
    rows, width = hid.shape
    cols = wq.shape[0]
    heads, length = s_sc.shape[1:]
    src_len = ck.shape[2]
    piece = rows // PIECES
    f32, bf16 = jnp.float32, jnp.bfloat16
    pair, xnb, ynb, diag, peers = neighbours(me)

    count = []

    def local(src, dst):
        copy = pltpu.make_async_copy(src, dst, loc_sem.at[len(count)])
        copy.start()
        count.append(copy)
        return copy

    small = [local(hid, hid_v), local(wr, wr_all.at[me]), local(eid, eid_s), local(pos, pos_s), local(bias, bias_v),
             local(ln_s, ln_sv.at[0]), local(ln_c, ln_cv.at[0]), local(ln_f, ln_fv.at[0]), local(mask, mask_v)]
    proj = [local(w, wqkv.at[i]) for i, w in enumerate((wq, wk, wv))]
    entry_barrier(me, n)
    for c in small:
        c.wait()
    first = [remote(hid_v, hall.at[me], send.at[0], recv.at[0], p) for p in peers]
    others = pl.ds(0, n - 1)

    def all_of(ref, i):
        return remote(ref.at[others], ref.at[others], send.at[i], recv.at[i], peers[0])

    for c in first:
        c.start()

    fulls = ((wo, wo_all), (wqc, wqc_all), (woc, woc_all))
    half = cols // 2
    own_copies = []
    moves = {}

    def move(name, i, src_dev, lo, size, sem, peer, src=None):
        dst = fulls[i][1].at[pl.ds(pl.multiple_of(src_dev * cols + lo, half), size)]
        moves[name, i] = remote(dst if src is None else src, dst, sw.at[i], sem, peer)
        moves[name, i].start()

    def own_share(i):
        src, dst = fulls[i]
        upper, lower = src.at[pl.ds(0, half)], src.at[pl.ds(half, half)]
        move('x0', i, me, 0, half, rw.at[0, i], xnb, upper)
        move('y1', i, me, half, half, rw.at[1, i], ynb, lower)
        move('x1', i, me, half, half, rw.at[2, i], xnb, lower)
        move('y0', i, me, 0, half, rw.at[3, i], ynb, upper)
        move('pair', i, me, 0, cols, rp.at[i], pair, src)
        own_copies.append(local(src, dst.at[pl.ds(pl.multiple_of(me * cols, cols), cols)]))

    load_self = [local(src.at[pl.ds(t * piece, piece)], self_kv[i * PIECES + t])
                 for i, src in enumerate((sk, sv)) for t in range(PIECES)]
    load_cross = [local(ck, ck_v), local(cv.at[pl.ds(0, piece)], cv_v)]
    hall[me] = hid_v[...]
    col_sc[...] = jnp.zeros_like(col_sc)
    for r in range(rows):
        eid_all[me, r:r + 1, :] = jnp.full((1, LANES), eid_s[r], jnp.int32)

    own_share(0)
    key_pos = lax.broadcasted_iota(jnp.int32, (1, length), 1)
    table = reverse_lanes(jnp.concatenate(
        [bias_v[...], jnp.zeros((heads - bias_v.shape[0], length), f32)], axis=0))

    @pl.loop(0, rows // BIAS_GROUP)
    def _(i):
        marks = [jnp.full((1, length), pos_s[i * BIAS_GROUP + j], jnp.int32) for j in range(BIAS_GROUP)]
        turned, step = [table] * BIAS_GROUP, 1
        while step < length:
            turned = [jnp.where(((p + 1) & step) != 0, pltpu.roll(t, step, 1), t) for p, t in zip(marks, turned)]
            step *= 2
        for j in range(BIAS_GROUP):
            s_sc[i * BIAS_GROUP + j] = jnp.where(key_pos <= marks[j], turned[j], NEG_BIG)

    all_of(hall, 0).wait_recv()
    for c in proj:
        c.wait()
    x_norm = rms_norm(hall[...].reshape(n * rows, width), ln_sv[...])
    for i in range(3):
        snd[:, i] = project(x_norm, wqkv[i]).astype(bf16).reshape(n, rows, cols)
    second = [remote(snd.at[p], qkv.at[me], send.at[3], recv.at[3], p) for p in peers]
    for c in second:
        c.start()
    qkv[me] = snd[me]
    own_share(1)

    def relay(i):
        moves['x0', i].wait_recv()
        move('ry', i, xnb, 0, half, rw.at[4, i], ynb)
        moves['y1', i].wait_recv()
        move('rx', i, ynb, half, half, rw.at[5, i], xnb)
        move('p0', i, xnb, 0, half, rp.at[i], pair)
        move('p1', i, ynb, half, half, rp.at[i], pair)

    def relay_rest(i):
        moves['x1', i].wait_recv()
        move('p2', i, xnb, half, half, rp.at[i], pair)
        moves['y0', i].wait_recv()
        move('p3', i, ynb, 0, half, rp.at[i], pair)

    def relay_diag(i):
        moves['ry', i].wait_recv()
        move('p4', i, diag, 0, half, rp.at[i], pair)
        moves['rx', i].wait_recv()
        move('p5', i, diag, half, half, rp.at[i], pair)

    def wait_weight(i):
        theirs = fulls[i][1].at[pl.ds(0, 4 * cols)]
        remote(theirs, theirs, sw.at[i], rp.at[i], pair).wait_recv()
        own_copies[i].wait()

    all_of(qkv, 3).wait_recv()
    for c in load_self[:PIECES]:
        c.wait()

    def assemble(i):
        return jnp.concatenate([qkv[p, i].astype(f32) for p in range(n)], axis=1)

    q_sc[...] = assemble(0)
    kv_out[0] = assemble(1)
    kv_out[1] = assemble(2)
    head_mask = head_mask_of(heads, width, head_dim)

    def over_rows(lo, hi, body, group=GROUP):
        @pl.loop(0, (hi - lo) // group)
        def _(i):
            for j in range(group):
                body(lo + i * group + j, i * group + j)

    def softmax(s):
        e = jnp.exp(s - jnp.max(s, axis=-1, keepdims=True))
        return (e / jnp.sum(e, axis=-1, keepdims=True)).astype(bf16)

    split = MXU_HEADS * head_dim
    lane = lax.broadcasted_iota(jnp.int32, (1, LANES), 1)

    def store_context(b, probs, vals, r, new=0.0):
        size = probs.shape[1]
        o = jnp.concatenate([project(probs, vals[r, 0:split]), jnp.zeros((heads, width - split), f32)], axis=1) + new
        ctx_sc[pl.ds(b, 1), :] = jnp.sum(jnp.where(head_mask, o, 0.0), axis=0, keepdims=True)
        weights = probs.astype(f32)
        for lo in range(split, width, head_dim):
            h = lo // head_dim
            terms = vals[r, lo:lo + head_dim].astype(f32) * weights[h:h + 1]
            folded = functools.reduce(jnp.add, [terms[:, c:c + LANES] for c in range(0, size, LANES)])
            column = jnp.sum(folded, axis=1, keepdims=True)
            at = slice(lo - split, lo - split + head_dim)
            col_sc[at] = jnp.where(lane == b, column, col_sc[at])

    def contexts():
        late = col_sc[...].T[0:rows]
        return (ctx_sc[...] + jnp.concatenate([jnp.zeros((rows, split), f32), late], axis=1)).astype(bf16)

    def self_scores(t):
        def body(b, r):
            q = jnp.where(head_mask, q_sc[pl.ds(b, 1), :], 0.0)
            s_new = jnp.sum(q * kv_out[0, pl.ds(b, 1), :], axis=1, keepdims=True)
            s = jnp.dot(q.astype(bf16), self_kv[t][r], preferred_element_type=f32)
            s_sc[b] = jnp.where(key_pos == pos_s[b], s_new, s) + s_sc[b]
        over_rows(t * piece, (t + 1) * piece, body)

    def self_softmax():
        def body(b, r):
            probs = softmax(s_sc[b]).astype(f32)
            hit = key_pos == pos_s[b]
            p_new = jnp.sum(jnp.where(hit, probs, 0.0), axis=1, keepdims=True)
            pn_sc[b] = jnp.broadcast_to(p_new, (heads, LANES))
            p_sc[b] = jnp.where(hit, 0.0, probs).astype(bf16)
        over_rows(0, rows, body, SOFTMAX_GROUP)

    def self_context(t):
        def body(b, r):
            store_context(b, p_sc[b], self_kv[PIECES + t], r, pn_sc[b, :, 0:1] * kv_out[1, pl.ds(b, 1), :])
        over_rows(t * piece, (t + 1) * piece, body)

    relay(0)
    self_scores(0)
    relay(1)
    own_share(2)
    self_scores(1)
    relay_rest(0)
    self_softmax()
    for c in load_self[PIECES:]:
        c.wait()
    self_context(0)
    relay_diag(0)
    relay_rest(1)
    self_context(1)
    relay_diag(1)
    wait_weight(0)
    h1 = (hid_v[...].astype(f32) + project(contexts(), wo_all[...])).astype(bf16)
    relay(2)
    for p in peers:
        remote(eid_all.at[me], eid_all.at[me], send.at[1], recv.at[1], p).start()
        remote(wr_all.at[me], wr_all.at[me], send.at[2], recv.at[2], p).start()

    wait_weight(1)
    q_sc[...] = project(rms_norm(h1, ln_cv[...]), wqc_all[...]).astype(bf16).astype(f32)
    for c in load_cross:
        c.wait()

    def cross_scores(b, r):
        q = jnp.where(head_mask, q_sc[pl.ds(b, 1), :], 0.0).astype(bf16)
        s_sc[b, :, 0:src_len] = (jnp.dot(q, ck_v[b], preferred_element_type=f32)
                                 + jnp.where(mask_v[pl.ds(b, 1), :] == 1, 0.0, NEG_BIG))

    def cross_softmax(b, r):
        p_sc[b, :, 0:src_len] = softmax(s_sc[b, :, 0:src_len])

    def cross_context(b, r):
        store_context(b, p_sc[b, :, 0:src_len], cv_v, b)

    def cross_context_late(b, r):
        store_context(b, p_sc[b, :, 0:src_len], ck_v, r)

    over_rows(0, piece, cross_scores)
    load_late = local(cv.at[pl.ds(piece, piece)], ck_v.at[pl.ds(0, piece)])
    over_rows(piece, rows, cross_scores)
    relay_rest(2)
    over_rows(0, rows, cross_softmax, SOFTMAX_GROUP)
    over_rows(0, piece, cross_context)
    relay_diag(2)
    load_late.wait()
    over_rows(piece, rows, cross_context_late)
    wait_weight(2)
    h2 = (h1.astype(f32) + project(contexts(), woc_all[...])).astype(bf16)
    xall[me] = rms_norm(h2, ln_fv[...])
    h2_out[...] = h2
    third = [remote(xall.at[me], xall.at[me], send.at[4], recv.at[4], p) for p in peers]
    for c in third:
        c.start()
    for i, ref in enumerate((kt_out, vt_out)):
        cols_t = jnp.concatenate([kv_out[i], jnp.zeros((LANES - rows, width), f32)], axis=0).T
        for g in range(rows // UPDATE):
            shifted = cols_t if g == 0 else pltpu.roll(cols_t, LANES - g * UPDATE, 1)
            ref[g] = shifted.astype(bf16)
    for j in range(READY):
        hit = key_pos == pos_s[j]
        for i, ref in enumerate((kt_out, vt_out)):
            cache = self_kv[i * PIECES]
            cache[j] = jnp.where(hit, ref[0, :, j:j + 1], cache[j])
    for i, ref in ((1, eid_all), (2, wr_all), (4, xall)):
        all_of(ref, i).wait_recv()
    for i, ref in enumerate((hall, eid_all, wr_all, snd, xall)):
        all_of(ref, i).wait_send()
    for i in range(3):
        moved = fulls[i][1].at[pl.ds(0, 7 * cols)]
        remote(moved, moved, sw.at[i], rp.at[i], pair).wait_send()


def update_kernel(n, capacity, pos, kt, vt, xall, eid_all, wr_all, win, wout, *rest):
    (part, gate, nk, nv), self_kv, (hidden_sc, out_sem) = (
        rest[2 * PIECES:2 * PIECES + 4], rest[2 * PIECES + 4:-2], rest[-2:])
    me = lax.axis_index('ws')
    _, rows, width = xall.shape
    experts, _, units = win.shape
    group_rows = n * rows
    piece = rows // PIECES
    f32 = jnp.float32
    lane = lax.broadcasted_iota(jnp.int32, (1, LANES), 1)

    for b in range(READY):
        pltpu.make_async_copy(self_kv[0].at[b], nk.at[b], out_sem.at[0]).start()
        pltpu.make_async_copy(self_kv[PIECES].at[b], nv.at[b], out_sem.at[1]).start()

    for t in range(PIECES):
        keys, vals = self_kv[t], self_kv[PIECES + t]

        @pl.loop(READY // UPDATE if t == 0 else 0, piece // UPDATE)
        def _(i):
            g = t * (piece // UPDATE) + i
            def write(j):
                r = i * UPDATE + j
                b = t * piece + r
                pltpu.make_async_copy(keys.at[r], nk.at[b], out_sem.at[0]).start()
                pltpu.make_async_copy(vals.at[r], nv.at[b], out_sem.at[1]).start()

            for j in range(UPDATE):
                r = i * UPDATE + j
                b = t * piece + r
                p = pos[b]
                win_at = pl.ds(pl.multiple_of((p // LANES) * LANES, LANES), LANES)
                hit = lane == p % LANES
                for cache, new in ((keys, kt), (vals, vt)):
                    cache[r, :, win_at] = jnp.where(hit, new[g, :, j:j + 1], cache[r, :, win_at])
                if j:
                    write(j - 1)
            write(UPDATE - 1)

    eid = eid_all[...].reshape(group_rows, LANES)
    eid_col = eid[:, 0:1]
    xs = xall[...].reshape(group_rows, width)
    for e in range(experts):
        u = jnp.dot(xs, win[e], preferred_element_type=f32)
        hidden_sc[:, e * units:(e + 1) * units] = jnp.where(eid_col == e, jnp.maximum(u, 0.0), 0.0).astype(jnp.bfloat16)
    y = jnp.dot(hidden_sc[...], wout[...].reshape(experts * units, width), preferred_element_type=f32)
    part[...] = y.reshape(n, rows, width)

    x_own = xall[me].astype(f32)
    logits = [jnp.sum(x_own * wr_all[e], axis=-1, keepdims=True) for e in range(experts)]
    top = functools.reduce(jnp.maximum, logits)
    exps = [jnp.exp(l - top) for l in logits]
    total = functools.reduce(jnp.add, exps)
    own_col = eid_all[me][:, 0:1]
    chosen = functools.reduce(jnp.add, [jnp.where(own_col == e, exps[e], 0.0) for e in range(experts)])
    across = eid.astype(f32).T[0:1, :].astype(jnp.int32)
    row_ids = me * rows + lax.broadcasted_iota(jnp.int32, (rows, group_rows), 0)
    earlier = (across == own_col) & (lax.broadcasted_iota(jnp.int32, (rows, group_rows), 1) < row_ids)
    slot = jnp.sum(jnp.where(earlier, 1.0, 0.0), axis=1, keepdims=True)
    gate[...] = jnp.broadcast_to(jnp.where(slot < capacity, chosen / total, 0.0), gate.shape)

    for i, ref in enumerate((nk, nv)):
        pltpu.make_async_copy(ref, ref, out_sem.at[i]).wait()


def reduce_kernel(n, part, gate, h2, out, near, mixed, far, s1, r1, s2, r2):
    me = lax.axis_index('ws')
    f32 = jnp.float32
    entry_barrier(me, n)
    _, _, _, _, (diag, diag_o, x_same, y_same, x_o, y_o, pair) = neighbours(me)
    to_pair = [remote(part.at[d], near.at[t], s1.at[t], r1.at[t], pair) for t, d in enumerate((diag, x_same, y_same, pair))]
    for c in to_pair:
        c.start()
    to_far = []
    for t, d in enumerate((diag_o, x_o, y_o)):
        to_pair[t].wait_recv()
        mixed[t] = part[d] + near[t]
        to_far.append(remote(mixed.at[t], far.at[t], s2.at[t], r2.at[t], d))
        to_far[-1].start()
    to_pair[3].wait_recv()
    y_own = part[me] + near[3]
    for t, c in enumerate(to_far):
        c.wait_recv()
        y_own = y_own + far[t]
    out[...] = (h2[...].astype(f32) + y_own.astype(jnp.bfloat16).astype(f32) * gate[:, 0:1]).astype(jnp.bfloat16)
    for c in to_pair + to_far:
        c.wait_send()


def solution(mesh):
    n = mesh.shape['ws']
    row_axes = ('dp', 'ws')
    row_vec = P(row_axes)
    row_mat = P(row_axes, None)
    cache_spec = P(row_axes, None, None, None)
    col_split = P(None, 'ws')
    in_specs = (row_mat, cache_spec, cache_spec, cache_spec, cache_spec, row_vec, row_mat, P(None, None), row_vec,
                P(None), P(None), P(None), col_split, col_split, col_split, col_split, col_split, col_split,
                col_split, P(None, None, 'ws'), P(None, 'ws', None))
    out_specs = (row_mat, cache_spec, cache_spec)

    def decoder_block(hidden, self_k, self_v, cross_k, cross_v, positions, enc_mask, rel_bias, expert_idx,
                      ln_self, ln_cross, ln_ffn, wq_self, wk_self, wv_self, wo_self, wq_cross, wo_cross,
                      w_router, w_in, w_out):
        rows, width = hidden.shape
        heads, head_dim = self_k.shape[1], self_k.shape[3]
        cols = wq_self.shape[1]
        experts, _, units = w_in.shape
        group_rows = rows * n
        capacity = (2 * group_rows + experts - 1) // experts
        bf16, f32, i32 = jnp.bfloat16, jnp.float32, jnp.int32
        pad_heads = 16
        dma = pltpu.SemaphoreType.DMA

        def flat(cache):
            return cache.transpose(0, 1, 3, 2).reshape(rows, heads * head_dim, cache.shape[2])

        sk, sv, ck, cv = (flat(c) for c in (self_k, self_v, cross_k, cross_v))
        pieces = [pltpu.VMEM((rows // PIECES,) + c.shape[1:], bf16) for c in (sk, sv) for _ in range(PIECES)]
        length, src_len = sk.shape[2], ck.shape[2]
        row_bf16, row_f32 = pltpu.VMEM((rows, width), bf16), pltpu.VMEM((rows, width), f32)
        full = pltpu.VMEM((n * cols, width), bf16)
        columns = pltpu.VMEM((rows // UPDATE, width, LANES), bf16)
        ln_row = pltpu.VMEM((1, width), f32)
        index = pltpu.SMEM((rows,), i32)
        exchange = pltpu.VMEM((n, 3, rows, cols), bf16)
        operands = (hidden, positions, expert_idx, enc_mask, ln_self, ln_cross, ln_ffn, rel_bias, w_router.T,
                    wq_self.T, wk_self.T, wv_self.T, wo_self.T, wq_cross.T, wo_cross.T, sk, sv, ck, cv)
        gathered = pl.pallas_call(
            functools.partial(gather_kernel, n, head_dim),
            out_shape=(row_bf16, pltpu.VMEM((n, rows, width), bf16),
                       pltpu.VMEM((n, rows, LANES), i32), pltpu.VMEM((n, 1, width), f32),
                       columns, columns, *pieces),
            in_specs=[HBM] * len(operands),
            out_specs=(VMEM,) * (6 + len(pieces)),
            scratch_shapes=[pltpu.VMEM(ck.shape, bf16), pltpu.VMEM((rows // PIECES,) + cv.shape[1:], bf16), full, full, full,
                            row_bf16, index, index, pltpu.VMEM(enc_mask.shape, i32), ln_row, ln_row, ln_row,
                            pltpu.VMEM(rel_bias.shape, f32), pltpu.VMEM((n, rows, width), bf16),
                            pltpu.VMEM((3, cols, width), bf16), exchange, exchange, row_f32, pltpu.VMEM((2, rows, width), f32),
                            pltpu.VMEM((rows, pad_heads, length), f32), pltpu.VMEM((rows, pad_heads, length), bf16),
                            pltpu.VMEM((rows, pad_heads, LANES), f32), row_f32,
                            pltpu.VMEM((width - MXU_HEADS * head_dim, LANES), f32),
                            dma((20 + 2 * PIECES,)), dma((5,)), dma((5,)), dma((3,)), dma((6, 3)), dma((3,))],
            compiler_params=pltpu.CompilerParams(collective_id=0, has_side_effects=True, vmem_limit_bytes=40 << 19),
            name='gather')(*(hbm(x) for x in operands))
        h2, xall, eid_all, wr_all, kt, vt, *caches = gathered

        part, gate, new_k, new_v, *_ = pl.pallas_call(
            functools.partial(update_kernel, n, capacity),
            out_shape=(pltpu.VMEM((n, rows, width), f32), pltpu.VMEM((rows, LANES), f32),
                       pltpu.HBM(sk.shape, bf16), pltpu.HBM(sv.shape, bf16), *pieces),
            in_specs=[SMEM] + [VMEM] * (7 + len(pieces)),
            out_specs=(VMEM, VMEM, HBM, HBM) + (VMEM,) * len(pieces),
            input_output_aliases={8 + t: 4 + t for t in range(len(pieces))},
            scratch_shapes=[pltpu.VMEM((group_rows, experts * units), bf16), dma((2,))],
            compiler_params=pltpu.CompilerParams(vmem_limit_bytes=10 << 19),
            name='attend')(positions, kt, vt, xall, eid_all, wr_all, w_in, w_out, *caches)

        hidden_out = pl.pallas_call(
            functools.partial(reduce_kernel, n),
            out_shape=jax.ShapeDtypeStruct((rows, width), bf16),
            in_specs=[VMEM] * 3,
            out_specs=VMEM,
            scratch_shapes=[pltpu.VMEM((4, rows, width), f32), pltpu.VMEM((3, rows, width), f32),
                            pltpu.VMEM((3, rows, width), f32), dma((4,)), dma((4,)), dma((3,)), dma((3,))],
            compiler_params=pltpu.CompilerParams(collective_id=1, has_side_effects=True, vmem_limit_bytes=4 << 20),
            name='experts')(part, gate, h2)

        def unflat(cache):
            return cache.reshape(rows, heads, head_dim, cache.shape[2]).transpose(0, 1, 3, 2)

        return hidden_out, unflat(new_k), unflat(new_v)

    return jax.shard_map(decoder_block, mesh=mesh, in_specs=in_specs, out_specs=out_specs, check_vma=False)
```

```python
import functools
import jax
import jax.numpy as jnp
from jax import lax
from jax.sharding import PartitionSpec as P
from jax.experimental import pallas as pl
from jax.experimental.pallas import tpu as pltpu

EPSILON = 1e-6
NEG_BIG = -1e30
LANES = 128
GROUP = 4
SOFTMAX_GROUP = 8
BIAS_GROUP = 4
MXU_HEADS = 6
UPDATE = 4
READY = 4
PIECES = 2
NT = (((1,), (1,)), ((), ()))
MESH = pl.DeviceIdType.MESH
VMEM = pl.BlockSpec(memory_space=pltpu.VMEM)
HBM = pl.BlockSpec(memory_space=pltpu.HBM)
SMEM = pl.BlockSpec(memory_space=pltpu.SMEM)


def hbm(x):
    return pltpu.with_memory_space_constraint(x, pltpu.HBM)


def rms_norm(hidden, scale):
    hid_f32 = hidden.astype(jnp.float32)
    inv_rms = lax.rsqrt(jnp.mean(hid_f32 * hid_f32, axis=-1, keepdims=True) + EPSILON)
    return (hid_f32 * inv_rms * scale).astype(jnp.bfloat16)


def entry_barrier(me, n):
    barrier = pltpu.get_barrier_semaphore()
    for k in range(1, n):
        pl.semaphore_signal(barrier, inc=1, device_id={'ws': lax.rem(me + k, n)}, device_id_type=MESH)
    pl.semaphore_wait(barrier, n - 1)


def neighbours(me):
    core, xpos, ypos = lax.rem(me, 2), lax.rem(me // 2, 2), me // 4
    other, across_x, across_y = 1 - 2 * core, 2 - 4 * xpos, 4 - 8 * ypos
    xnb, ynb, diag = me + across_x, me + across_y, me + across_x + across_y
    far_first = [diag, diag + other, xnb, ynb, xnb + other, ynb + other, me + other]
    return me + other, xnb, ynb, diag, far_first


def remote(src, dst, send_sem, recv_sem, peer):
    return pltpu.make_async_remote_copy(src_ref=src, dst_ref=dst, send_sem=send_sem, recv_sem=recv_sem,
                                        device_id={'ws': peer}, device_id_type=MESH)


def reverse_lanes(x):
    size = x.shape[-1]
    lane = lax.broadcasted_iota(jnp.int32, x.shape, 1)
    step = 1
    while step < size:
        x = jnp.where((lane & step) != 0, pltpu.roll(x, step, 1), pltpu.roll(x, size - step, 1))
        step *= 2
    return x


def head_mask_of(heads, width, head_dim):
    lane = lax.broadcasted_iota(jnp.int32, (heads, width), 1)
    return lane // head_dim == lax.broadcasted_iota(jnp.int32, (heads, width), 0)


def project(x, w):
    return lax.dot_general(x, w, NT, preferred_element_type=jnp.float32)


def gather_kernel(n, head_dim, hid, pos, eid, mask, ln_s, ln_c, ln_f, bias, wr, wq, wk, wv, wo, wqc, woc,
                  sk, sv, ck, cv,
                  h2_out, xall, eid_all, wr_all, *rest):
    (kt_out, vt_out), self_kv = rest[:2], rest[2:2 * PIECES + 2]
    (ck_v, cv_v, wo_all, wqc_all, woc_all, hid_v, pos_s, eid_s, mask_v, ln_sv, ln_cv, ln_fv, bias_v, hall, wqkv, snd, qkv,
     q_sc, kv_out, s_sc, p_sc, pn_sc, ctx_sc, col_sc, loc_sem, send, recv, sw, rw, rp) = rest[2 * PIECES + 2:]
    me = lax.axis_index('ws')
    rows, width = hid.shape
    cols = wq.shape[0]
    heads, length = s_sc.shape[1:]
    src_len = ck.shape[2]
    piece = rows // PIECES
    f32, bf16 = jnp.float32, jnp.bfloat16
    pair, xnb, ynb, diag, peers = neighbours(me)

    count = []

    def local(src, dst):
        copy = pltpu.make_async_copy(src, dst, loc_sem.at[len(count)])
        copy.start()
        count.append(copy)
        return copy

    small = [local(hid, hid_v), local(wr, wr_all.at[me]), local(eid, eid_s), local(pos, pos_s), local(bias, bias_v),
             local(ln_s, ln_sv.at[0]), local(ln_c, ln_cv.at[0]), local(ln_f, ln_fv.at[0]), local(mask, mask_v)]
    proj = [local(w, wqkv.at[i]) for i, w in enumerate((wq, wk, wv))]
    entry_barrier(me, n)
    for c in small:
        c.wait()
    first = [remote(hid_v, hall.at[me], send.at[0], recv.at[0], p) for p in peers]
    others = pl.ds(0, n - 1)

    def all_of(ref, i):
        return remote(ref.at[others], ref.at[others], send.at[i], recv.at[i], peers[0])

    for c in first:
        c.start()

    fulls = ((wo, wo_all), (wqc, wqc_all), (woc, woc_all))
    half = cols // 2
    own_copies = []
    moves = {}

    def move(name, i, src_dev, lo, size, sem, peer, src=None):
        dst = fulls[i][1].at[pl.ds(pl.multiple_of(src_dev * cols + lo, half), size)]
        moves[name, i] = remote(dst if src is None else src, dst, sw.at[i], sem, peer)
        moves[name, i].start()

    def own_share(i):
        src, dst = fulls[i]
        upper, lower = src.at[pl.ds(0, half)], src.at[pl.ds(half, half)]
        move('x0', i, me, 0, half, rw.at[0, i], xnb, upper)
        move('y1', i, me, half, half, rw.at[1, i], ynb, lower)
        move('x1', i, me, half, half, rw.at[2, i], xnb, lower)
        move('y0', i, me, 0, half, rw.at[3, i], ynb, upper)
        move('pair', i, me, 0, cols, rp.at[i], pair, src)
        own_copies.append(local(src, dst.at[pl.ds(pl.multiple_of(me * cols, cols), cols)]))

    load_self = [local(src.at[pl.ds(t * piece, piece)], self_kv[i * PIECES + t])
                 for i, src in enumerate((sk, sv)) for t in range(PIECES)]
    load_cross = [local(ck, ck_v), local(cv.at[pl.ds(0, piece)], cv_v)]
    hall[me] = hid_v[...]
    col_sc[...] = jnp.zeros_like(col_sc)
    for r in range(rows):
        eid_all[me, r:r + 1, :] = jnp.full((1, LANES), eid_s[r], jnp.int32)

    own_share(0)
    key_pos = lax.broadcasted_iota(jnp.int32, (1, length), 1)
    table = reverse_lanes(jnp.concatenate(
        [bias_v[...], jnp.zeros((heads - bias_v.shape[0], length), f32)], axis=0))

    @pl.loop(0, rows // BIAS_GROUP)
    def _(i):
        marks = [jnp.full((1, length), pos_s[i * BIAS_GROUP + j], jnp.int32) for j in range(BIAS_GROUP)]
        turned, step = [table] * BIAS_GROUP, 1
        while step < length:
            turned = [jnp.where(((p + 1) & step) != 0, pltpu.roll(t, step, 1), t) for p, t in zip(marks, turned)]
            step *= 2
        for j in range(BIAS_GROUP):
            s_sc[i * BIAS_GROUP + j] = jnp.where(key_pos <= marks[j], turned[j], NEG_BIG)

    all_of(hall, 0).wait_recv()
    for c in proj:
        c.wait()
    x_norm = rms_norm(hall[...].reshape(n * rows, width), ln_sv[...])
    for i in range(3):
        snd[:, i] = project(x_norm, wqkv[i]).astype(bf16).reshape(n, rows, cols)
    second = [remote(snd.at[p], qkv.at[me], send.at[3], recv.at[3], p) for p in peers]
    for c in second:
        c.start()
    qkv[me] = snd[me]
    own_share(1)

    def relay(i):
        moves['x0', i].wait_recv()
        move('ry', i, xnb, 0, half, rw.at[4, i], ynb)
        moves['y1', i].wait_recv()
        move('rx', i, ynb, half, half, rw.at[5, i], xnb)
        move('p0', i, xnb, 0, half, rp.at[i], pair)
        move('p1', i, ynb, half, half, rp.at[i], pair)

    def relay_rest(i):
        moves['x1', i].wait_recv()
        move('p2', i, xnb, half, half, rp.at[i], pair)
        moves['y0', i].wait_recv()
        move('p3', i, ynb, 0, half, rp.at[i], pair)

    def relay_diag(i):
        moves['ry', i].wait_recv()
        move('p4', i, diag, 0, half, rp.at[i], pair)
        moves['rx', i].wait_recv()
        move('p5', i, diag, half, half, rp.at[i], pair)

    def wait_weight(i):
        theirs = fulls[i][1].at[pl.ds(0, 4 * cols)]
        remote(theirs, theirs, sw.at[i], rp.at[i], pair).wait_recv()
        own_copies[i].wait()

    all_of(qkv, 3).wait_recv()
    for c in load_self[:PIECES]:
        c.wait()

    def assemble(i):
        return jnp.concatenate([qkv[p, i].astype(f32) for p in range(n)], axis=1)

    q_sc[...] = assemble(0)
    kv_out[0] = assemble(1)
    kv_out[1] = assemble(2)
    head_mask = head_mask_of(heads, width, head_dim)

    def over_rows(lo, hi, body, group=GROUP):
        @pl.loop(0, (hi - lo) // group)
        def _(i):
            for j in range(group):
                body(lo + i * group + j, i * group + j)

    def softmax(s):
        e = jnp.exp(s - jnp.max(s, axis=-1, keepdims=True))
        return (e / jnp.sum(e, axis=-1, keepdims=True)).astype(bf16)

    split = MXU_HEADS * head_dim
    lane = lax.broadcasted_iota(jnp.int32, (1, LANES), 1)

    def store_context(b, probs, vals, r, new=0.0):
        size = probs.shape[1]
        o = jnp.concatenate([project(probs, vals[r, 0:split]), jnp.zeros((heads, width - split), f32)], axis=1) + new
        ctx_sc[pl.ds(b, 1), :] = jnp.sum(jnp.where(head_mask, o, 0.0), axis=0, keepdims=True)
        weights = probs.astype(f32)
        for lo in range(split, width, head_dim):
            h = lo // head_dim
            terms = vals[r, lo:lo + head_dim].astype(f32) * weights[h:h + 1]
            folded = functools.reduce(jnp.add, [terms[:, c:c + LANES] for c in range(0, size, LANES)])
            column = jnp.sum(folded, axis=1, keepdims=True)
            at = slice(lo - split, lo - split + head_dim)
            col_sc[at] = jnp.where(lane == b, column, col_sc[at])

    def contexts():
        late = col_sc[...].T[0:rows]
        return (ctx_sc[...] + jnp.concatenate([jnp.zeros((rows, split), f32), late], axis=1)).astype(bf16)

    def self_scores(t):
        def body(b, r):
            q = jnp.where(head_mask, q_sc[pl.ds(b, 1), :], 0.0)
            s_new = jnp.sum(q * kv_out[0, pl.ds(b, 1), :], axis=1, keepdims=True)
            s = jnp.dot(q.astype(bf16), self_kv[t][r], preferred_element_type=f32)
            s_sc[b] = jnp.where(key_pos == pos_s[b], s_new, s) + s_sc[b]
        over_rows(t * piece, (t + 1) * piece, body)

    def self_softmax():
        def body(b, r):
            probs = softmax(s_sc[b]).astype(f32)
            hit = key_pos == pos_s[b]
            p_new = jnp.sum(jnp.where(hit, probs, 0.0), axis=1, keepdims=True)
            pn_sc[b] = jnp.broadcast_to(p_new, (heads, LANES))
            p_sc[b] = jnp.where(hit, 0.0, probs).astype(bf16)
        over_rows(0, rows, body, SOFTMAX_GROUP)

    def self_context(t):
        def body(b, r):
            store_context(b, p_sc[b], self_kv[PIECES + t], r, pn_sc[b, :, 0:1] * kv_out[1, pl.ds(b, 1), :])
        over_rows(t * piece, (t + 1) * piece, body)

    relay(0)
    self_scores(0)
    relay(1)
    own_share(2)
    self_scores(1)
    relay_rest(0)
    self_softmax()
    for c in load_self[PIECES:]:
        c.wait()
    self_context(0)
    relay_diag(0)
    relay_rest(1)
    self_context(1)
    relay_diag(1)
    wait_weight(0)
    h1 = (hid_v[...].astype(f32) + project(contexts(), wo_all[...])).astype(bf16)
    relay(2)

    wait_weight(1)
    q_sc[...] = project(rms_norm(h1, ln_cv[...]), wqc_all[...]).astype(bf16).astype(f32)
    for c in load_cross:
        c.wait()

    def cross_scores(b, r):
        q = jnp.where(head_mask, q_sc[pl.ds(b, 1), :], 0.0).astype(bf16)
        s_sc[b, :, 0:src_len] = (jnp.dot(q, ck_v[b], preferred_element_type=f32)
                                 + jnp.where(mask_v[pl.ds(b, 1), :] == 1, 0.0, NEG_BIG))

    def cross_softmax(b, r):
        p_sc[b, :, 0:src_len] = softmax(s_sc[b, :, 0:src_len])

    def cross_context(b, r):
        store_context(b, p_sc[b, :, 0:src_len], cv_v, b)

    def cross_context_late(b, r):
        store_context(b, p_sc[b, :, 0:src_len], ck_v, r)

    over_rows(0, piece, cross_scores)
    load_late = local(cv.at[pl.ds(piece, piece)], ck_v.at[pl.ds(0, piece)])
    over_rows(piece, rows, cross_scores)
    relay_rest(2)
    for p in peers:
        remote(eid_all.at[me], eid_all.at[me], send.at[1], recv.at[1], p).start()
        remote(wr_all.at[me], wr_all.at[me], send.at[2], recv.at[2], p).start()
    over_rows(0, rows, cross_softmax, SOFTMAX_GROUP)
    over_rows(0, piece, cross_context)
    relay_diag(2)
    load_late.wait()
    over_rows(piece, rows, cross_context_late)
    wait_weight(2)
    h2 = (h1.astype(f32) + project(contexts(), woc_all[...])).astype(bf16)
    xall[me] = rms_norm(h2, ln_fv[...])
    h2_out[...] = h2
    third = [remote(xall.at[me], xall.at[me], send.at[4], recv.at[4], p) for p in peers]
    for c in third:
        c.start()
    for i, ref in enumerate((kt_out, vt_out)):
        cols_t = jnp.concatenate([kv_out[i], jnp.zeros((LANES - rows, width), f32)], axis=0).T
        for g in range(rows // UPDATE):
            shifted = cols_t if g == 0 else pltpu.roll(cols_t, LANES - g * UPDATE, 1)
            ref[g] = shifted.astype(bf16)
    for j in range(READY):
        hit = key_pos == pos_s[j]
        for i, ref in enumerate((kt_out, vt_out)):
            cache = self_kv[i * PIECES]
            cache[j] = jnp.where(hit, ref[0, :, j:j + 1], cache[j])
    for i, ref in ((1, eid_all), (2, wr_all), (4, xall)):
        all_of(ref, i).wait_recv()
    for i, ref in enumerate((hall, eid_all, wr_all, snd, xall)):
        all_of(ref, i).wait_send()
    for i in range(3):
        moved = fulls[i][1].at[pl.ds(0, 7 * cols)]
        remote(moved, moved, sw.at[i], rp.at[i], pair).wait_send()


def update_kernel(n, capacity, pos, kt, vt, xall, eid_all, wr_all, win, wout, *rest):
    (part, gate, nk, nv), self_kv, (hidden_sc, out_sem) = (
        rest[2 * PIECES:2 * PIECES + 4], rest[2 * PIECES + 4:-2], rest[-2:])
    me = lax.axis_index('ws')
    _, rows, width = xall.shape
    experts, _, units = win.shape
    group_rows = n * rows
    piece = rows // PIECES
    f32 = jnp.float32
    lane = lax.broadcasted_iota(jnp.int32, (1, LANES), 1)

    for b in range(READY):
        pltpu.make_async_copy(self_kv[0].at[b], nk.at[b], out_sem.at[0]).start()
        pltpu.make_async_copy(self_kv[PIECES].at[b], nv.at[b], out_sem.at[1]).start()

    for t in range(PIECES):
        keys, vals = self_kv[t], self_kv[PIECES + t]

        @pl.loop(READY // UPDATE if t == 0 else 0, piece // UPDATE)
        def _(i):
            g = t * (piece // UPDATE) + i
            def write(j):
                r = i * UPDATE + j
                b = t * piece + r
                pltpu.make_async_copy(keys.at[r], nk.at[b], out_sem.at[0]).start()
                pltpu.make_async_copy(vals.at[r], nv.at[b], out_sem.at[1]).start()

            for j in range(UPDATE):
                r = i * UPDATE + j
                b = t * piece + r
                p = pos[b]
                win_at = pl.ds(pl.multiple_of((p // LANES) * LANES, LANES), LANES)
                hit = lane == p % LANES
                for cache, new in ((keys, kt), (vals, vt)):
                    cache[r, :, win_at] = jnp.where(hit, new[g, :, j:j + 1], cache[r, :, win_at])
                if j:
                    write(j - 1)
            write(UPDATE - 1)

    eid = eid_all[...].reshape(group_rows, LANES)
    eid_col = eid[:, 0:1]
    xs = xall[...].reshape(group_rows, width)
    for e in range(experts):
        u = jnp.dot(xs, win[e], preferred_element_type=f32)
        hidden_sc[:, e * units:(e + 1) * units] = jnp.where(eid_col == e, jnp.maximum(u, 0.0), 0.0).astype(jnp.bfloat16)
    y = jnp.dot(hidden_sc[...], wout[...].reshape(experts * units, width), preferred_element_type=f32)
    part[...] = y.reshape(n, rows, width)

    x_own = xall[me].astype(f32)
    logits = [jnp.sum(x_own * wr_all[e], axis=-1, keepdims=True) for e in range(experts)]
    top = functools.reduce(jnp.maximum, logits)
    exps = [jnp.exp(l - top) for l in logits]
    total = functools.reduce(jnp.add, exps)
    own_col = eid_all[me][:, 0:1]
    chosen = functools.reduce(jnp.add, [jnp.where(own_col == e, exps[e], 0.0) for e in range(experts)])
    across = eid.astype(f32).T[0:1, :].astype(jnp.int32)
    row_ids = me * rows + lax.broadcasted_iota(jnp.int32, (rows, group_rows), 0)
    earlier = (across == own_col) & (lax.broadcasted_iota(jnp.int32, (rows, group_rows), 1) < row_ids)
    slot = jnp.sum(jnp.where(earlier, 1.0, 0.0), axis=1, keepdims=True)
    gate[...] = jnp.broadcast_to(jnp.where(slot < capacity, chosen / total, 0.0), gate.shape)

    for i, ref in enumerate((nk, nv)):
        pltpu.make_async_copy(ref, ref, out_sem.at[i]).wait()


def reduce_kernel(n, part, gate, h2, out, near, mixed, far, s1, r1, s2, r2):
    me = lax.axis_index('ws')
    f32 = jnp.float32
    entry_barrier(me, n)
    _, _, _, _, (diag, diag_o, x_same, y_same, x_o, y_o, pair) = neighbours(me)
    to_pair = [remote(part.at[d], near.at[t], s1.at[t], r1.at[t], pair) for t, d in enumerate((diag, x_same, y_same, pair))]
    for c in to_pair:
        c.start()
    to_far = []
    for t, d in enumerate((diag_o, x_o, y_o)):
        to_pair[t].wait_recv()
        mixed[t] = part[d] + near[t]
        to_far.append(remote(mixed.at[t], far.at[t], s2.at[t], r2.at[t], d))
        to_far[-1].start()
    to_pair[3].wait_recv()
    y_own = part[me] + near[3]
    for t, c in enumerate(to_far):
        c.wait_recv()
        y_own = y_own + far[t]
    out[...] = (h2[...].astype(f32) + y_own.astype(jnp.bfloat16).astype(f32) * gate[:, 0:1]).astype(jnp.bfloat16)
    for c in to_pair + to_far:
        c.wait_send()


def solution(mesh):
    n = mesh.shape['ws']
    row_axes = ('dp', 'ws')
    row_vec = P(row_axes)
    row_mat = P(row_axes, None)
    cache_spec = P(row_axes, None, None, None)
    col_split = P(None, 'ws')
    in_specs = (row_mat, cache_spec, cache_spec, cache_spec, cache_spec, row_vec, row_mat, P(None, None), row_vec,
                P(None), P(None), P(None), col_split, col_split, col_split, col_split, col_split, col_split,
                col_split, P(None, None, 'ws'), P(None, 'ws', None))
    out_specs = (row_mat, cache_spec, cache_spec)

    def decoder_block(hidden, self_k, self_v, cross_k, cross_v, positions, enc_mask, rel_bias, expert_idx,
                      ln_self, ln_cross, ln_ffn, wq_self, wk_self, wv_self, wo_self, wq_cross, wo_cross,
                      w_router, w_in, w_out):
        rows, width = hidden.shape
        heads, head_dim = self_k.shape[1], self_k.shape[3]
        cols = wq_self.shape[1]
        experts, _, units = w_in.shape
        group_rows = rows * n
        capacity = (2 * group_rows + experts - 1) // experts
        bf16, f32, i32 = jnp.bfloat16, jnp.float32, jnp.int32
        pad_heads = 16
        dma = pltpu.SemaphoreType.DMA

        def flat(cache):
            return cache.transpose(0, 1, 3, 2).reshape(rows, heads * head_dim, cache.shape[2])

        sk, sv, ck, cv = (flat(c) for c in (self_k, self_v, cross_k, cross_v))
        pieces = [pltpu.VMEM((rows // PIECES,) + c.shape[1:], bf16) for c in (sk, sv) for _ in range(PIECES)]
        length, src_len = sk.shape[2], ck.shape[2]
        row_bf16, row_f32 = pltpu.VMEM((rows, width), bf16), pltpu.VMEM((rows, width), f32)
        full = pltpu.VMEM((n * cols, width), bf16)
        columns = pltpu.VMEM((rows // UPDATE, width, LANES), bf16)
        ln_row = pltpu.VMEM((1, width), f32)
        index = pltpu.SMEM((rows,), i32)
        exchange = pltpu.VMEM((n, 3, rows, cols), bf16)
        operands = (hidden, positions, expert_idx, enc_mask, ln_self, ln_cross, ln_ffn, rel_bias, w_router.T,
                    wq_self.T, wk_self.T, wv_self.T, wo_self.T, wq_cross.T, wo_cross.T, sk, sv, ck, cv)
        gathered = pl.pallas_call(
            functools.partial(gather_kernel, n, head_dim),
            out_shape=(row_bf16, pltpu.VMEM((n, rows, width), bf16),
                       pltpu.VMEM((n, rows, LANES), i32), pltpu.VMEM((n, 1, width), f32),
                       columns, columns, *pieces),
            in_specs=[HBM] * len(operands),
            out_specs=(VMEM,) * (6 + len(pieces)),
            scratch_shapes=[pltpu.VMEM(ck.shape, bf16), pltpu.VMEM((rows // PIECES,) + cv.shape[1:], bf16), full, full, full,
                            row_bf16, index, index, pltpu.VMEM(enc_mask.shape, i32), ln_row, ln_row, ln_row,
                            pltpu.VMEM(rel_bias.shape, f32), pltpu.VMEM((n, rows, width), bf16),
                            pltpu.VMEM((3, cols, width), bf16), exchange, exchange, row_f32, pltpu.VMEM((2, rows, width), f32),
                            pltpu.VMEM((rows, pad_heads, length), f32), pltpu.VMEM((rows, pad_heads, length), bf16),
                            pltpu.VMEM((rows, pad_heads, LANES), f32), row_f32,
                            pltpu.VMEM((width - MXU_HEADS * head_dim, LANES), f32),
                            dma((20 + 2 * PIECES,)), dma((5,)), dma((5,)), dma((3,)), dma((6, 3)), dma((3,))],
            compiler_params=pltpu.CompilerParams(collective_id=0, has_side_effects=True, vmem_limit_bytes=40 << 19),
            name='gather')(*(hbm(x) for x in operands))
        h2, xall, eid_all, wr_all, kt, vt, *caches = gathered

        part, gate, new_k, new_v, *_ = pl.pallas_call(
            functools.partial(update_kernel, n, capacity),
            out_shape=(pltpu.VMEM((n, rows, width), f32), pltpu.VMEM((rows, LANES), f32),
                       pltpu.HBM(sk.shape, bf16), pltpu.HBM(sv.shape, bf16), *pieces),
            in_specs=[SMEM] + [VMEM] * (7 + len(pieces)),
            out_specs=(VMEM, VMEM, HBM, HBM) + (VMEM,) * len(pieces),
            input_output_aliases={8 + t: 4 + t for t in range(len(pieces))},
            scratch_shapes=[pltpu.VMEM((group_rows, experts * units), bf16), dma((2,))],
            compiler_params=pltpu.CompilerParams(vmem_limit_bytes=10 << 19),
            name='attend')(positions, kt, vt, xall, eid_all, wr_all, w_in, w_out, *caches)

        hidden_out = pl.pallas_call(
            functools.partial(reduce_kernel, n),
            out_shape=jax.ShapeDtypeStruct((rows, width), bf16),
            in_specs=[VMEM] * 3,
            out_specs=VMEM,
            scratch_shapes=[pltpu.VMEM((4, rows, width), f32), pltpu.VMEM((3, rows, width), f32),
                            pltpu.VMEM((3, rows, width), f32), dma((4,)), dma((4,)), dma((3,)), dma((3,))],
            compiler_params=pltpu.CompilerParams(collective_id=1, has_side_effects=True, vmem_limit_bytes=4 << 20),
            name='experts')(part, gate, h2)

        def unflat(cache):
            return cache.reshape(rows, heads, head_dim, cache.shape[2]).transpose(0, 1, 3, 2)

        return hidden_out, unflat(new_k), unflat(new_v)

    return jax.shard_map(decoder_block, mesh=mesh, in_specs=in_specs, out_specs=out_specs, check_vma=False)
```
